32 devices in a mesh: dp: 8 (over z, y), group: 4 (over x, core).
Axes of the slice: x: 2, y: 2, z: 4, core: 2. Of those that a mesh axis runs over, the one named last changes fastest.
Arguments:
- tokens: bfloat16 [16384, 1024], P(('dp', 'group')), may hold values from -16 to 16
- segment_ids: int32 [16384], P(('dp', 'group')), may hold values from 0 to 3, as said below
- positions: int32 [16384], P(('dp', 'group')), may hold values from 0 to 1999, as said below
- cotangent: bfloat16 [16384, 1024], P(('dp', 'group')), may hold values from -6 to 6
- qkv_weight: float32 [1024, 4096], P('group'), may hold values from -1 to 1
- out_weight: float32 [2048, 1024], P('group'), may hold values from -1 to 1
- gate_up_weight: float32 [1024, 6144], P('group'), may hold values from -0.1875 to 0.1875
- down_weight: float32 [3072, 1024], P('group'), may hold values from -0.109375 to 0.109375
- norm_gains: float32 [2, 1024], P(None, 'group'), may hold values from 0.5 to 1.5
- head_gains: float32 [2, 128], P(None, 'group'), may hold values from 0.6 to 1.4
- qkv_moments: float32 [2, 1024, 4096], P(None, 'group'), as said below
- out_moments: float32 [2, 2048, 1024], P(None, 'group'), as said below
- gate_up_moments: float32 [2, 1024, 6144], P(None, 'group'), as said below
- down_moments: float32 [2, 3072, 1024], P(None, 'group'), as said below
- norm_moments: float32 [2, 2, 1024], P(None, None, 'group'), as said below
- head_moments: float32 [2, 2, 128], P(None, None, 'group'), as said below
Outputs:
- output: bfloat16 [16384, 1024], P(('dp', 'group'))
- tokens_grad: bfloat16 [16384, 1024], P(('dp', 'group'))
- qkv_grad: float32 [1024, 4096], P('group', 'dp')
- out_grad: float32 [2048, 1024], P('group', 'dp')
- gate_up_grad: float32 [1024, 6144], P('group', 'dp')
- down_grad: float32 [3072, 1024], P('group', 'dp')
- norm_grad: float32 [2, 1024], P(None, 'group')
- head_grad: float32 [2, 128], P(None, 'group')
- new_qkv_weight: float32 [1024, 4096], P('group')
- new_out_weight: float32 [2048, 1024], P('group')
- new_gate_up_weight: float32 [1024, 6144], P('group')
- new_down_weight: float32 [3072, 1024], P('group')
- new_norm_gains: float32 [2, 1024], P(None, 'group')
- new_head_gains: float32 [2, 128], P(None, 'group')
- new_qkv_moments: float32 [2, 1024, 4096], P(None, 'group')
- new_out_moments: float32 [2, 2048, 1024], P(None, 'group')
- new_gate_up_moments: float32 [2, 1024, 6144], P(None, 'group')
- new_down_moments: float32 [2, 3072, 1024], P(None, 'group')
- new_norm_moments: float32 [2, 2, 1024], P(None, None, 'group')
- new_head_moments: float32 [2, 2, 128], P(None, None, 'group')
The draws below stay inside these ranges and needn't reach their ends.
Inputs may be any that keep to these rules, and one draw needn't show every extreme that they name: `segment_ids`: along each sequence of 512 consecutive tokens the ids never fall; equal ids within a sequence mark one document. A token's position counts from its document's first token, which may lie in an earlier sequence; within a document positions rise by one. `qkv_moments`: the second moments are positive. `out_moments`: the second moments are positive. `gate_up_moments`: the second moments are positive. `down_moments`: the second moments are positive. `norm_moments`: the second moments are positive. `head_moments`: the second moments are positive.
All inputs are finite; a program needn't handle non-finite values.
Results may differ from the reference program's by a relative error of at most 0.013.
The reference program's roundings to bfloat16 on the way count: a program that leaves them out, or rounds other values in their place, can miss the bound.
Values may be sent and summed in bfloat16 or wider, within the bound.
A program may use at most 320 MiB of HBM per device.

```python
import math
import jax
import jax.numpy as jnp
from jax import lax

D = 1024
HQ = 16
HK = 8
HD = 128
FF = 3072
SEQ_LEN = 512
DOC_MIN = 200
DOC_MAX = 2000
TOKENS = 16384
PARAMS = 15730944


def draw_tokens(key, part):
    feature = jnp.arange(D, dtype=jnp.float32) / D
    spread = jnp.exp(jnp.log(3.0) * feature)
    values = jax.random.normal(key, (TOKENS, D), jnp.float32) * spread
    return jnp.clip(values, -16.0, 16.0).astype(jnp.bfloat16)


def document_layout(key):
    seq_count = TOKENS // SEQ_LEN
    lengths = jax.random.randint(jax.random.fold_in(key, 11), (seq_count, 8), DOC_MIN, DOC_MAX + 1)
    lengths = lengths.at[0, 1:].set(DOC_MIN)
    lengths = lengths.at[1, 0].set(DOC_MAX)
    before = jax.random.randint(jax.random.fold_in(key, 12), (seq_count, 1), 0, lengths[:, :1])
    before = before.at[0, 0].set(lengths[0, 0] - 1)
    before = before.at[1, 0].set(DOC_MAX - SEQ_LEN)
    ends = jnp.cumsum(lengths, axis=1) - before
    starts = ends - lengths
    places = jnp.arange(SEQ_LEN, dtype=jnp.int32)
    segment = jnp.sum((ends[:, None, :] <= places[None, :, None]).astype(jnp.int32), axis=2)
    start_of = jnp.take_along_axis(starts, segment, axis=1)
    return (segment.reshape(TOKENS).astype(jnp.int32), (places[None, :] - start_of).reshape(TOKENS).astype(jnp.int32))


def draw_segment_ids(key, part):
    return document_layout(key)[0]


def draw_positions(key, part):
    return document_layout(key)[1]


def draw_qkv_weight(key, part):
    columns = (HQ + 2 * HK) * HD
    values = jax.random.normal(key, (D, columns), jnp.float32) / math.sqrt(D)
    return jnp.clip(values, -1.0, 1.0)


def draw_head_gains(key, part):
    return jax.random.uniform(key, (2, HD), jnp.float32, 0.6, 1.4)


def moment_pair(key, layout):
    first_moment = jnp.clip(jax.random.normal(key, layout, jnp.float32), -4.0, 4.0) * 0.15
    low_end = math.log(0.05 / 0.95)
    high_end = math.log(4.0 * 0.05 / 0.95)
    second = jnp.exp(jax.random.uniform(jax.random.fold_in(key, 5), layout, jnp.float32, low_end, high_end))
    return jnp.stack([first_moment, second])


def draw_qkv_moments(key, part):
    return moment_pair(jax.random.fold_in(key, 101), (D, (HQ + 2 * HK) * HD))


def draw_out_moments(key, part):
    return moment_pair(jax.random.fold_in(key, 102), (HQ * HD, D))


def draw_gate_up_moments(key, part):
    return moment_pair(jax.random.fold_in(key, 103), (D, 2 * FF))


def draw_down_moments(key, part):
    return moment_pair(jax.random.fold_in(key, 104), (FF, D))


def draw_norm_moments(key, part):
    return moment_pair(jax.random.fold_in(key, 105), (2, D))


def draw_head_moments(key, part):
    return moment_pair(jax.random.fold_in(key, 106), (2, HD))


def shard_levels(own_key, dims, shards, smallest, top_value):
    def one(dim, parts):
        steps = jax.random.uniform(jax.random.fold_in(jax.random.fold_in(own_key, 6), dim), (parts,), jnp.float32, smallest / len(shards), top_value / len(shards))
        return jnp.repeat(jnp.exp(steps), dims[dim] // parts).reshape((-1,) + (1,) * (len(dims) - dim - 1))

    level = one(*shards[0])
    for cut in shards[1:]:
        level = level * one(*cut)
    return level


def noise(stream_key, shape, scale, reach, cuts=(), kind=jnp.bfloat16):
    result = scale * jax.random.normal(stream_key, shape, jnp.float32)
    if cuts:
        result = result * shard_levels(stream_key, shape, cuts, -0.22, 0.18)
    return jnp.clip(result, -reach, reach).astype(kind)


def setup_inputs(seed: int = 0) -> dict:
    streams_of = jax.random.split(jax.random.key(seed), 17)
    return {
        "tokens": draw_tokens(jax.random.fold_in(streams_of[16], 71), 0),
        "segment_ids": draw_segment_ids(jax.random.fold_in(streams_of[16], 71), 0),
        "positions": draw_positions(jax.random.fold_in(streams_of[16], 71), 0),
        "cotangent": noise(streams_of[3], (TOKENS, D), 1.0, 6.0, ((0, 32),)),
        "qkv_weight": draw_qkv_weight(jax.random.fold_in(streams_of[16], 71), 0),
        "out_weight": noise(streams_of[5], (HQ * HD, D), (HQ * HD // 64) ** -0.5, 1.0, ((0, 4),), jnp.float32),
        "gate_up_weight": noise(streams_of[6], (D, 2 * FF), D ** -0.5, 0.1875, ((0, 4),), jnp.float32),
        "down_weight": noise(streams_of[7], (FF, D), FF ** -0.5, 0.109375, ((0, 4),), jnp.float32),
        "norm_gains": jnp.clip(1.0 + 0.1 * jax.random.normal(streams_of[8], (2, D), jnp.float32), 0.5, 1.5),
        "head_gains": draw_head_gains(jax.random.fold_in(streams_of[16], 71), 0),
        "qkv_moments": draw_qkv_moments(jax.random.fold_in(streams_of[16], 71), 0),
        "out_moments": draw_out_moments(jax.random.fold_in(streams_of[16], 71), 0),
        "gate_up_moments": draw_gate_up_moments(jax.random.fold_in(streams_of[16], 71), 0),
        "down_moments": draw_down_moments(jax.random.fold_in(streams_of[16], 71), 0),
        "norm_moments": draw_norm_moments(jax.random.fold_in(streams_of[16], 71), 0),
        "head_moments": draw_head_moments(jax.random.fold_in(streams_of[16], 71), 0),
    }


@jax.custom_vjp
def low(v):
    return lax.optimization_barrier(v.astype(jnp.bfloat16)).astype(jnp.float32)

@jax.custom_vjp
def low_back(v):
    return v

def low_keep(v):
    return (low(v), None)

def low_pass(kept, grad):
    return (grad,)

def back_keep(v):
    return (v, None)

def back_low(kept, grad):
    return (low(grad),)
low.defvjp(low_keep, low_pass)
low_back.defvjp(back_keep, back_low)
EPS_NORM = 1e-06
ROPE_BASE = 1000000.0
MASKED = -1e+30
LEARN_RATE = 0.03
GAIN_RATE = 0.3
WEIGHT_DECAY = 0.1
BETA_ONE = 0.9
BETA_TWO = 0.95
ADAM_EPS = 1e-08
STEP_COUNT = 3.0

def exact_dot(left_side, right_side):
    return jnp.dot(left_side, right_side, precision=lax.Precision.HIGHEST)

def normalize(values):
    return values * lax.rsqrt(lax.optimization_barrier(jnp.mean(values * values, axis=-1, keepdims=True)) + EPS_NORM)

def rotary_tables(places, width):
    half_width = width // 2
    frequency = ROPE_BASE ** (-(jnp.arange(half_width, dtype=jnp.float32) * 2.0) / width)
    angles = places.astype(jnp.float32)[:, None] * frequency[None, :]
    return (jnp.cos(angles), jnp.sin(angles))

def rotate(values, cosine, sine_table):
    half_width = values.shape[-1] // 2
    front_half = values[..., :half_width]
    back_half = values[..., half_width:]
    cosine = cosine[:, None, :]
    sine_table = sine_table[:, None, :]
    return jnp.concatenate([front_half * cosine - back_half * sine_table, back_half * cosine + front_half * sine_table], axis=-1)

def block_layer(weights, inputs, segment, places):
    qkv_w, out_w, gate_up_w, down_w, gains_norm, gains_head = weights
    groups = HQ // HK
    hidden_one = low(normalize(inputs) * gains_norm[0])
    projected = low_back(exact_dot(hidden_one, qkv_w))
    query_heads = projected[:, :HQ * HD].reshape(SEQ_LEN, HQ, HD)
    key_heads = projected[:, HQ * HD:(HQ + HK) * HD].reshape(SEQ_LEN, HK, HD)
    value_heads = low(projected[:, (HQ + HK) * HD:].reshape(SEQ_LEN, HK, HD))
    cosine, sine_table = rotary_tables(places, HD)
    query_heads = low(rotate(normalize(query_heads) * gains_head[0], cosine, sine_table))
    key_heads = low(rotate(normalize(key_heads) * gains_head[1], cosine, sine_table))
    query_heads = query_heads.reshape(SEQ_LEN, HK, groups, HD)
    scores = jnp.einsum('qkgd,pkd->kgqp', query_heads, key_heads, precision=lax.Precision.HIGHEST) * (1.0 / math.sqrt(HD))
    scores = low_back(scores)
    places_idx = jnp.arange(SEQ_LEN)
    allowed = (segment[:, None] == segment[None, :]) & (places_idx[:, None] >= places_idx[None, :])
    scores = jnp.where(allowed, scores, MASKED)
    attn_probs = low(jax.nn.softmax(scores, axis=-1))
    mixed_heads = jnp.einsum('kgqp,pkd->qkgd', attn_probs, value_heads, precision=lax.Precision.HIGHEST)
    mixed_heads = low(low_back(mixed_heads)).reshape(SEQ_LEN, HQ * HD)
    residual = inputs + low_back(exact_dot(mixed_heads, out_w))
    hidden_two = low(normalize(residual) * gains_norm[1])
    gate_up = low_back(exact_dot(hidden_two, gate_up_w))
    activated = low(jax.nn.silu(gate_up[:, :FF]) * gate_up[:, FF:])
    return residual + low_back(exact_dot(activated, down_w))

def adam_update(master, moment, gradient, factor, step_rate, decay_rate):
    clipped = gradient * factor
    first_moment = BETA_ONE * moment[0] + (1.0 - BETA_ONE) * clipped
    second = BETA_TWO * moment[1] + (1.0 - BETA_TWO) * clipped * clipped
    first_hat = first_moment / (1.0 - BETA_ONE ** STEP_COUNT)
    second_hat = second / (1.0 - BETA_TWO ** STEP_COUNT)
    renewed = master - step_rate * (first_hat / (jnp.sqrt(second_hat) + ADAM_EPS) + decay_rate * master)
    return (renewed, jnp.stack([first_moment, second]))

def reference(tokens, segment_ids, positions, cotangent, qkv_weight, out_weight, gate_up_weight, down_weight, norm_gains, head_gains, qkv_moments, out_moments, gate_up_moments, down_moments, norm_moments, head_moments):
    masters = (qkv_weight, out_weight, gate_up_weight, down_weight, norm_gains, head_gains)
    moments = (qkv_moments, out_moments, gate_up_moments, down_moments, norm_moments, head_moments)
    seq_count = TOKENS // SEQ_LEN
    per_step = math.gcd(seq_count, max(1, 4096 // SEQ_LEN))
    steps_shape = (seq_count // per_step, per_step, SEQ_LEN)
    inputs = tokens.astype(jnp.float32).reshape(steps_shape + (D,))
    upstream = cotangent.astype(jnp.float32).reshape(steps_shape + (D,))
    segments = segment_ids.reshape(steps_shape)
    places = positions.reshape(steps_shape)

    def forward(weights, acts):
        rounded = tuple((low(weight) for weight in weights))

        def one_step(block_pack):
            acts_block, seg_block, place_block = block_pack

            def single(acts_one, seg_one, place_one):
                return block_layer(rounded, acts_one, seg_one, place_one)
            return jax.vmap(single)(acts_block, seg_block, place_block)
        return lax.map(jax.checkpoint(one_step), (acts, segments, places))
    outs, pullback = jax.vjp(forward, masters, inputs)
    grads, grad_inputs = pullback(upstream)
    output = outs.reshape(TOKENS, D).astype(jnp.bfloat16)
    tokens_grad = grad_inputs.reshape(TOKENS, D).astype(jnp.bfloat16)
    squares = sum((jnp.sum(gradient * gradient) for gradient in grads))
    clip_limit = math.sqrt(PARAMS)
    factor = clip_limit / jnp.maximum(jnp.sqrt(squares), clip_limit)
    rates = (LEARN_RATE, LEARN_RATE, LEARN_RATE, LEARN_RATE, GAIN_RATE, GAIN_RATE)
    decays = (WEIGHT_DECAY, WEIGHT_DECAY, WEIGHT_DECAY, WEIGHT_DECAY, 0.0, 0.0)
    renewed_all = []
    moments_all = []
    for master, moment, gradient, step_rate, decay_rate in zip(masters, moments, grads, rates, decays):
        renewed, stacked = adam_update(master, moment, gradient, factor, step_rate, decay_rate)
        renewed_all.append(renewed)
        moments_all.append(stacked)
    return (output, tokens_grad, grads[0], grads[1], grads[2], grads[3], grads[4], grads[5], renewed_all[0], renewed_all[1], renewed_all[2], renewed_all[3], renewed_all[4], renewed_all[5], moments_all[0], moments_all[1], moments_all[2], moments_all[3], moments_all[4], moments_all[5])
```

```python
import math

import jax
import jax.numpy as jnp
from jax import lax
from jax.experimental import pallas as pl
from jax.experimental.pallas import tpu as pltpu
from jax.sharding import PartitionSpec as P

HQ = 16
HK = 8
HD = 128
FF = 3072
SEQ_LEN = 512
PARAMS = 15730944


EPS_NORM = 1e-06
ROPE_BASE = 1000000.0
MASKED = -1e30
LEARN_RATE = 0.03
GAIN_RATE = 0.3
WEIGHT_DECAY = 0.1
BETA_ONE = 0.9
BETA_TWO = 0.95
ADAM_EPS = 1e-08
STEP_COUNT = 3.0


def rotary_tables(places, width):
    half_width = width // 2
    frequency = ROPE_BASE ** (-(jnp.arange(half_width, dtype=jnp.float32) * 2.0) / width)
    angles = places.astype(jnp.float32)[:, None] * frequency[None, :]
    return (jnp.cos(angles), jnp.sin(angles))


def rotate(values, cosine, sine_table):
    half_width = values.shape[-1] // 2
    front_half = values[..., :half_width]
    back_half = values[..., half_width:]
    cosine = cosine[:, None, :]
    sine_table = sine_table[:, None, :]
    return jnp.concatenate(
        [
            front_half * cosine - back_half * sine_table,
            back_half * cosine + front_half * sine_table,
        ],
        axis=-1,
    )


def contract_rows(left_side, right_side):
    return lax.dot_general(
        left_side, right_side, (((0,), (0,)), ((), ())), preferred_element_type=jnp.float32
    )


def contract_cols(left_side, right_side):
    return lax.dot_general(
        left_side, right_side, (((1,), (1,)), ((), ())), preferred_element_type=jnp.float32
    )


def norm_back(grad_out, normed, inv_root, gain):
    scaled = grad_out * gain
    return inv_root * (scaled - normed * jnp.mean(normed * scaled, axis=-1, keepdims=True))


def swap(value, axis, mask):
    count = lax.axis_size(axis)
    return lax.ppermute(value, axis, [(i, i ^ mask) for i in range(count)])


def bit_masks(count):
    return [1 << i for i in range(count.bit_length() - 1)]


def gather_rows(shard):
    owners = lax.axis_size("group")
    copies = lax.axis_size("dp")
    mine = lax.axis_index("group")
    rows, columns = shard.shape
    half = rows // 2
    side = lax.axis_index("dp") & 1
    split = copies > 1
    pieces = [(shard, 0, 0)]
    for mask in bit_masks(owners)[1:]:
        if mask == 2 and split:
            near = lax.dynamic_slice_in_dim(shard, side * half, half, 0)
            first = swap(near, "group", mask)
            second = swap(first, "dp", 1)
            pieces += [(first, mask, side * half), (second, mask, (1 - side) * half)]
        else:
            pieces += [(swap(v, "group", mask), dg ^ mask, off) for v, dg, off in pieces]
    pieces += [(swap(v, "group", 1), dg ^ 1, off) for v, dg, off in pieces]
    full = jnp.zeros((rows * owners, columns), shard.dtype)
    for value, delta, offset in pieces:
        start = (mine ^ delta) * rows + offset
        full = lax.dynamic_update_slice(full, value, (start, 0))
    return full


def spread_bits(position, masks):
    total = 0
    count = len(masks)
    for i, mask in enumerate(masks):
        total = total + ((position >> (count - 1 - i)) & 1) * mask
    return total


def grad_blocks(left, right, row_sets, column_masks):
    tokens, rows = left.shape
    columns = right.shape[1]
    owners = lax.axis_size("group")
    copies = lax.axis_size("dp")
    row_block = rows // owners
    column_block = columns // copies
    mine = lax.axis_index("group")
    here = lax.axis_index("dp")
    if column_block % 128 or row_block % 16:
        ordered = jnp.concatenate(
            [
                lax.dynamic_slice_in_dim(
                    right, (here ^ spread_bits(p, column_masks)) * column_block, column_block, 1
                )
                for p in range(copies)
            ],
            axis=1,
        )
        return [
            jnp.stack(
                [
                    contract_rows(
                        lax.dynamic_slice_in_dim(left, (mine ^ dg) * row_block, row_block, 1),
                        ordered,
                    ).astype(jnp.bfloat16)
                    for dg in row_set
                ]
            )
            for row_set in row_sets
        ]

    def body(where, left_ref, right_ref, *rest):
        outs, turned = rest[:-1], rest[-1]

        @pl.when(pl.program_id(0) == 0)
        def _():
            turned[...] = left_ref[...].T

        for out, row_set in zip(outs, row_sets):
            for k, dg in enumerate(row_set):
                start = pl.multiple_of((where[0] ^ dg) * row_block, row_block)
                out[k] = jnp.dot(
                    turned[pl.ds(start, row_block), :],
                    right_ref[...],
                    preferred_element_type=jnp.float32,
                ).astype(jnp.bfloat16)

    count = sum(len(row_set) for row_set in row_sets)
    return pl.pallas_call(
        body,
        out_shape=[
            jax.ShapeDtypeStruct((len(row_set), row_block, columns), jnp.bfloat16)
            for row_set in row_sets
        ],
        grid_spec=pltpu.PrefetchScalarGridSpec(
            num_scalar_prefetch=1,
            grid=(copies,),
            in_specs=[
                pl.BlockSpec((tokens, rows), lambda p, where: (0, 0)),
                pl.BlockSpec(
                    (tokens, column_block),
                    lambda p, where: (0, where[1] ^ spread_bits(p, column_masks)),
                ),
            ],
            out_specs=[
                pl.BlockSpec((len(row_set), row_block, column_block), lambda p, where: (0, 0, p))
                for row_set in row_sets
            ],
            scratch_shapes=[pltpu.VMEM((rows, tokens), jnp.bfloat16)],
        ),
        compiler_params=pltpu.CompilerParams(vmem_limit_bytes=48 * 1024 * 1024),
        cost_estimate=pl.CostEstimate(
            flops=2 * tokens * count * row_block * columns,
            bytes_accessed=2 * (tokens * rows + tokens * columns + count * row_block * columns),
            transcendentals=0,
        ),
    )(jnp.stack([mine, here]).astype(jnp.int32), left, right)


def reduce_grad(left, right):
    owners = lax.axis_size("group")
    copies = lax.axis_size("dp")
    group_masks = bit_masks(owners)
    column_masks = bit_masks(copies)
    row_sets = []
    for i, mask in enumerate(group_masks):
        later = group_masks[i + 1 :]
        row_sets.append([mask + spread_bits(p, later) for p in range(1 << len(later))])
    row_sets.append([0])
    first = grad_blocks(left, right, row_sets[:1], column_masks)
    others = grad_blocks(left, right, row_sets[1:], column_masks)
    kept = list(first) + list(others)
    got = []
    for i, mask in enumerate(group_masks):
        size = 1 << (len(group_masks) - 1 - i)
        outgoing = kept[i]
        if got:
            outgoing = sum(
                (v[size : 2 * size].astype(jnp.float32) for v in got),
                outgoing.astype(jnp.float32),
            ).astype(jnp.bfloat16)
        got.append(swap(outgoing, "group", mask))
    parts = [kept[-1][0]] + [v[0] for v in got]
    width = right.shape[1]
    for mask in column_masks:
        width //= 2
        outgoing = sum(v[:, width : 2 * width].astype(jnp.float32) for v in parts)
        parts.append(swap(outgoing.astype(jnp.bfloat16), "dp", mask))
    return sum(v[:, :width].astype(jnp.float32) for v in parts)


def gather_grad(own):
    blocks = [(own.astype(jnp.bfloat16), 0)]
    for mask in reversed(bit_masks(lax.axis_size("dp"))):
        blocks += [(swap(v, "dp", mask), dd ^ mask) for v, dd in blocks]
    return blocks


def adam_core(master, first_moment, second_moment, clipped, step_rate, decay_rate):
    first_new = BETA_ONE * first_moment + (1.0 - BETA_ONE) * clipped
    second_new = BETA_TWO * second_moment + (1.0 - BETA_TWO) * clipped * clipped
    first_hat = first_new / (1.0 - BETA_ONE**STEP_COUNT)
    second_hat = second_new / (1.0 - BETA_TWO**STEP_COUNT)
    renewed = master - step_rate * (
        first_hat / (jnp.sqrt(second_hat) + ADAM_EPS) + decay_rate * master
    )
    return renewed, first_new, second_new


def adam_blocks(master, moment, blocks, factor, step_rate, decay_rate):
    rows, columns = master.shape
    copies = lax.axis_size("dp")
    here = lax.axis_index("dp")
    width = columns // copies
    if width % 128:
        full = jnp.zeros(master.shape, jnp.float32)
        for value, dd in blocks:
            full = lax.dynamic_update_slice(
                full, value.astype(jnp.float32), (0, (here ^ dd) * width)
            )
        return adam_update(master, moment, full, factor, step_rate, decay_rate)
    tile = 32

    def body(where, factor_ref, master_ref, moment_ref, *rest):
        grads, (new_ref, state_ref) = rest[:-2], rest[-2:]
        scale = factor_ref[0, 0]
        for grad, (_, dd) in zip(grads, blocks):
            at = pl.ds(pl.multiple_of((where[0] ^ dd) * width, 128), width)
            renewed, first_new, second_new = adam_core(
                master_ref[:, at],
                moment_ref[0, :, at],
                moment_ref[1, :, at],
                grad[...].astype(jnp.float32) * scale,
                step_rate,
                decay_rate,
            )
            new_ref[:, at] = renewed
            state_ref[0, :, at] = first_new
            state_ref[1, :, at] = second_new

    return pl.pallas_call(
        body,
        out_shape=[
            jax.ShapeDtypeStruct(master.shape, jnp.float32),
            jax.ShapeDtypeStruct(moment.shape, jnp.float32),
        ],
        grid_spec=pltpu.PrefetchScalarGridSpec(
            num_scalar_prefetch=1,
            grid=(rows // tile,),
            in_specs=[
                pl.BlockSpec(memory_space=pltpu.SMEM),
                pl.BlockSpec((tile, columns), lambda i, where: (i, 0)),
                pl.BlockSpec((2, tile, columns), lambda i, where: (0, i, 0)),
            ]
            + [pl.BlockSpec((tile, width), lambda i, where: (i, 0))] * len(blocks),
            out_specs=[
                pl.BlockSpec((tile, columns), lambda i, where: (i, 0)),
                pl.BlockSpec((2, tile, columns), lambda i, where: (0, i, 0)),
            ],
        ),
        compiler_params=pltpu.CompilerParams(vmem_limit_bytes=48 * 1024 * 1024),
        cost_estimate=pl.CostEstimate(
            flops=20 * rows * columns,
            bytes_accessed=26 * rows * columns,
            transcendentals=rows * columns,
        ),
    )(
        here.reshape(1).astype(jnp.int32),
        factor.reshape(1, 1),
        master,
        moment,
        *[value for value, _ in blocks],
    )


def adam_update(master, moment, gradient, factor, step_rate, decay_rate):
    clipped = gradient * factor
    first_moment = BETA_ONE * moment[0] + (1.0 - BETA_ONE) * clipped
    second = BETA_TWO * moment[1] + (1.0 - BETA_TWO) * clipped * clipped
    first_hat = first_moment / (1.0 - BETA_ONE**STEP_COUNT)
    second_hat = second / (1.0 - BETA_TWO**STEP_COUNT)
    renewed = master - step_rate * (
        first_hat / (jnp.sqrt(second_hat) + ADAM_EPS) + decay_rate * master
    )
    return (renewed, jnp.stack([first_moment, second]))


def on_device(
    tokens,
    segment_ids,
    positions,
    cotangent,
    qkv_weight,
    out_weight,
    gate_up_weight,
    down_weight,
    norm_gains,
    head_gains,
    qkv_moments,
    out_moments,
    gate_up_moments,
    down_moments,
    norm_moments,
    head_moments,
):
    full_norm = lax.all_gather(norm_gains.astype(jnp.bfloat16), "group", axis=1, tiled=True)
    full_head = lax.all_gather(head_gains.astype(jnp.bfloat16), "group", axis=1, tiled=True)
    full_qkv = gather_rows(qkv_weight.astype(jnp.bfloat16))
    full_out = gather_rows(out_weight.astype(jnp.bfloat16))
    full_gate_up = gather_rows(gate_up_weight.astype(jnp.bfloat16))
    full_down = gather_rows(down_weight.astype(jnp.bfloat16))
    token_rows = tokens.shape[0]
    seq_count = token_rows // SEQ_LEN
    groups = HQ // HK
    inv_head = 1.0 / math.sqrt(HD)
    gain_one = full_norm[0].astype(jnp.float32)
    gain_two = full_norm[1].astype(jnp.float32)
    gain_query = full_head[0].astype(jnp.float32)
    gain_key = full_head[1].astype(jnp.float32)
    inputs = tokens.astype(jnp.float32)
    root_one = lax.rsqrt(jnp.mean(inputs * inputs, axis=-1, keepdims=True) + EPS_NORM)
    normed_one = inputs * root_one
    hidden_one = (normed_one * gain_one).astype(jnp.bfloat16)
    projected = jnp.dot(hidden_one, full_qkv, preferred_element_type=jnp.float32)
    query_raw = projected[:, : HQ * HD].reshape(token_rows, HQ, HD)
    key_raw = projected[:, HQ * HD : (HQ + HK) * HD].reshape(token_rows, HK, HD)
    value_low = projected[:, (HQ + HK) * HD :].reshape(token_rows, HK, HD).astype(jnp.bfloat16)
    cosine, sine_table = rotary_tables(positions, HD)
    query_root = lax.rsqrt(jnp.mean(query_raw * query_raw, axis=-1, keepdims=True) + EPS_NORM)
    query_normed = query_raw * query_root
    query_low = rotate(query_normed * gain_query, cosine, sine_table).astype(jnp.bfloat16)
    key_root = lax.rsqrt(jnp.mean(key_raw * key_raw, axis=-1, keepdims=True) + EPS_NORM)
    key_normed = key_raw * key_root
    key_low = rotate(key_normed * gain_key, cosine, sine_table).astype(jnp.bfloat16)
    query_blocks = query_low.reshape(seq_count, SEQ_LEN, HK, groups, HD)
    key_blocks = key_low.reshape(seq_count, SEQ_LEN, HK, HD)
    value_blocks = value_low.reshape(seq_count, SEQ_LEN, HK, HD)
    seg_blocks = segment_ids.reshape(seq_count, SEQ_LEN)
    places_idx = jnp.arange(SEQ_LEN)
    allowed = (seg_blocks[:, :, None] == seg_blocks[:, None, :]) & (
        places_idx[:, None] >= places_idx[None, :]
    )[None]
    allowed = allowed[:, None, None, :, :]

    def scores_of():
        raw_scores = (
            jnp.einsum(
                "sqkgd,spkd->skgqp", query_blocks, key_blocks, preferred_element_type=jnp.float32
            )
            * inv_head
        )
        return jnp.where(allowed, raw_scores, MASKED)

    scores = scores_of()
    row_peak = jnp.max(scores, axis=-1, keepdims=True)
    exp_total = jnp.sum(jnp.exp(scores - row_peak), axis=-1, keepdims=True)
    log_total = row_peak + jnp.log(exp_total)
    probs_low = jnp.exp(scores - log_total).astype(jnp.bfloat16)
    mixed_heads = jnp.einsum(
        "skgqp,spkd->sqkgd", probs_low, value_blocks, preferred_element_type=jnp.float32
    )
    mixed_low = mixed_heads.reshape(token_rows, HQ * HD).astype(jnp.bfloat16)
    attended = jnp.dot(mixed_low, full_out, preferred_element_type=jnp.float32)
    residual = inputs + attended
    root_two = lax.rsqrt(jnp.mean(residual * residual, axis=-1, keepdims=True) + EPS_NORM)
    normed_two = residual * root_two
    hidden_two = (normed_two * gain_two).astype(jnp.bfloat16)
    gate_up = jnp.dot(hidden_two, full_gate_up, preferred_element_type=jnp.float32)
    gate_part = gate_up[:, :FF]
    upward = gate_up[:, FF:]
    sigmoid_gate = jax.nn.sigmoid(gate_part)
    activated = (gate_part * sigmoid_gate * upward).astype(jnp.bfloat16)
    branch = jnp.dot(activated, full_down, preferred_element_type=jnp.float32)
    output = (residual + branch).astype(jnp.bfloat16)
    upstream = cotangent.astype(jnp.float32)
    down_own = reduce_grad(activated, cotangent)
    grad_act = contract_cols(cotangent, full_down)
    grad_gate = grad_act * upward * sigmoid_gate * (1.0 + gate_part * (1.0 - sigmoid_gate))
    grad_up = grad_act * gate_part * sigmoid_gate
    grad_gate_up = jnp.concatenate([grad_gate, grad_up], axis=-1).astype(jnp.bfloat16)
    gate_up_own = reduce_grad(hidden_two, grad_gate_up)
    grad_hidden_two = contract_cols(grad_gate_up, full_gate_up)
    grad_gain_two = jnp.sum(grad_hidden_two * normed_two, axis=0)
    grad_residual = upstream + norm_back(grad_hidden_two, normed_two, root_two, gain_two)
    residual_low = grad_residual.astype(jnp.bfloat16)
    out_own = reduce_grad(mixed_low, residual_low)
    grad_mixed = (
        contract_cols(residual_low, full_out)
        .astype(jnp.bfloat16)
        .reshape(seq_count, SEQ_LEN, HK, groups, HD)
    )
    attn_probs = jnp.exp(scores_of() - log_total)
    grad_probs = jnp.einsum(
        "sqkgd,spkd->skgqp", grad_mixed, value_blocks, preferred_element_type=jnp.float32
    )
    grad_value = jnp.einsum(
        "skgqp,sqkgd->spkd",
        attn_probs.astype(jnp.bfloat16),
        grad_mixed,
        preferred_element_type=jnp.float32,
    )
    grad_scores = (
        attn_probs * (grad_probs - jnp.sum(attn_probs * grad_probs, axis=-1, keepdims=True))
    ).astype(jnp.bfloat16)
    grad_query = (
        jnp.einsum("skgqp,spkd->sqkgd", grad_scores, key_blocks, preferred_element_type=jnp.float32)
        * inv_head
    )
    grad_key = (
        jnp.einsum(
            "skgqp,sqkgd->spkd", grad_scores, query_blocks, preferred_element_type=jnp.float32
        )
        * inv_head
    )
    grad_query = rotate(grad_query.reshape(token_rows, HQ, HD), cosine, -sine_table)
    grad_key = rotate(grad_key.reshape(token_rows, HK, HD), cosine, -sine_table)
    grad_gain_query = jnp.sum(grad_query * query_normed, axis=(0, 1))
    grad_gain_key = jnp.sum(grad_key * key_normed, axis=(0, 1))
    grad_query_raw = norm_back(grad_query, query_normed, query_root, gain_query)
    grad_key_raw = norm_back(grad_key, key_normed, key_root, gain_key)
    grad_projected = jnp.concatenate(
        [
            grad_query_raw.reshape(token_rows, HQ * HD),
            grad_key_raw.reshape(token_rows, HK * HD),
            grad_value.reshape(token_rows, HK * HD),
        ],
        axis=-1,
    ).astype(jnp.bfloat16)
    qkv_own = reduce_grad(hidden_one, grad_projected)
    grad_hidden_one = contract_cols(grad_projected, full_qkv)
    grad_gain_one = jnp.sum(grad_hidden_one * normed_one, axis=0)
    grad_inputs = grad_residual + norm_back(grad_hidden_one, normed_one, root_one, gain_one)
    tokens_grad = grad_inputs.astype(jnp.bfloat16)
    small = jnp.concatenate(
        [
            jnp.stack([grad_gain_one, grad_gain_two]),
            jnp.stack([grad_gain_query, grad_gain_key]),
        ],
        axis=1,
    )
    small = lax.psum(small, ("dp", "group"))
    width = small.shape[1] - HD
    norm_total = small[:, :width]
    head_total = small[:, width:]
    owned = (qkv_own, out_own, gate_up_own, down_own)
    squares = lax.psum(sum(jnp.sum(v * v) for v in owned), ("dp", "group"))
    squares = squares + jnp.sum(small * small)
    clip_limit = math.sqrt(PARAMS)
    factor = clip_limit / jnp.maximum(jnp.sqrt(squares), clip_limit)
    gathered = [gather_grad(v) for v in owned]
    masters = (qkv_weight, out_weight, gate_up_weight, down_weight)
    moments = (qkv_moments, out_moments, gate_up_moments, down_moments)
    renewed = [
        adam_blocks(master, moment, blocks, factor, LEARN_RATE, WEIGHT_DECAY)
        for master, moment, blocks in zip(masters, moments, gathered)
    ]
    mine = lax.axis_index("group")
    norm_grad = lax.dynamic_slice_in_dim(
        norm_total, mine * norm_gains.shape[1], norm_gains.shape[1], 1
    )
    head_grad = lax.dynamic_slice_in_dim(
        head_total, mine * head_gains.shape[1], head_gains.shape[1], 1
    )
    renewed.append(adam_update(norm_gains, norm_moments, norm_grad, factor, GAIN_RATE, 0.0))
    renewed.append(adam_update(head_gains, head_moments, head_grad, factor, GAIN_RATE, 0.0))
    return (
        output,
        tokens_grad,
        *owned,
        norm_grad,
        head_grad,
        *[new for new, _ in renewed],
        *[state for _, state in renewed],
    )


def solution(mesh):
    placed = (
        P(("dp", "group"), None),
        P(("dp", "group")),
        P(("dp", "group")),
        P(("dp", "group"), None),
        P("group", None),
        P("group", None),
        P("group", None),
        P("group", None),
        P(None, "group"),
        P(None, "group"),
        P(None, "group", None),
        P(None, "group", None),
        P(None, "group", None),
        P(None, "group", None),
        P(None, None, "group"),
        P(None, None, "group"),
    )
    return jax.shard_map(
        on_device,
        mesh=mesh,
        in_specs=placed,
        out_specs=(
            P(("dp", "group"), None),
            P(("dp", "group"), None),
            P("group", "dp"),
            P("group", "dp"),
            P("group", "dp"),
            P("group", "dp"),
            P(None, "group"),
            P(None, "group"),
            P("group", None),
            P("group", None),
            P("group", None),
            P("group", None),
            P(None, "group"),
            P(None, "group"),
            P(None, "group", None),
            P(None, "group", None),
            P(None, "group", None),
            P(None, "group", None),
            P(None, None, "group"),
            P(None, None, "group"),
        ),
        check_vma=False,
    )
```

```python
import math

import jax
import jax.numpy as jnp
from jax import lax
from jax.experimental import pallas as pl
from jax.experimental.pallas import tpu as pltpu
from jax.sharding import PartitionSpec as P

HQ = 16
HK = 8
HD = 128
FF = 3072
SEQ_LEN = 512
PARAMS = 15730944


EPS_NORM = 1e-06
ROPE_BASE = 1000000.0
MASKED = -1e30
LEARN_RATE = 0.03
GAIN_RATE = 0.3
WEIGHT_DECAY = 0.1
BETA_ONE = 0.9
BETA_TWO = 0.95
ADAM_EPS = 1e-08
STEP_COUNT = 3.0


def rotary_tables(places, width):
    half_width = width // 2
    frequency = ROPE_BASE ** (-(jnp.arange(half_width, dtype=jnp.float32) * 2.0) / width)
    angles = places.astype(jnp.float32)[:, None] * frequency[None, :]
    cosine, sine = jnp.cos(angles), jnp.sin(angles)
    return (
        jnp.concatenate([cosine, cosine], axis=1),
        jnp.concatenate([-sine, sine], axis=1),
    )


def contract_rows(left_side, right_side):
    return lax.dot_general(
        left_side, right_side, (((0,), (0,)), ((), ())), preferred_element_type=jnp.float32
    )


def contract_cols(left_side, right_side):
    return lax.dot_general(
        left_side, right_side, (((1,), (1,)), ((), ())), preferred_element_type=jnp.float32
    )


def norm_back(grad_out, normed, inv_root, gain):
    scaled = grad_out * gain
    return inv_root * (scaled - normed * jnp.mean(normed * scaled, axis=-1, keepdims=True))


def swap(value, axis, mask):
    count = lax.axis_size(axis)
    return lax.ppermute(value, axis, [(i, i ^ mask) for i in range(count)])


def bit_masks(count):
    return [1 << i for i in range(count.bit_length() - 1)]


def after(value, *others):
    return lax.optimization_barrier((value, others))[0]


def gather_rows(shard, chunks, previous):
    owners = lax.axis_size("group")
    copies = lax.axis_size("dp")
    mine = lax.axis_index("group")
    rows, columns = shard.shape
    half = rows // 2
    side = lax.axis_index("dp") & 1
    split = copies > 1
    pieces = [(shard, 0, 0)]
    order = previous
    for mask in bit_masks(owners)[1:]:
        if mask == 2 and split:
            size = half // chunks
            for c in range(chunks):
                near_at = side * half + c * size
                far_at = (1 - side) * half + c * size
                near = lax.dynamic_slice_in_dim(shard, near_at, size, 0)
                if order is not None:
                    near = after(near, order)
                order = swap(near, "group", mask)
                pieces += [
                    (order, mask, near_at),
                    (swap(order, "dp", 1), mask, far_at),
                ]
        else:
            pieces += [(swap(v, "group", mask), dg ^ mask, off) for v, dg, off in pieces]
    pieces += [(swap(v, "group", 1), dg ^ 1, off) for v, dg, off in pieces]
    full = jnp.zeros((rows * owners, columns), shard.dtype)
    for value, delta, offset in pieces:
        start = (mine ^ delta) * rows + offset
        full = lax.dynamic_update_slice(full, value, (start, 0))
    return full, order


def gather_small(shard):
    owners = lax.axis_size("group")
    mine = lax.axis_index("group")
    width = shard.shape[1]
    held = shard[None]
    deltas = [0]
    for mask in reversed(bit_masks(owners)):
        held = jnp.concatenate([held, swap(held, "group", mask)], axis=0)
        deltas += [d ^ mask for d in deltas]
    full = jnp.zeros((shard.shape[0], width * owners), shard.dtype)
    for k, delta in enumerate(deltas):
        full = lax.dynamic_update_slice(full, held[k], (0, (mine ^ delta) * width))
    return full


def sum_all(value):
    for axis in ("group", "dp"):
        for mask in bit_masks(lax.axis_size(axis)):
            value = value + swap(value, axis, mask)
    return value


def spread_bits(position, masks):
    total = 0
    count = len(masks)
    for i, mask in enumerate(masks):
        total = total + ((position >> (count - 1 - i)) & 1) * mask
    return total


def grad_blocks(left, right):
    tokens, rows = left.shape
    columns = right.shape[1]
    owners = lax.axis_size("group")
    copies = lax.axis_size("dp")
    column_masks = bit_masks(copies)
    later = bit_masks(owners)[1:]
    staying = [spread_bits(p, later) for p in range(1 << len(later))]
    row_sets = [[dg + 1 for dg in staying], staying] if owners > 1 else [[0]]
    row_block = rows // owners
    column_block = columns // copies
    mine = lax.axis_index("group")
    here = lax.axis_index("dp")
    if column_block % 128 or row_block % 16:
        ordered = jnp.concatenate(
            [
                lax.dynamic_slice_in_dim(
                    right, (here ^ spread_bits(p, column_masks)) * column_block, column_block, 1
                )
                for p in range(copies)
            ],
            axis=1,
        )
        return [
            jnp.stack(
                [
                    contract_rows(
                        lax.dynamic_slice_in_dim(left, (mine ^ dg) * row_block, row_block, 1),
                        ordered,
                    ).astype(jnp.bfloat16)
                    for dg in row_set
                ]
            )
            for row_set in row_sets
        ]
    wide = 2 if column_block % 256 and copies % 2 == 0 else 1

    def body(where, left_ref, *rest):
        rights, outs, turned = rest[:wide], rest[wide:-1], rest[-1]

        @pl.when(pl.program_id(0) == 0)
        def _():
            turned[...] = left_ref[...].T

        block = jnp.concatenate([ref[...] for ref in rights], axis=1)
        for out, row_set in zip(outs, row_sets):
            for k, dg in enumerate(row_set):
                start = pl.multiple_of((where[0] ^ dg) * row_block, row_block)
                out[k] = jnp.dot(
                    turned[pl.ds(start, row_block), :],
                    block,
                    preferred_element_type=jnp.float32,
                ).astype(jnp.bfloat16)

    def right_spec(j):
        return pl.BlockSpec(
            (tokens, column_block),
            lambda p, where: (0, where[1] ^ spread_bits(p * wide + j, column_masks)),
        )

    return pl.pallas_call(
        body,
        out_shape=[
            jax.ShapeDtypeStruct((len(row_set), row_block, columns), jnp.bfloat16)
            for row_set in row_sets
        ],
        grid_spec=pltpu.PrefetchScalarGridSpec(
            num_scalar_prefetch=1,
            grid=(copies // wide,),
            in_specs=[pl.BlockSpec((tokens, rows), lambda p, where: (0, 0))]
            + [right_spec(j) for j in range(wide)],
            out_specs=[
                pl.BlockSpec(
                    (len(row_set), row_block, column_block * wide), lambda p, where: (0, 0, p)
                )
                for row_set in row_sets
            ],
            scratch_shapes=[pltpu.VMEM((rows, tokens), jnp.bfloat16)],
        ),
        compiler_params=pltpu.CompilerParams(vmem_limit_bytes=48 * 1024 * 1024),
        cost_estimate=pl.CostEstimate(
            flops=2 * tokens * rows * columns,
            bytes_accessed=2 * (tokens * rows + tokens * columns + rows * columns),
            transcendentals=0,
        ),
    )(jnp.stack([mine, here]).astype(jnp.int32), left, *[right] * wide)


class GradSum:
    def __init__(self, left, right):
        blocks = grad_blocks(left, right)
        self.blocks = blocks
        group = [("group", m) for m in bit_masks(lax.axis_size("group"))]
        other = [("dp", m) for m in bit_masks(lax.axis_size("dp"))]
        held = [blocks[-1]]
        if group:
            held.append(swap(blocks[0], "group", 1))
        rest = group[1:]
        self.orders = [rest + other, other[:1] + rest + other[1:]]
        half = blocks[-1].shape[1] // 2
        self.parts = [
            [v[:, i * half : (i + 1) * half] for v in held] for i in range(2)
        ]
        self.length = len(rest) + len(other)
        self.step = 0

    def advance(self):
        sent = []
        if self.step == self.length:
            return sent
        for i, order in enumerate(self.orders):
            axis, mask = order[self.step]
            dim = 0 if axis == "group" else 2
            size = self.parts[i][0].shape[dim] // 2
            away = sum(
                lax.slice_in_dim(v, size, 2 * size, axis=dim).astype(jnp.float32)
                for v in self.parts[i]
            ).astype(jnp.bfloat16)
            stay = [lax.slice_in_dim(v, 0, size, axis=dim) for v in self.parts[i]]
            self.parts[i] = stay + [swap(away, axis, mask)]
            sent.append(away)
        self.step += 1
        return sent

    def finish(self):
        while self.step < self.length:
            self.advance()
        return jnp.concatenate(
            [sum(v[0].astype(jnp.float32) for v in part) for part in self.parts], axis=0
        )


def gather_grad(own):
    held = own.astype(jnp.bfloat16)[None]
    deltas = [0]
    groups = [(held, deltas)]
    masks = list(reversed(bit_masks(lax.axis_size("dp"))))
    for i, mask in enumerate(masks):
        got = swap(held, "dp", mask)
        got_deltas = [d ^ mask for d in deltas]
        if i + 1 < len(masks):
            held = jnp.concatenate([held, got], axis=0)
            deltas = deltas + got_deltas
            groups = [(held, deltas)]
        else:
            groups.append((got, got_deltas))
    return groups


def adam_core(master, first_moment, second_moment, clipped, step_rate, decay_rate):
    first_new = BETA_ONE * first_moment + (1.0 - BETA_ONE) * clipped
    second_new = BETA_TWO * second_moment + (1.0 - BETA_TWO) * clipped * clipped
    first_hat = first_new / (1.0 - BETA_ONE**STEP_COUNT)
    second_hat = second_new / (1.0 - BETA_TWO**STEP_COUNT)
    renewed = master - step_rate * (
        first_hat / (jnp.sqrt(second_hat) + ADAM_EPS) + decay_rate * master
    )
    return renewed, first_new, second_new


def adam_blocks(master, moment, blocks, factor, step_rate, decay_rate):
    rows, columns = master.shape
    copies = lax.axis_size("dp")
    here = lax.axis_index("dp")
    width = columns // copies
    if width % 128:
        full = jnp.zeros(master.shape, jnp.float32)
        for value, deltas in blocks:
            for k, dd in enumerate(deltas):
                full = lax.dynamic_update_slice(
                    full, value[k].astype(jnp.float32), (0, (here ^ dd) * width)
                )
        return adam_update(master, moment, full, factor, step_rate, decay_rate)
    tile = 32

    def body(where, factor_ref, master_ref, moment_ref, *rest):
        grads, (new_ref, state_ref) = rest[:-2], rest[-2:]
        scale = factor_ref[0, 0]
        for grad, (_, deltas) in zip(grads, blocks):
            for k, dd in enumerate(deltas):
                at = pl.ds(pl.multiple_of((where[0] ^ dd) * width, 128), width)
                renewed, first_new, second_new = adam_core(
                    master_ref[:, at],
                    moment_ref[0, :, at],
                    moment_ref[1, :, at],
                    grad[k].astype(jnp.float32) * scale,
                    step_rate,
                    decay_rate,
                )
                new_ref[:, at] = renewed
                state_ref[0, :, at] = first_new
                state_ref[1, :, at] = second_new

    return pl.pallas_call(
        body,
        out_shape=[
            jax.ShapeDtypeStruct(master.shape, jnp.float32),
            jax.ShapeDtypeStruct(moment.shape, jnp.float32),
        ],
        grid_spec=pltpu.PrefetchScalarGridSpec(
            num_scalar_prefetch=1,
            grid=(rows // tile,),
            in_specs=[
                pl.BlockSpec(memory_space=pltpu.SMEM),
                pl.BlockSpec((tile, columns), lambda i, where: (i, 0)),
                pl.BlockSpec((2, tile, columns), lambda i, where: (0, i, 0)),
            ]
            + [
                pl.BlockSpec((len(deltas), tile, width), lambda i, where: (0, i, 0))
                for _, deltas in blocks
            ],
            out_specs=[
                pl.BlockSpec((tile, columns), lambda i, where: (i, 0)),
                pl.BlockSpec((2, tile, columns), lambda i, where: (0, i, 0)),
            ],
        ),
        compiler_params=pltpu.CompilerParams(vmem_limit_bytes=48 * 1024 * 1024),
        cost_estimate=pl.CostEstimate(
            flops=20 * rows * columns,
            bytes_accessed=26 * rows * columns,
            transcendentals=rows * columns,
        ),
    )(
        here.reshape(1).astype(jnp.int32),
        factor.reshape(1, 1),
        master,
        moment,
        *[value for value, _ in blocks],
    )


def adam_update(master, moment, gradient, factor, step_rate, decay_rate):
    clipped = gradient * factor
    first_moment = BETA_ONE * moment[0] + (1.0 - BETA_ONE) * clipped
    second = BETA_TWO * moment[1] + (1.0 - BETA_TWO) * clipped * clipped
    first_hat = first_moment / (1.0 - BETA_ONE**STEP_COUNT)
    second_hat = second / (1.0 - BETA_TWO**STEP_COUNT)
    renewed = master - step_rate * (
        first_hat / (jnp.sqrt(second_hat) + ADAM_EPS) + decay_rate * master
    )
    return (renewed, jnp.stack([first_moment, second]))


def head_forward(raw, gain, cosine, sine):
    root = lax.rsqrt(jnp.mean(raw * raw, axis=-1, keepdims=True) + EPS_NORM)
    normed = raw * root
    scaled = normed * gain
    turned = scaled * cosine + pltpu.roll(scaled, HD // 2, 1) * sine
    return turned.astype(jnp.bfloat16), normed, root


def head_backward(grad, normed, root, gain, cosine, sine):
    turned = grad * cosine - pltpu.roll(grad, HD // 2, 1) * sine
    grad_gain = jnp.sum(turned * normed, axis=0, keepdims=True)
    scaled = turned * gain
    raw = root * (scaled - normed * jnp.mean(normed * scaled, axis=-1, keepdims=True))
    return raw, grad_gain


SPAN = 256


def span_weights(query_low, key_low, seg_row_ref, seg_col_ref, start):
    stop = start + SPAN
    scores = lax.dot_general(
        key_low[:stop],
        query_low[start:stop],
        (((1,), (1,)), ((), ())),
        preferred_element_type=jnp.float32,
    ) * (1.0 / math.sqrt(HD))
    key_at = lax.broadcasted_iota(jnp.int32, (stop, SPAN), 0)
    query_at = lax.broadcasted_iota(jnp.int32, (stop, SPAN), 1) + start
    allowed = (key_at <= query_at) & (seg_col_ref[:stop, :] == seg_row_ref[:, start:stop])
    scores = jnp.where(allowed, scores, MASKED)
    raised = jnp.exp(scores - jnp.max(scores, axis=0, keepdims=True))
    return raised * (1.0 / jnp.sum(raised, axis=0, keepdims=True))


def attend_body(
    query_ref, key_ref, value_ref, cos_ref, sin_ref, row_ref, col_ref, gain_ref, out_ref
):
    cosine, sine = cos_ref[...], sin_ref[...]
    key_low, _, _ = head_forward(key_ref[...], gain_ref[1:2, :], cosine, sine)
    value_turned = value_ref[...].astype(jnp.bfloat16).T
    for g in range(HQ // HK):
        at = slice(g * HD, (g + 1) * HD)
        query_low, _, _ = head_forward(query_ref[:, at], gain_ref[0:1, :], cosine, sine)
        for start in range(0, SEQ_LEN, SPAN):
            stop = start + SPAN
            weights = span_weights(query_low, key_low, row_ref, col_ref, start)
            mixed = jnp.dot(
                value_turned[:, :stop],
                weights.astype(jnp.bfloat16),
                preferred_element_type=jnp.float32,
            )
            out_ref[start:stop, at] = mixed.T.astype(jnp.bfloat16)


def attend_back_body(
    query_ref, key_ref, value_ref, cos_ref, sin_ref, row_ref, col_ref, gain_ref, grad_ref,
    out_ref, gain_out_ref,
):
    head = pl.program_id(1)
    cosine, sine = cos_ref[...], sin_ref[...]
    inv_head = 1.0 / math.sqrt(HD)

    @pl.when((pl.program_id(0) == 0) & (head == 0))
    def _():
        gain_out_ref[...] = jnp.zeros_like(gain_out_ref)

    key_low, key_normed, key_root = head_forward(key_ref[...], gain_ref[1:2, :], cosine, sine)
    value_low = value_ref[...].astype(jnp.bfloat16)
    key_turned = key_low.T
    grad_key = [jnp.zeros((SPAN, HD), jnp.float32)] * (SEQ_LEN // SPAN)
    grad_value = list(grad_key)
    gain_query = jnp.zeros((1, HD), jnp.float32)
    for g in range(HQ // HK):
        at = slice(g * HD, (g + 1) * HD)
        query_low, normed, root = head_forward(query_ref[:, at], gain_ref[0:1, :], cosine, sine)
        grad_query = []
        for start in range(0, SEQ_LEN, SPAN):
            stop = start + SPAN
            weights = span_weights(query_low, key_low, row_ref, col_ref, start)
            grad_out = grad_ref[start:stop, at]
            grad_weights = lax.dot_general(
                value_low[:stop],
                grad_out,
                (((1,), (1,)), ((), ())),
                preferred_element_type=jnp.float32,
            )
            more_value = jnp.dot(
                weights.astype(jnp.bfloat16), grad_out, preferred_element_type=jnp.float32
            )
            product = weights * grad_weights
            grad_scores = (
                weights * (grad_weights - jnp.sum(product, axis=0, keepdims=True))
            ).astype(jnp.bfloat16)
            more_key = jnp.dot(
                grad_scores, query_low[start:stop], preferred_element_type=jnp.float32
            )
            grad_query.append(
                jnp.dot(
                    key_turned[:, :stop], grad_scores, preferred_element_type=jnp.float32
                ).T
            )
            for j in range(stop // SPAN):
                part = slice(j * SPAN, (j + 1) * SPAN)
                grad_key[j] = grad_key[j] + more_key[part]
                grad_value[j] = grad_value[j] + more_value[part]
        raw, more_gain = head_backward(
            jnp.concatenate(grad_query, axis=0) * inv_head,
            normed,
            root,
            gain_ref[0:1, :],
            cosine,
            sine,
        )
        gain_query = gain_query + more_gain
        place = pl.multiple_of((head * (HQ // HK) + g) * HD, HD)
        out_ref[:, pl.ds(place, HD)] = raw.astype(jnp.bfloat16)
    raw, gain_key = head_backward(
        jnp.concatenate(grad_key, axis=0) * inv_head,
        key_normed,
        key_root,
        gain_ref[1:2, :],
        cosine,
        sine,
    )
    out_ref[:, pl.ds(pl.multiple_of((HQ + head) * HD, HD), HD)] = raw.astype(jnp.bfloat16)
    out_ref[:, pl.ds(pl.multiple_of((HQ + HK + head) * HD, HD), HD)] = jnp.concatenate(
        grad_value, axis=0
    ).astype(jnp.bfloat16)
    gain_out_ref[0:1, :] += gain_query
    gain_out_ref[1:2, :] += gain_key


def attention_call(body, projected, tables, segments, gains, grad_out):
    token_rows = projected.shape[0]
    seq_count = token_rows // SEQ_LEN
    groups = HQ // HK
    wide = groups * HD
    full = lambda s, h: (s, 0)
    in_specs = [
        pl.BlockSpec((SEQ_LEN, wide), lambda s, h: (s, h)),
        pl.BlockSpec((SEQ_LEN, HD), lambda s, h: (s, HQ + h)),
        pl.BlockSpec((SEQ_LEN, HD), lambda s, h: (s, HQ + HK + h)),
        pl.BlockSpec((SEQ_LEN, HD), full),
        pl.BlockSpec((SEQ_LEN, HD), full),
        pl.BlockSpec((1, SEQ_LEN), lambda s, h: (0, s)),
        pl.BlockSpec((SEQ_LEN, 1), full),
        pl.BlockSpec((2, HD), lambda s, h: (0, 0)),
    ]
    operands = [
        projected,
        projected,
        projected,
        *tables,
        segments[None, :],
        segments[:, None],
        gains,
    ]
    pairs = token_rows * SEQ_LEN * HQ
    if grad_out is None:
        out_specs = pl.BlockSpec((SEQ_LEN, wide), lambda s, h: (s, h))
        out_shape = jax.ShapeDtypeStruct((token_rows, HQ * HD), jnp.bfloat16)
    else:
        columns = projected.shape[1]
        in_specs.append(pl.BlockSpec((SEQ_LEN, wide), lambda s, h: (s, h)))
        operands.append(grad_out)
        out_specs = [
            pl.BlockSpec((SEQ_LEN, columns), full),
            pl.BlockSpec((2, HD), lambda s, h: (0, 0)),
        ]
        out_shape = [
            jax.ShapeDtypeStruct((token_rows, columns), jnp.bfloat16),
            jax.ShapeDtypeStruct((2, HD), jnp.float32),
        ]
    return pl.pallas_call(
        body,
        grid=(seq_count, HK),
        in_specs=in_specs,
        out_specs=out_specs,
        out_shape=out_shape,
        compiler_params=pltpu.CompilerParams(vmem_limit_bytes=48 * 1024 * 1024),
        cost_estimate=pl.CostEstimate(
            flops=(4 if grad_out is None else 10) * pairs * HD * 2,
            bytes_accessed=projected.size * 6,
            transcendentals=pairs,
        ),
    )(*operands)


def on_device(
    tokens,
    segment_ids,
    positions,
    cotangent,
    qkv_weight,
    out_weight,
    gate_up_weight,
    down_weight,
    norm_gains,
    head_gains,
    qkv_moments,
    out_moments,
    gate_up_moments,
    down_moments,
    norm_moments,
    head_moments,
):
    width = norm_gains.shape[1]
    gains_low = jnp.concatenate([norm_gains, head_gains], axis=1).astype(jnp.bfloat16)
    owners = lax.axis_size("group")
    gains_all = gather_small(gains_low).reshape(2, owners, -1)
    full_norm = gains_all[:, :, :width].reshape(2, -1)
    full_head = gains_all[:, :, width:].reshape(2, -1)
    full_qkv, order = gather_rows(qkv_weight.astype(jnp.bfloat16), 2, None)
    full_out, order = gather_rows(out_weight.astype(jnp.bfloat16), 1, order)
    full_gate_up, order = gather_rows(gate_up_weight.astype(jnp.bfloat16), 2, order)
    full_down, order = gather_rows(down_weight.astype(jnp.bfloat16), 1, order)
    gain_one = full_norm[0].astype(jnp.float32)
    gain_two = full_norm[1].astype(jnp.float32)
    head_gain = full_head.astype(jnp.float32)
    inputs = tokens.astype(jnp.float32)
    root_one = lax.rsqrt(jnp.mean(inputs * inputs, axis=-1, keepdims=True) + EPS_NORM)
    normed_one = inputs * root_one
    hidden_one = (normed_one * gain_one).astype(jnp.bfloat16)
    projected = jnp.dot(hidden_one, full_qkv, preferred_element_type=jnp.float32)
    tables = rotary_tables(positions, HD)
    mixed_low = attention_call(attend_body, projected, tables, segment_ids, head_gain, None)
    attended = jnp.dot(mixed_low, full_out, preferred_element_type=jnp.float32)
    residual = inputs + attended
    root_two = lax.rsqrt(jnp.mean(residual * residual, axis=-1, keepdims=True) + EPS_NORM)
    normed_two = residual * root_two
    hidden_two = (normed_two * gain_two).astype(jnp.bfloat16)
    gate_up = jnp.dot(hidden_two, full_gate_up, preferred_element_type=jnp.float32)
    gate_part = gate_up[:, :FF]
    upward = gate_up[:, FF:]
    sigmoid_gate = jax.nn.sigmoid(gate_part)
    activated = (gate_part * sigmoid_gate * upward).astype(jnp.bfloat16)
    branch = jnp.dot(activated, full_down, preferred_element_type=jnp.float32)
    output = (residual + branch).astype(jnp.bfloat16)
    upstream = cotangent.astype(jnp.float32)
    down_sum = GradSum(activated, cotangent)
    grad_act = contract_cols(after(cotangent, *down_sum.blocks), full_down)
    grad_gate = grad_act * upward * sigmoid_gate * (1.0 + gate_part * (1.0 - sigmoid_gate))
    grad_up = grad_act * gate_part * sigmoid_gate
    grad_gate_up = jnp.concatenate([grad_gate, grad_up], axis=-1).astype(jnp.bfloat16)
    gate_up_sum = GradSum(hidden_two, after(grad_gate_up, *down_sum.advance()))
    grad_hidden_two = contract_cols(after(grad_gate_up, *gate_up_sum.blocks), full_gate_up)
    grad_gain_two = jnp.sum(grad_hidden_two * normed_two, axis=0)
    grad_residual = upstream + norm_back(grad_hidden_two, normed_two, root_two, gain_two)
    residual_low = grad_residual.astype(jnp.bfloat16)
    out_sum = GradSum(mixed_low, after(residual_low, *gate_up_sum.advance()))
    grad_mixed = contract_cols(after(residual_low, *out_sum.blocks), full_out).astype(
        jnp.bfloat16
    )
    grad_mixed = after(grad_mixed, *down_sum.advance(), *out_sum.advance())
    grad_projected, grad_gain_head = attention_call(
        attend_back_body, projected, tables, segment_ids, head_gain, grad_mixed
    )
    qkv_sum = GradSum(hidden_one, grad_projected)
    grad_hidden_one = contract_cols(after(grad_projected, *qkv_sum.blocks), full_qkv)
    grad_gain_one = jnp.sum(grad_hidden_one * normed_one, axis=0)
    grad_inputs = grad_residual + norm_back(grad_hidden_one, normed_one, root_one, gain_one)
    tokens_grad = grad_inputs.astype(jnp.bfloat16)
    small = jnp.concatenate(
        [jnp.stack([grad_gain_one, grad_gain_two]), grad_gain_head],
        axis=1,
    )
    small = sum_all(small)
    norm_total = small[:, :-HD]
    head_total = small[:, -HD:]
    owned = tuple(v.finish() for v in (qkv_sum, out_sum, gate_up_sum, down_sum))
    squares = sum_all(sum(jnp.sum(v * v) for v in owned).reshape(1, 1))[0, 0]
    squares = squares + jnp.sum(small * small)
    clip_limit = math.sqrt(PARAMS)
    factor = clip_limit / jnp.maximum(jnp.sqrt(squares), clip_limit)
    gathered = [gather_grad(v) for v in owned]
    masters = (qkv_weight, out_weight, gate_up_weight, down_weight)
    moments = (qkv_moments, out_moments, gate_up_moments, down_moments)
    renewed = [
        adam_blocks(master, moment, blocks, factor, LEARN_RATE, WEIGHT_DECAY)
        for master, moment, blocks in zip(masters, moments, gathered)
    ]
    mine = lax.axis_index("group")
    norm_grad = lax.dynamic_slice_in_dim(
        norm_total, mine * norm_gains.shape[1], norm_gains.shape[1], 1
    )
    head_grad = lax.dynamic_slice_in_dim(
        head_total, mine * head_gains.shape[1], head_gains.shape[1], 1
    )
    renewed.append(adam_update(norm_gains, norm_moments, norm_grad, factor, GAIN_RATE, 0.0))
    renewed.append(adam_update(head_gains, head_moments, head_grad, factor, GAIN_RATE, 0.0))
    return (
        output,
        tokens_grad,
        *owned,
        norm_grad,
        head_grad,
        *[new for new, _ in renewed],
        *[state for _, state in renewed],
    )


def solution(mesh):
    placed = (
        P(("dp", "group"), None),
        P(("dp", "group")),
        P(("dp", "group")),
        P(("dp", "group"), None),
        P("group", None),
        P("group", None),
        P("group", None),
        P("group", None),
        P(None, "group"),
        P(None, "group"),
        P(None, "group", None),
        P(None, "group", None),
        P(None, "group", None),
        P(None, "group", None),
        P(None, None, "group"),
        P(None, None, "group"),
    )
    return jax.shard_map(
        on_device,
        mesh=mesh,
        in_specs=placed,
        out_specs=(
            P(("dp", "group"), None),
            P(("dp", "group"), None),
            P("group", "dp"),
            P("group", "dp"),
            P("group", "dp"),
            P("group", "dp"),
            P(None, "group"),
            P(None, "group"),
            P("group", None),
            P("group", None),
            P("group", None),
            P("group", None),
            P(None, "group"),
            P(None, "group"),
            P(None, "group", None),
            P(None, "group", None),
            P(None, "group", None),
            P(None, "group", None),
            P(None, None, "group"),
            P(None, None, "group"),
        ),
        check_vma=False,
    )
```

```python
import math

import jax
import jax.numpy as jnp
from jax import lax
from jax.experimental import pallas as pl
from jax.experimental.pallas import tpu as pltpu
from jax.sharding import PartitionSpec as P


HQ = 16
HK = 8
HD = 128
FF = 3072
SEQ_LEN = 512
PARAMS = 15730944


EPS_NORM = 1e-06
ROPE_BASE = 1000000.0
MASKED = -1e30
LEARN_RATE = 0.03
GAIN_RATE = 0.3
WEIGHT_DECAY = 0.1
BETA_ONE = 0.9
BETA_TWO = 0.95
ADAM_EPS = 1e-08
STEP_COUNT = 3.0


def rotary_tables(places, width):
    half_width = width // 2
    frequency = ROPE_BASE ** (-(jnp.arange(half_width, dtype=jnp.float32) * 2.0) / width)
    angles = places.astype(jnp.float32)[:, None] * frequency[None, :]
    cosine, sine = jnp.cos(angles), jnp.sin(angles)
    return (
        jnp.concatenate([cosine, cosine], axis=1),
        jnp.concatenate([-sine, sine], axis=1),
    )


def contract_rows(left_side, right_side):
    return lax.dot_general(
        left_side, right_side, (((0,), (0,)), ((), ())), preferred_element_type=jnp.float32
    )


def contract_cols(left_side, right_side):
    return lax.dot_general(
        left_side, right_side, (((1,), (1,)), ((), ())), preferred_element_type=jnp.float32
    )


def norm_back(grad_out, normed, inv_root, gain):
    scaled = grad_out * gain
    return inv_root * (scaled - normed * jnp.mean(normed * scaled, axis=-1, keepdims=True))


def swap(value, axis, mask):
    count = lax.axis_size(axis)
    return lax.ppermute(value, axis, [(i, i ^ mask) for i in range(count)])


def bit_masks(count):
    return [1 << i for i in range(count.bit_length() - 1)]


def after(value, *others):
    return lax.optimization_barrier((value, others))[0]


def gather_rows(shard, previous):
    owners = lax.axis_size("group")
    copies = lax.axis_size("dp")
    mine = lax.axis_index("group")
    here = lax.axis_index("dp")
    if previous is not None:
        shard = after(shard, previous)
    shard = shard.astype(jnp.bfloat16)
    rows, columns = shard.shape
    pieces = [(shard, 0, 0)]
    order = shard
    if owners == 4 and copies % 4 == 0 and rows % 128 == 0:
        quarter, half = rows // 4, rows // 8
        place = (here & 1) * 2 + ((here >> 1) & 1)
        order = swap(
            lax.dynamic_slice_in_dim(shard, place * quarter, quarter, 0), "group", 2
        )
        by_one = swap(order, "dp", 1)
        by_two = swap(order, "dp", 2)
        last = (place ^ 3) * quarter
        pieces += [
            (order, 2, place * quarter),
            (by_one, 2, (place ^ 2) * quarter),
            (by_two, 2, (place ^ 1) * quarter),
            (swap(by_two[:half], "dp", 1), 2, last),
            (swap(by_one[half:], "dp", 2), 2, last + half),
        ]
    else:
        for mask in bit_masks(owners)[1:]:
            pieces += [(swap(v, "group", mask), dg ^ mask, off) for v, dg, off in pieces]
    pieces += [(swap(v, "group", 1), dg ^ 1, off) for v, dg, off in pieces]
    full = jnp.zeros((rows * owners, columns), shard.dtype)
    for value, delta, offset in pieces:
        start = (mine ^ delta) * rows + offset
        full = lax.dynamic_update_slice(full, value, (start, 0))
    return full, order


def gather_small(shard):
    owners = lax.axis_size("group")
    mine = lax.axis_index("group")
    width = shard.shape[1]
    held = shard[None]
    deltas = [0]
    for mask in reversed(bit_masks(owners)):
        held = jnp.concatenate([held, swap(held, "group", mask)], axis=0)
        deltas += [d ^ mask for d in deltas]
    full = jnp.zeros((shard.shape[0], width * owners), shard.dtype)
    for k, delta in enumerate(deltas):
        full = lax.dynamic_update_slice(full, held[k], (0, (mine ^ delta) * width))
    return full


def sum_all(value):
    owners = lax.axis_size("group")
    copies = lax.axis_size("dp")
    mesh_type = pl.DeviceIdType.MESH

    def body(in_ref, out_ref, near, near_sum, far, near_send, near_recv, far_send, far_recv):
        mine = lax.axis_index("group")
        here = lax.axis_index("dp")
        near_peers = [(here, mine ^ k) for k in range(1, owners)]
        far_peers = [(here ^ k, mine) for k in range(1, copies)]
        barrier = pltpu.get_barrier_semaphore()
        for peer in near_peers + far_peers:
            pl.semaphore_signal(barrier, inc=1, device_id=peer, device_id_type=mesh_type)
        pl.semaphore_wait(barrier, len(near_peers) + len(far_peers))

        def exchange(source, slots, index, peers, sends, recvs):
            slots[index] = source[...]
            copies_out = [
                pltpu.make_async_remote_copy(
                    src_ref=source,
                    dst_ref=slots.at[index],
                    send_sem=sends.at[k],
                    recv_sem=recvs.at[k],
                    device_id=peer,
                    device_id_type=mesh_type,
                )
                for k, peer in enumerate(peers)
            ]
            for copy in copies_out:
                copy.start()
            for copy in copies_out:
                copy.wait()
            total = slots[0]
            for k in range(1, len(peers) + 1):
                total = total + slots[k]
            return total

        near_sum[...] = exchange(in_ref, near, mine, near_peers, near_send, near_recv)
        out_ref[...] = exchange(near_sum, far, here, far_peers, far_send, far_recv)

    shape = value.shape
    return pl.pallas_call(
        body,
        out_shape=jax.ShapeDtypeStruct(shape, jnp.float32),
        in_specs=[pl.BlockSpec(memory_space=pltpu.VMEM)],
        out_specs=pl.BlockSpec(memory_space=pltpu.VMEM),
        scratch_shapes=[
            pltpu.VMEM((owners,) + shape, jnp.float32),
            pltpu.VMEM(shape, jnp.float32),
            pltpu.VMEM((copies,) + shape, jnp.float32),
            pltpu.SemaphoreType.DMA((owners - 1,)),
            pltpu.SemaphoreType.DMA((owners - 1,)),
            pltpu.SemaphoreType.DMA((copies - 1,)),
            pltpu.SemaphoreType.DMA((copies - 1,)),
        ],
        compiler_params=pltpu.CompilerParams(collective_id=0, has_side_effects=True),
    )(value)


def spread_bits(position, masks):
    total = 0
    count = len(masks)
    for i, mask in enumerate(masks):
        total = total + ((position >> (count - 1 - i)) & 1) * mask
    return total


def grad_blocks(left, right):
    tokens, rows = left.shape
    columns = right.shape[1]
    owners = lax.axis_size("group")
    copies = lax.axis_size("dp")
    column_masks = bit_masks(copies)
    later = bit_masks(owners)[1:]
    staying = [spread_bits(p, later) for p in range(1 << len(later))]
    row_sets = [[dg + 1 for dg in staying], staying] if owners > 1 else [[0]]
    row_block = rows // owners
    column_block = columns // copies
    mine = lax.axis_index("group")
    here = lax.axis_index("dp")
    if column_block % 128 or row_block % 16:
        ordered = jnp.concatenate(
            [
                lax.dynamic_slice_in_dim(
                    right, (here ^ spread_bits(p, column_masks)) * column_block, column_block, 1
                )
                for p in range(copies)
            ],
            axis=1,
        )
        return [
            jnp.stack(
                [
                    contract_rows(
                        lax.dynamic_slice_in_dim(left, (mine ^ dg) * row_block, row_block, 1),
                        ordered,
                    ).astype(jnp.bfloat16)
                    for dg in row_set
                ]
            )
            for row_set in row_sets
        ]
    wide = 2 if column_block % 256 and copies % 2 == 0 else 1

    def body(where, left_ref, *rest):
        rights, outs, turned = rest[:wide], rest[wide:-1], rest[-1]

        @pl.when(pl.program_id(0) == 0)
        def _():
            turned[...] = left_ref[...].T

        block = jnp.concatenate([ref[...] for ref in rights], axis=1)
        for out, row_set in zip(outs, row_sets):
            for k, dg in enumerate(row_set):
                start = pl.multiple_of((where[0] ^ dg) * row_block, row_block)
                out[k] = jnp.dot(
                    turned[pl.ds(start, row_block), :],
                    block,
                    preferred_element_type=jnp.float32,
                ).astype(jnp.bfloat16)

    def right_spec(j):
        return pl.BlockSpec(
            (tokens, column_block),
            lambda p, where: (0, where[1] ^ spread_bits(p * wide + j, column_masks)),
        )

    return pl.pallas_call(
        body,
        out_shape=[
            jax.ShapeDtypeStruct((len(row_set), row_block, columns), jnp.bfloat16)
            for row_set in row_sets
        ],
        grid_spec=pltpu.PrefetchScalarGridSpec(
            num_scalar_prefetch=1,
            grid=(copies // wide,),
            in_specs=[pl.BlockSpec((tokens, rows), lambda p, where: (0, 0))]
            + [right_spec(j) for j in range(wide)],
            out_specs=[
                pl.BlockSpec(
                    (len(row_set), row_block, column_block * wide), lambda p, where: (0, 0, p)
                )
                for row_set in row_sets
            ],
            scratch_shapes=[pltpu.VMEM((rows, tokens), jnp.bfloat16)],
        ),
        compiler_params=pltpu.CompilerParams(vmem_limit_bytes=48 * 1024 * 1024),
        cost_estimate=pl.CostEstimate(
            flops=2 * tokens * rows * columns,
            bytes_accessed=2 * (tokens * rows + tokens * columns + rows * columns),
            transcendentals=0,
        ),
    )(jnp.stack([mine, here]).astype(jnp.int32), left, *[right] * wide)


class GradSum:
    def __init__(self, left, right, split):
        blocks = grad_blocks(left, right)
        self.blocks = blocks
        group = [("group", m) for m in bit_masks(lax.axis_size("group"))]
        other = [("dp", m) for m in bit_masks(lax.axis_size("dp"))]
        held = [blocks[-1]]
        if group:
            held.append(swap(blocks[0], "group", 1))
        rest = group[1:]
        self.orders = [rest + other]
        if split:
            self.orders.append(other[:1] + rest + other[1:])
        count = len(self.orders)
        size = blocks[-1].shape[1] // count
        self.parts = [[v[:, i * size : (i + 1) * size] for v in held] for i in range(count)]
        self.common = len(rest) + 1
        self.length = len(rest) + len(other)
        self.step = 0

    def hold(self, *others):
        self.parts = [[after(v, *others) for v in part] for part in self.parts]

    def advance(self):
        sent = []
        if self.step == self.length:
            return sent
        exchange = []
        for i, order in enumerate(self.orders):
            axis, mask = order[self.step]
            dim = 0 if axis == "group" else 2
            size = self.parts[i][0].shape[dim] // 2
            away = sum(
                lax.slice_in_dim(v, size, 2 * size, axis=dim).astype(jnp.float32)
                for v in self.parts[i]
            ).astype(jnp.bfloat16)
            self.parts[i] = [lax.slice_in_dim(v, 0, size, axis=dim) for v in self.parts[i]]
            exchange.append((away, axis, mask))
        if self.step >= self.common:
            rows = exchange[0][0].shape[1]
            away = jnp.concatenate([v for v, _, _ in exchange], axis=1)
            got = swap(away, *exchange[0][1:])
            for i, part in enumerate(self.parts):
                part.append(got[:, i * rows : (i + 1) * rows])
            sent.append(away)
        else:
            for i, (away, axis, mask) in enumerate(exchange):
                self.parts[i].append(swap(away, axis, mask))
                sent.append(away)
        self.step += 1
        return sent

    def finish(self):
        while self.step < self.length:
            self.advance()
        return jnp.concatenate(
            [sum(v[0].astype(jnp.float32) for v in part) for part in self.parts], axis=0
        )


def gather_grad(own):
    held = own.astype(jnp.bfloat16)[None]
    deltas = [0]
    groups = [(held, deltas)]
    masks = list(reversed(bit_masks(lax.axis_size("dp"))))
    for i, mask in enumerate(masks):
        got = swap(held, "dp", mask)
        got_deltas = [d ^ mask for d in deltas]
        if i + 1 < len(masks):
            held = jnp.concatenate([held, got], axis=0)
            deltas = deltas + got_deltas
            groups = [(held, deltas)]
        else:
            groups.append((got, got_deltas))
    return groups


def adam_core(master, first_moment, second_moment, clipped, step_rate, decay_rate):
    first_new = BETA_ONE * first_moment + (1.0 - BETA_ONE) * clipped
    second_new = BETA_TWO * second_moment + (1.0 - BETA_TWO) * clipped * clipped
    first_hat = first_new * (1.0 / (1.0 - BETA_ONE**STEP_COUNT))
    second_hat = second_new * (1.0 / (1.0 - BETA_TWO**STEP_COUNT))
    renewed = master - step_rate * (
        first_hat / (jnp.sqrt(second_hat) + ADAM_EPS) + decay_rate * master
    )
    return renewed, first_new, second_new


def adam_blocks(master, moment, blocks, factor, step_rate, decay_rate):
    rows, columns = master.shape
    copies = lax.axis_size("dp")
    here = lax.axis_index("dp")
    width = columns // copies
    if width % 128:
        full = jnp.zeros(master.shape, jnp.float32)
        for value, deltas in blocks:
            for k, dd in enumerate(deltas):
                full = lax.dynamic_update_slice(
                    full, value[k].astype(jnp.float32), (0, (here ^ dd) * width)
                )
        return adam_update(master, moment, full, factor, step_rate, decay_rate)
    tile = rows
    while tile % 32 == 0 and tile * columns > 256 * 1024:
        tile //= 2

    def body(where, factor_ref, master_ref, moment_ref, *rest):
        grads, (new_ref, state_ref) = rest[:-2], rest[-2:]
        scale = factor_ref[0, 0]
        for grad, (_, deltas) in zip(grads, blocks):
            for k, dd in enumerate(deltas):
                at = pl.ds(pl.multiple_of((where[0] ^ dd) * width, 128), width)
                renewed, first_new, second_new = adam_core(
                    master_ref[:, at],
                    moment_ref[0, :, at],
                    moment_ref[1, :, at],
                    grad[k].astype(jnp.float32) * scale,
                    step_rate,
                    decay_rate,
                )
                new_ref[:, at] = renewed
                state_ref[0, :, at] = first_new
                state_ref[1, :, at] = second_new

    return pl.pallas_call(
        body,
        out_shape=[
            jax.ShapeDtypeStruct(master.shape, jnp.float32),
            jax.ShapeDtypeStruct(moment.shape, jnp.float32),
        ],
        grid_spec=pltpu.PrefetchScalarGridSpec(
            num_scalar_prefetch=1,
            grid=(rows // tile,),
            in_specs=[
                pl.BlockSpec(memory_space=pltpu.SMEM),
                pl.BlockSpec((tile, columns), lambda i, where: (i, 0)),
                pl.BlockSpec((2, tile, columns), lambda i, where: (0, i, 0)),
            ]
            + [
                pl.BlockSpec((len(deltas), tile, width), lambda i, where: (0, i, 0))
                for _, deltas in blocks
            ],
            out_specs=[
                pl.BlockSpec((tile, columns), lambda i, where: (i, 0)),
                pl.BlockSpec((2, tile, columns), lambda i, where: (0, i, 0)),
            ],
        ),
        compiler_params=pltpu.CompilerParams(vmem_limit_bytes=48 * 1024 * 1024),
        cost_estimate=pl.CostEstimate(
            flops=20 * rows * columns,
            bytes_accessed=26 * rows * columns,
            transcendentals=rows * columns,
        ),
    )(
        here.reshape(1).astype(jnp.int32),
        factor.reshape(1, 1),
        master,
        moment,
        *[value for value, _ in blocks],
    )


def adam_update(master, moment, gradient, factor, step_rate, decay_rate):
    clipped = gradient * factor
    first_moment = BETA_ONE * moment[0] + (1.0 - BETA_ONE) * clipped
    second = BETA_TWO * moment[1] + (1.0 - BETA_TWO) * clipped * clipped
    first_hat = first_moment / (1.0 - BETA_ONE**STEP_COUNT)
    second_hat = second / (1.0 - BETA_TWO**STEP_COUNT)
    renewed = master - step_rate * (
        first_hat / (jnp.sqrt(second_hat) + ADAM_EPS) + decay_rate * master
    )
    return (renewed, jnp.stack([first_moment, second]))


def head_forward(raw, gain, cosine, sine):
    root = lax.rsqrt(jnp.mean(raw * raw, axis=-1, keepdims=True) + EPS_NORM)
    normed = raw * root
    scaled = normed * gain
    turned = scaled * cosine + pltpu.roll(scaled, HD // 2, 1) * sine
    return turned.astype(jnp.bfloat16), normed, root


def head_backward(grad, normed, root, gain, cosine, sine):
    turned = grad * cosine - pltpu.roll(grad, HD // 2, 1) * sine
    grad_gain = jnp.sum(turned * normed, axis=0, keepdims=True)
    scaled = turned * gain
    raw = root * (scaled - normed * jnp.mean(normed * scaled, axis=-1, keepdims=True))
    return raw, grad_gain


SPAN = 256


def span_weights(query_low, key_low, seg_row_ref, seg_col_ref, start):
    stop = start + SPAN
    scores = lax.dot_general(
        key_low[:stop],
        query_low[start:stop],
        (((1,), (1,)), ((), ())),
        preferred_element_type=jnp.float32,
    ) * (1.0 / math.sqrt(HD))
    key_at = lax.broadcasted_iota(jnp.int32, (stop, SPAN), 0)
    query_at = lax.broadcasted_iota(jnp.int32, (stop, SPAN), 1) + start
    allowed = (key_at <= query_at) & (seg_col_ref[:stop, :] == seg_row_ref[:, start:stop])
    scores = jnp.where(allowed, scores, MASKED)
    raised = jnp.exp(scores - jnp.max(scores, axis=0, keepdims=True))
    return raised * (1.0 / jnp.sum(raised, axis=0, keepdims=True))


def attend_body(
    query_ref, key_ref, value_ref, cos_ref, sin_ref, row_ref, col_ref, gain_ref, out_ref
):
    cosine, sine = cos_ref[...], sin_ref[...]
    key_low, _, _ = head_forward(key_ref[...], gain_ref[1:2, :], cosine, sine)
    value_turned = value_ref[...].astype(jnp.bfloat16).T
    for g in range(HQ // HK):
        at = slice(g * HD, (g + 1) * HD)
        query_low, _, _ = head_forward(query_ref[:, at], gain_ref[0:1, :], cosine, sine)
        for start in range(0, SEQ_LEN, SPAN):
            stop = start + SPAN
            weights = span_weights(query_low, key_low, row_ref, col_ref, start)
            mixed = jnp.dot(
                value_turned[:, :stop],
                weights.astype(jnp.bfloat16),
                preferred_element_type=jnp.float32,
            )
            out_ref[start:stop, at] = mixed.T.astype(jnp.bfloat16)


def attend_back_body(
    query_ref, key_ref, value_ref, cos_ref, sin_ref, row_ref, col_ref, gain_ref, grad_ref,
    out_ref, gain_out_ref,
):
    head = pl.program_id(1)
    cosine, sine = cos_ref[...], sin_ref[...]
    inv_head = 1.0 / math.sqrt(HD)

    @pl.when((pl.program_id(0) == 0) & (head == 0))
    def _():
        gain_out_ref[...] = jnp.zeros_like(gain_out_ref)

    key_low, key_normed, key_root = head_forward(key_ref[...], gain_ref[1:2, :], cosine, sine)
    value_low = value_ref[...].astype(jnp.bfloat16)
    key_turned = key_low.T
    grad_key = [jnp.zeros((SPAN, HD), jnp.float32)] * (SEQ_LEN // SPAN)
    grad_value = list(grad_key)
    gain_query = jnp.zeros((1, HD), jnp.float32)
    for g in range(HQ // HK):
        at = slice(g * HD, (g + 1) * HD)
        query_low, normed, root = head_forward(query_ref[:, at], gain_ref[0:1, :], cosine, sine)
        grad_query = []
        for start in range(0, SEQ_LEN, SPAN):
            stop = start + SPAN
            weights = span_weights(query_low, key_low, row_ref, col_ref, start)
            grad_out = grad_ref[start:stop, at]
            grad_weights = lax.dot_general(
                value_low[:stop],
                grad_out,
                (((1,), (1,)), ((), ())),
                preferred_element_type=jnp.float32,
            )
            more_value = jnp.dot(
                weights.astype(jnp.bfloat16), grad_out, preferred_element_type=jnp.float32
            )
            product = weights * grad_weights
            grad_scores = (
                weights * (grad_weights - jnp.sum(product, axis=0, keepdims=True))
            ).astype(jnp.bfloat16)
            more_key = jnp.dot(
                grad_scores, query_low[start:stop], preferred_element_type=jnp.float32
            )
            grad_query.append(
                jnp.dot(
                    key_turned[:, :stop], grad_scores, preferred_element_type=jnp.float32
                ).T
            )
            for j in range(stop // SPAN):
                part = slice(j * SPAN, (j + 1) * SPAN)
                grad_key[j] = grad_key[j] + more_key[part]
                grad_value[j] = grad_value[j] + more_value[part]
        raw, more_gain = head_backward(
            jnp.concatenate(grad_query, axis=0) * inv_head,
            normed,
            root,
            gain_ref[0:1, :],
            cosine,
            sine,
        )
        gain_query = gain_query + more_gain
        place = pl.multiple_of((head * (HQ // HK) + g) * HD, HD)
        out_ref[:, pl.ds(place, HD)] = raw.astype(jnp.bfloat16)
    raw, gain_key = head_backward(
        jnp.concatenate(grad_key, axis=0) * inv_head,
        key_normed,
        key_root,
        gain_ref[1:2, :],
        cosine,
        sine,
    )
    out_ref[:, pl.ds(pl.multiple_of((HQ + head) * HD, HD), HD)] = raw.astype(jnp.bfloat16)
    out_ref[:, pl.ds(pl.multiple_of((HQ + HK + head) * HD, HD), HD)] = jnp.concatenate(
        grad_value, axis=0
    ).astype(jnp.bfloat16)
    gain_out_ref[0:1, :] += gain_query
    gain_out_ref[1:2, :] += gain_key


def attention_call(body, projected, tables, segments, gains, grad_out):
    token_rows = projected.shape[0]
    seq_count = token_rows // SEQ_LEN
    groups = HQ // HK
    wide = groups * HD
    full = lambda s, h: (s, 0)
    in_specs = [
        pl.BlockSpec((SEQ_LEN, wide), lambda s, h: (s, h)),
        pl.BlockSpec((SEQ_LEN, HD), lambda s, h: (s, HQ + h)),
        pl.BlockSpec((SEQ_LEN, HD), lambda s, h: (s, HQ + HK + h)),
        pl.BlockSpec((SEQ_LEN, HD), full),
        pl.BlockSpec((SEQ_LEN, HD), full),
        pl.BlockSpec((1, SEQ_LEN), lambda s, h: (0, s)),
        pl.BlockSpec((SEQ_LEN, 1), full),
        pl.BlockSpec((2, HD), lambda s, h: (0, 0)),
    ]
    operands = [
        projected,
        projected,
        projected,
        *tables,
        segments[None, :],
        segments[:, None],
        gains,
    ]
    pairs = token_rows * SEQ_LEN * HQ
    if grad_out is None:
        out_specs = pl.BlockSpec((SEQ_LEN, wide), lambda s, h: (s, h))
        out_shape = jax.ShapeDtypeStruct((token_rows, HQ * HD), jnp.bfloat16)
    else:
        columns = projected.shape[1]
        in_specs.append(pl.BlockSpec((SEQ_LEN, wide), lambda s, h: (s, h)))
        operands.append(grad_out)
        out_specs = [
            pl.BlockSpec((SEQ_LEN, columns), full),
            pl.BlockSpec((2, HD), lambda s, h: (0, 0)),
        ]
        out_shape = [
            jax.ShapeDtypeStruct((token_rows, columns), jnp.bfloat16),
            jax.ShapeDtypeStruct((2, HD), jnp.float32),
        ]
    return pl.pallas_call(
        body,
        grid=(seq_count, HK),
        in_specs=in_specs,
        out_specs=out_specs,
        out_shape=out_shape,
        compiler_params=pltpu.CompilerParams(vmem_limit_bytes=48 * 1024 * 1024),
        cost_estimate=pl.CostEstimate(
            flops=(4 if grad_out is None else 10) * pairs * HD * 2,
            bytes_accessed=projected.size * 6,
            transcendentals=pairs,
        ),
    )(*operands)


def on_device(
    tokens,
    segment_ids,
    positions,
    cotangent,
    qkv_weight,
    out_weight,
    gate_up_weight,
    down_weight,
    norm_gains,
    head_gains,
    qkv_moments,
    out_moments,
    gate_up_moments,
    down_moments,
    norm_moments,
    head_moments,
):
    width = norm_gains.shape[1]
    gains_low = jnp.concatenate([norm_gains, head_gains], axis=1).astype(jnp.bfloat16)
    owners = lax.axis_size("group")
    gains_all = gather_small(gains_low).reshape(2, owners, -1)
    full_norm = gains_all[:, :, :width].reshape(2, -1)
    full_head = gains_all[:, :, width:].reshape(2, -1)
    full_qkv, order = gather_rows(qkv_weight, None)
    full_out, order = gather_rows(out_weight, order)
    full_gate_up, order = gather_rows(gate_up_weight, order)
    gain_one = full_norm[0].astype(jnp.float32)
    gain_two = full_norm[1].astype(jnp.float32)
    head_gain = full_head.astype(jnp.float32)
    inputs = tokens.astype(jnp.float32)
    root_one = lax.rsqrt(jnp.mean(inputs * inputs, axis=-1, keepdims=True) + EPS_NORM)
    normed_one = inputs * root_one
    hidden_one = (normed_one * gain_one).astype(jnp.bfloat16)
    projected = jnp.dot(hidden_one, full_qkv, preferred_element_type=jnp.float32)
    full_down, _ = gather_rows(down_weight, (order, projected))
    tables = rotary_tables(positions, HD)
    mixed_low = attention_call(attend_body, projected, tables, segment_ids, head_gain, None)
    attended = jnp.dot(mixed_low, full_out, preferred_element_type=jnp.float32)
    residual = inputs + attended
    root_two = lax.rsqrt(jnp.mean(residual * residual, axis=-1, keepdims=True) + EPS_NORM)
    normed_two = residual * root_two
    hidden_two = (normed_two * gain_two).astype(jnp.bfloat16)
    gate_up = jnp.dot(hidden_two, full_gate_up, preferred_element_type=jnp.float32)
    gate_part = gate_up[:, :FF]
    upward = gate_up[:, FF:]
    sigmoid_gate = jax.nn.sigmoid(gate_part)
    activated = (gate_part * sigmoid_gate * upward).astype(jnp.bfloat16)
    branch = jnp.dot(activated, full_down, preferred_element_type=jnp.float32)
    output = (residual + branch).astype(jnp.bfloat16)
    upstream = cotangent.astype(jnp.float32)
    down_sum = GradSum(activated, cotangent, False)
    grad_act = contract_cols(after(cotangent, *down_sum.blocks), full_down)
    grad_gate = grad_act * upward * sigmoid_gate * (1.0 + gate_part * (1.0 - sigmoid_gate))
    grad_up = grad_act * gate_part * sigmoid_gate
    grad_gate_up = jnp.concatenate([grad_gate, grad_up], axis=-1).astype(jnp.bfloat16)
    gate_up_sum = GradSum(hidden_two, after(grad_gate_up, *down_sum.advance()), True)
    grad_hidden_two = contract_cols(after(grad_gate_up, *gate_up_sum.blocks), full_gate_up)
    grad_gain_two = jnp.sum(grad_hidden_two * normed_two, axis=0)
    grad_residual = upstream + norm_back(grad_hidden_two, normed_two, root_two, gain_two)
    residual_low = grad_residual.astype(jnp.bfloat16)
    out_sum = GradSum(mixed_low, after(residual_low, *gate_up_sum.advance()), False)
    grad_mixed = contract_cols(after(residual_low, *out_sum.blocks), full_out).astype(
        jnp.bfloat16
    )
    down_sum.hold(out_sum.blocks)
    grad_mixed = after(grad_mixed, *down_sum.advance(), *out_sum.advance())
    grad_projected, grad_gain_head = attention_call(
        attend_back_body, projected, tables, segment_ids, head_gain, grad_mixed
    )
    gate_up_sum.hold(grad_projected)
    down_sum.hold(grad_projected)
    sent = gate_up_sum.advance() + down_sum.advance()
    qkv_sum = GradSum(hidden_one, after(grad_projected, *sent), True)
    sent = qkv_sum.advance()
    out_sum.hold(sent)
    gate_up_sum.hold(sent)
    sent = sent + out_sum.advance()
    grad_hidden_one = contract_cols(after(grad_projected, *qkv_sum.blocks, *sent), full_qkv)
    grad_gain_one = jnp.sum(grad_hidden_one * normed_one, axis=0)
    grad_inputs = grad_residual + norm_back(grad_hidden_one, normed_one, root_one, gain_one)
    tokens_grad = grad_inputs.astype(jnp.bfloat16)
    down_sum.hold(sent)
    small = jnp.concatenate(
        [jnp.stack([grad_gain_one, grad_gain_two]), grad_gain_head],
        axis=1,
    )
    sent = qkv_sum.advance()
    owned = tuple(v.finish() for v in (qkv_sum, out_sum, gate_up_sum, down_sum))
    local = sum(jnp.sum(v * v) for v in owned)
    summed = sum_all(
        jnp.concatenate(
            [small, jnp.full((6, small.shape[1]), local, jnp.float32)], axis=0
        )
    )
    small = summed[:2]
    norm_total = small[:, :-HD]
    head_total = small[:, -HD:]
    squares = summed[2, 0] + jnp.sum(small * small)
    clip_limit = math.sqrt(PARAMS)
    factor = clip_limit / jnp.maximum(jnp.sqrt(squares), clip_limit)
    gathered = [gather_grad(after(v, *sent)) for v in owned]
    masters = (qkv_weight, out_weight, gate_up_weight, down_weight)
    moments = (qkv_moments, out_moments, gate_up_moments, down_moments)
    later = after(factor, gathered[0][0][0])
    renewed = [
        adam_blocks(master, moment, blocks, scale, LEARN_RATE, WEIGHT_DECAY)
        for master, moment, blocks, scale in zip(
            masters, moments, gathered, (later, factor, later, later)
        )
    ]
    mine = lax.axis_index("group")
    norm_grad = lax.dynamic_slice_in_dim(
        norm_total, mine * norm_gains.shape[1], norm_gains.shape[1], 1
    )
    head_grad = lax.dynamic_slice_in_dim(
        head_total, mine * head_gains.shape[1], head_gains.shape[1], 1
    )
    renewed.append(adam_update(norm_gains, norm_moments, norm_grad, factor, GAIN_RATE, 0.0))
    renewed.append(adam_update(head_gains, head_moments, head_grad, factor, GAIN_RATE, 0.0))
    return (
        output,
        tokens_grad,
        *owned,
        norm_grad,
        head_grad,
        *[new for new, _ in renewed],
        *[state for _, state in renewed],
    )


def solution(mesh):
    placed = (
        P(("dp", "group"), None),
        P(("dp", "group")),
        P(("dp", "group")),
        P(("dp", "group"), None),
        P("group", None),
        P("group", None),
        P("group", None),
        P("group", None),
        P(None, "group"),
        P(None, "group"),
        P(None, "group", None),
        P(None, "group", None),
        P(None, "group", None),
        P(None, "group", None),
        P(None, None, "group"),
        P(None, None, "group"),
    )
    return jax.shard_map(
        on_device,
        mesh=mesh,
        in_specs=placed,
        out_specs=(
            P(("dp", "group"), None),
            P(("dp", "group"), None),
            P("group", "dp"),
            P("group", "dp"),
            P("group", "dp"),
            P("group", "dp"),
            P(None, "group"),
            P(None, "group"),
            P("group", None),
            P("group", None),
            P("group", None),
            P("group", None),
            P(None, "group"),
            P(None, "group"),
            P(None, "group", None),
            P(None, "group", None),
            P(None, "group", None),
            P(None, "group", None),
            P(None, None, "group"),
            P(None, None, "group"),
        ),
        check_vma=False,
    )
```

```python
import functools
import math

import jax
import jax.numpy as jnp
from jax import lax
from jax.experimental import pallas as pl
from jax.experimental.pallas import tpu as pltpu
from jax.sharding import PartitionSpec as P


HQ = 16
HK = 8
HD = 128
FF = 3072
SEQ_LEN = 512
PARAMS = 15730944


EPS_NORM = 1e-06
ROPE_BASE = 1000000.0
MASKED = -1e30
LEARN_RATE = 0.03
GAIN_RATE = 0.3
WEIGHT_DECAY = 0.1
BETA_ONE = 0.9
BETA_TWO = 0.95
ADAM_EPS = 1e-08
STEP_COUNT = 3.0


def rotary_tables(places, width):
    half_width = width // 2
    frequency = ROPE_BASE ** (-(jnp.arange(half_width, dtype=jnp.float32) * 2.0) / width)
    angles = places.astype(jnp.float32)[:, None] * frequency[None, :]
    cosine, sine = jnp.cos(angles), jnp.sin(angles)
    return (
        jnp.concatenate([cosine, cosine], axis=1),
        jnp.concatenate([-sine, sine], axis=1),
    )


def contract_rows(left_side, right_side):
    return lax.dot_general(
        left_side, right_side, (((0,), (0,)), ((), ())), preferred_element_type=jnp.float32
    )


def contract_cols(left_side, right_side):
    return lax.dot_general(
        left_side, right_side, (((1,), (1,)), ((), ())), preferred_element_type=jnp.float32
    )


def norm_back(grad_out, normed, inv_root, gain):
    scaled = grad_out * gain
    return inv_root * (scaled - normed * jnp.mean(normed * scaled, axis=-1, keepdims=True))


def swap(value, axis, mask):
    count = lax.axis_size(axis)
    return lax.ppermute(value, axis, [(i, i ^ mask) for i in range(count)])


def bit_masks(count):
    return [1 << i for i in range(count.bit_length() - 1)]


def after(value, *others):
    return lax.optimization_barrier((value, others))[0]


def blank(shape, kind):
    return pl.pallas_call(
        lambda out_ref: None,
        out_shape=jax.ShapeDtypeStruct(shape, kind),
        out_specs=pl.BlockSpec(memory_space=pl.ANY),
    )()


def gather_rows(shard, previous):
    owners = lax.axis_size("group")
    copies = lax.axis_size("dp")
    mine = lax.axis_index("group")
    here = lax.axis_index("dp")
    if previous is not None:
        shard = after(shard, previous)
    shard = shard.astype(jnp.bfloat16)
    rows, columns = shard.shape
    pieces = [(shard, 0, 0)]
    order = by_one = by_two = shard
    if owners == 4 and copies % 4 == 0 and rows % 128 == 0:
        quarter, half = rows // 4, rows // 8
        place = (here & 1) * 2 + ((here >> 1) & 1)
        near = lax.dynamic_slice_in_dim(shard, place * quarter, quarter, 0)
        order = swap(near, "group", 2)
        by_one = swap(order, "dp", 1)
        by_two = swap(order, "dp", 2)
        last = (place ^ 3) * quarter
        pieces += [
            (order, 2, place * quarter),
            (by_one, 2, (place ^ 2) * quarter),
            (by_two, 2, (place ^ 1) * quarter),
            (swap(by_two[:half], "dp", 1), 2, last),
            (swap(by_one[half:], "dp", 2), 2, last + half),
        ]
    else:
        for mask in bit_masks(owners)[1:]:
            pieces += [(swap(v, "group", mask), dg ^ mask, off) for v, dg, off in pieces]
    pieces += [(swap(v, "group", 1), dg ^ 1, off) for v, dg, off in pieces]
    full = blank((rows * owners, columns), shard.dtype)
    for value, delta, offset in pieces:
        start = (mine ^ delta) * rows + offset
        full = lax.dynamic_update_slice(full, value, (start, 0))
    return full, order, (by_one, by_two)


def gather_small(shard):
    owners = lax.axis_size("group")
    mine = lax.axis_index("group")
    width = shard.shape[1]
    held = shard[None]
    deltas = [0]
    for mask in reversed(bit_masks(owners)):
        held = jnp.concatenate([held, swap(held, "group", mask)], axis=0)
        deltas += [d ^ mask for d in deltas]
    full = jnp.zeros((shard.shape[0], width * owners), shard.dtype)
    for k, delta in enumerate(deltas):
        full = lax.dynamic_update_slice(full, held[k], (0, (mine ^ delta) * width))
    return full


def sum_all(value):
    owners = lax.axis_size("group")
    copies = lax.axis_size("dp")
    mesh_type = pl.DeviceIdType.MESH

    def body(in_ref, out_ref, near, near_sum, far, near_send, near_recv, far_send, far_recv):
        mine = lax.axis_index("group")
        here = lax.axis_index("dp")
        near_peers = [(here, mine ^ k) for k in range(1, owners)]
        far_peers = [(here ^ k, mine) for k in range(1, copies)]
        barrier = pltpu.get_barrier_semaphore()
        for peer in near_peers + far_peers:
            pl.semaphore_signal(barrier, inc=1, device_id=peer, device_id_type=mesh_type)
        pl.semaphore_wait(barrier, len(near_peers) + len(far_peers))

        def exchange(source, slots, index, peers, sends, recvs):
            slots[index] = source[...]
            copies_out = [
                pltpu.make_async_remote_copy(
                    src_ref=source,
                    dst_ref=slots.at[index],
                    send_sem=sends.at[k],
                    recv_sem=recvs.at[k],
                    device_id=peer,
                    device_id_type=mesh_type,
                )
                for k, peer in enumerate(peers)
            ]
            for copy in copies_out:
                copy.start()
            for copy in copies_out:
                copy.wait()
            total = slots[0]
            for k in range(1, len(peers) + 1):
                total = total + slots[k]
            return total

        near_sum[...] = exchange(in_ref, near, mine, near_peers, near_send, near_recv)
        out_ref[...] = exchange(near_sum, far, here, far_peers, far_send, far_recv)

    shape = value.shape
    return pl.pallas_call(
        body,
        out_shape=jax.ShapeDtypeStruct(shape, jnp.float32),
        in_specs=[pl.BlockSpec(memory_space=pltpu.VMEM)],
        out_specs=pl.BlockSpec(memory_space=pltpu.VMEM),
        scratch_shapes=[
            pltpu.VMEM((owners,) + shape, jnp.float32),
            pltpu.VMEM(shape, jnp.float32),
            pltpu.VMEM((copies,) + shape, jnp.float32),
            pltpu.SemaphoreType.DMA((owners - 1,)),
            pltpu.SemaphoreType.DMA((owners - 1,)),
            pltpu.SemaphoreType.DMA((copies - 1,)),
            pltpu.SemaphoreType.DMA((copies - 1,)),
        ],
        compiler_params=pltpu.CompilerParams(collective_id=0, has_side_effects=True),
    )(value)


def spread_bits(position, masks):
    total = 0
    count = len(masks)
    for i, mask in enumerate(masks):
        total = total + ((position >> (count - 1 - i)) & 1) * mask
    return total


def grad_blocks(left, right):
    tokens, rows = left.shape
    columns = right.shape[1]
    owners = lax.axis_size("group")
    copies = lax.axis_size("dp")
    column_masks = bit_masks(copies)
    later = bit_masks(owners)[1:]
    staying = [spread_bits(p, later) for p in range(1 << len(later))]
    row_sets = [[dg + 1 for dg in staying], staying] if owners > 1 else [[0]]
    row_block = rows // owners
    column_block = columns // copies
    mine = lax.axis_index("group")
    here = lax.axis_index("dp")
    if column_block % 128 or row_block % 16:
        ordered = jnp.concatenate(
            [
                lax.dynamic_slice_in_dim(
                    right, (here ^ spread_bits(p, column_masks)) * column_block, column_block, 1
                )
                for p in range(copies)
            ],
            axis=1,
        )
        return [
            jnp.stack(
                [
                    contract_rows(
                        lax.dynamic_slice_in_dim(left, (mine ^ dg) * row_block, row_block, 1),
                        ordered,
                    ).astype(jnp.bfloat16)
                    for dg in row_set
                ]
            )
            for row_set in row_sets
        ]
    wide = 2 if column_block % 256 and copies % 2 == 0 else 1

    def body(where, left_ref, *rest):
        rights, outs, turned = rest[:wide], rest[wide:-1], rest[-1]

        @pl.when(pl.program_id(0) == 0)
        def _():
            turned[...] = left_ref[...].T

        block = jnp.concatenate([ref[...] for ref in rights], axis=1)
        for out, row_set in zip(outs, row_sets):
            for k, dg in enumerate(row_set):
                start = pl.multiple_of((where[0] ^ dg) * row_block, row_block)
                out[k] = jnp.dot(
                    turned[pl.ds(start, row_block), :],
                    block,
                    preferred_element_type=jnp.float32,
                ).astype(jnp.bfloat16)

    def right_spec(j):
        return pl.BlockSpec(
            (tokens, column_block),
            lambda p, where: (0, where[1] ^ spread_bits(p * wide + j, column_masks)),
        )

    return pl.pallas_call(
        body,
        out_shape=[
            jax.ShapeDtypeStruct((len(row_set), row_block, columns), jnp.bfloat16)
            for row_set in row_sets
        ],
        grid_spec=pltpu.PrefetchScalarGridSpec(
            num_scalar_prefetch=1,
            grid=(copies // wide,),
            in_specs=[pl.BlockSpec((tokens, rows), lambda p, where: (0, 0))]
            + [right_spec(j) for j in range(wide)],
            out_specs=[
                pl.BlockSpec(
                    (len(row_set), row_block, column_block * wide), lambda p, where: (0, 0, p)
                )
                for row_set in row_sets
            ],
            scratch_shapes=[pltpu.VMEM((rows, tokens), jnp.bfloat16)],
        ),
        compiler_params=pltpu.CompilerParams(vmem_limit_bytes=48 * 1024 * 1024),
        cost_estimate=pl.CostEstimate(
            flops=2 * tokens * rows * columns,
            bytes_accessed=2 * (tokens * rows + tokens * columns + rows * columns),
            transcendentals=0,
        ),
    )(jnp.stack([mine, here]).astype(jnp.int32), left, *[right] * wide)


class GradSum:
    def __init__(self, left, right, split):
        blocks = grad_blocks(left, right)
        self.blocks = blocks
        group = [("group", m) for m in bit_masks(lax.axis_size("group"))]
        other = [("dp", m) for m in bit_masks(lax.axis_size("dp"))]
        self.arrays = [blocks[-1]]
        if group:
            self.arrays.append(swap(blocks[0], "group", 1))
        rest = group[1:]
        self.orders = [rest + other]
        if split:
            self.orders.append(other[:1] + rest + other[1:])
        count = len(self.orders)
        deep, tall, width = blocks[-1].shape
        size = tall // count
        self.parts = [
            [(k, [(0, deep), (i * size, (i + 1) * size), (0, width)]) for k in range(len(self.arrays))]
            for i in range(count)
        ]
        self.common = len(rest) + 1
        self.length = len(rest) + len(other)
        self.step = 0

    def hold(self, *others):
        self.arrays = list(lax.optimization_barrier((self.arrays, others))[0])

    def read(self, part):
        total = 0.0
        for k, ranges in part:
            at = tuple(slice(*r) for r in ranges)
            total = total + self.arrays[k][at].astype(jnp.float32)
        return total

    def exchange(self, away, axis, mask):
        self.arrays.append(swap(away, axis, mask))
        return len(self.arrays) - 1

    def advance(self):
        if self.step == self.length:
            return []
        outgoing = []
        for i, order in enumerate(self.orders):
            axis, mask = order[self.step]
            dim = 0 if axis == "group" else 2
            far, near = [], []
            for k, ranges in self.parts[i]:
                start, stop = ranges[dim]
                middle = (start + stop) // 2
                near.append((k, ranges[:dim] + [(start, middle)] + ranges[dim + 1 :]))
                far.append((k, ranges[:dim] + [(middle, stop)] + ranges[dim + 1 :]))
            self.parts[i] = near
            outgoing.append((self.read(far).astype(jnp.bfloat16), axis, mask))
        deep, tall, width = outgoing[0][0].shape
        if self.step >= self.common:
            away = jnp.concatenate([v for v, _, _ in outgoing], axis=1)
            sent = [away]
            k = self.exchange(away, *outgoing[0][1:])
            for i, part in enumerate(self.parts):
                part.append((k, [(0, deep), (i * tall, (i + 1) * tall), (0, width)]))
        else:
            sent = [v for v, _, _ in outgoing]
            for i, (away, axis, mask) in enumerate(outgoing):
                k = self.exchange(away, axis, mask)
                deep, tall, width = away.shape
                self.parts[i].append((k, [(0, deep), (0, tall), (0, width)]))
        self.step += 1
        return sent

    def finish(self):
        while self.step < self.length:
            self.advance()
        return jnp.concatenate([self.read(part)[0] for part in self.parts], axis=0)


def gather_grad(own, last):
    held = own.astype(jnp.bfloat16)[None]
    deltas = [0]
    groups = [(held, deltas)]
    masks = list(reversed(bit_masks(lax.axis_size("dp"))))
    for i, mask in enumerate(masks):
        away = held if last is None or i + 1 < len(masks) else after(held, last)
        got = swap(away, "dp", mask)
        got_deltas = [d ^ mask for d in deltas]
        if i + 1 < len(masks):
            held = jnp.concatenate([held, got], axis=0)
            deltas = deltas + got_deltas
            groups = [(held, deltas)]
        else:
            groups.append((got, got_deltas))
    return groups


def adam_core(master, first_moment, second_moment, clipped, step_rate, decay_rate):
    first_new = BETA_ONE * first_moment + (1.0 - BETA_ONE) * clipped
    second_new = BETA_TWO * second_moment + (1.0 - BETA_TWO) * clipped * clipped
    first_hat = first_new * (1.0 / (1.0 - BETA_ONE**STEP_COUNT))
    second_hat = second_new * (1.0 / (1.0 - BETA_TWO**STEP_COUNT))
    renewed = master - step_rate * (
        first_hat / (jnp.sqrt(second_hat) + ADAM_EPS) + decay_rate * master
    )
    return renewed, first_new, second_new


def adam_blocks(master, moment, blocks, factor, step_rate, decay_rate):
    rows, columns = master.shape
    copies = lax.axis_size("dp")
    here = lax.axis_index("dp")
    width = columns // copies
    if width % 128:
        full = jnp.zeros(master.shape, jnp.float32)
        for value, deltas in blocks:
            for k, dd in enumerate(deltas):
                full = lax.dynamic_update_slice(
                    full, value[k].astype(jnp.float32), (0, (here ^ dd) * width)
                )
        return adam_update(master, moment, full, factor, step_rate, decay_rate)
    tile = rows
    while tile % 32 == 0 and tile * columns > 256 * 1024:
        tile //= 2

    def body(where, factor_ref, master_ref, moment_ref, *rest):
        grads, (new_ref, state_ref) = rest[:-2], rest[-2:]
        scale = factor_ref[0, 0]
        for grad, (_, deltas) in zip(grads, blocks):
            for k, dd in enumerate(deltas):
                at = pl.ds(pl.multiple_of((where[0] ^ dd) * width, 128), width)
                renewed, first_new, second_new = adam_core(
                    master_ref[:, at],
                    moment_ref[0, :, at],
                    moment_ref[1, :, at],
                    grad[k].astype(jnp.float32) * scale,
                    step_rate,
                    decay_rate,
                )
                new_ref[:, at] = renewed
                state_ref[0, :, at] = first_new
                state_ref[1, :, at] = second_new

    return pl.pallas_call(
        body,
        out_shape=[
            jax.ShapeDtypeStruct(master.shape, jnp.float32),
            jax.ShapeDtypeStruct(moment.shape, jnp.float32),
        ],
        grid_spec=pltpu.PrefetchScalarGridSpec(
            num_scalar_prefetch=1,
            grid=(rows // tile,),
            in_specs=[
                pl.BlockSpec(memory_space=pltpu.SMEM),
                pl.BlockSpec((tile, columns), lambda i, where: (i, 0)),
                pl.BlockSpec((2, tile, columns), lambda i, where: (0, i, 0)),
            ]
            + [
                pl.BlockSpec((len(deltas), tile, width), lambda i, where: (0, i, 0))
                for _, deltas in blocks
            ],
            out_specs=[
                pl.BlockSpec((tile, columns), lambda i, where: (i, 0)),
                pl.BlockSpec((2, tile, columns), lambda i, where: (0, i, 0)),
            ],
        ),
        compiler_params=pltpu.CompilerParams(vmem_limit_bytes=48 * 1024 * 1024),
        cost_estimate=pl.CostEstimate(
            flops=20 * rows * columns,
            bytes_accessed=26 * rows * columns,
            transcendentals=rows * columns,
        ),
    )(
        here.reshape(1).astype(jnp.int32),
        factor.reshape(1, 1),
        master,
        moment,
        *[value for value, _ in blocks],
    )


def adam_update(master, moment, gradient, factor, step_rate, decay_rate):
    clipped = gradient * factor
    first_moment = BETA_ONE * moment[0] + (1.0 - BETA_ONE) * clipped
    second = BETA_TWO * moment[1] + (1.0 - BETA_TWO) * clipped * clipped
    first_hat = first_moment / (1.0 - BETA_ONE**STEP_COUNT)
    second_hat = second / (1.0 - BETA_TWO**STEP_COUNT)
    renewed = master - step_rate * (
        first_hat / (jnp.sqrt(second_hat) + ADAM_EPS) + decay_rate * master
    )
    return (renewed, jnp.stack([first_moment, second]))


def head_forward(raw, gain, cosine, sine):
    root = lax.rsqrt(jnp.mean(raw * raw, axis=-1, keepdims=True) + EPS_NORM)
    normed = raw * root
    scaled = normed * gain
    turned = scaled * cosine + pltpu.roll(scaled, HD // 2, 1) * sine
    return turned.astype(jnp.bfloat16), normed, root


def head_backward(grad, normed, root, gain, cosine, sine):
    turned = grad * cosine - pltpu.roll(grad, HD // 2, 1) * sine
    grad_gain = jnp.sum(turned * normed, axis=0, keepdims=True)
    scaled = turned * gain
    raw = root * (scaled - normed * jnp.mean(normed * scaled, axis=-1, keepdims=True))
    return raw, grad_gain


SPAN = 256


def span_weights(query_low, key_low, seg_row_ref, seg_col_ref, start):
    stop = start + SPAN
    scores = lax.dot_general(
        key_low[:stop],
        query_low[start:stop],
        (((1,), (1,)), ((), ())),
        preferred_element_type=jnp.float32,
    ) * (1.0 / math.sqrt(HD))
    key_at = lax.broadcasted_iota(jnp.int32, (stop, SPAN), 0)
    query_at = lax.broadcasted_iota(jnp.int32, (stop, SPAN), 1) + start
    allowed = (key_at <= query_at) & (seg_col_ref[:stop, :] == seg_row_ref[:, start:stop])
    scores = jnp.where(allowed, scores, MASKED)
    raised = jnp.exp(scores - jnp.max(scores, axis=0, keepdims=True))
    return raised * (1.0 / jnp.sum(raised, axis=0, keepdims=True))


def attend_body(
    query_ref, key_ref, value_ref, cos_ref, sin_ref, row_ref, col_ref, gain_ref, out_ref
):
    cosine, sine = cos_ref[...], sin_ref[...]
    key_low, _, _ = head_forward(key_ref[...], gain_ref[1:2, :], cosine, sine)
    value_turned = value_ref[...].astype(jnp.bfloat16).T
    for g in range(HQ // HK):
        at = slice(g * HD, (g + 1) * HD)
        query_low, _, _ = head_forward(query_ref[:, at], gain_ref[0:1, :], cosine, sine)
        for start in range(0, SEQ_LEN, SPAN):
            stop = start + SPAN
            weights = span_weights(query_low, key_low, row_ref, col_ref, start)
            mixed = jnp.dot(
                value_turned[:, :stop],
                weights.astype(jnp.bfloat16),
                preferred_element_type=jnp.float32,
            )
            out_ref[start:stop, at] = mixed.T.astype(jnp.bfloat16)


def attend_back_body(
    query_ref, key_ref, value_ref, cos_ref, sin_ref, row_ref, col_ref, gain_ref, grad_ref,
    *rest,
    first,
):
    out_ref, gain_out_ref = rest[-2:]
    head = pl.program_id(1) + first
    cosine, sine = cos_ref[...], sin_ref[...]
    inv_head = 1.0 / math.sqrt(HD)

    @pl.when((pl.program_id(0) == 0) & (head == first))
    def _():
        gain_out_ref[...] = jnp.zeros_like(gain_out_ref)

    if len(rest) == 3:

        @pl.when(head == first)
        def _():
            out_ref[...] = rest[0][...]

    key_low, key_normed, key_root = head_forward(key_ref[...], gain_ref[1:2, :], cosine, sine)
    value_low = value_ref[...].astype(jnp.bfloat16)
    key_turned = key_low.T
    grad_key = [jnp.zeros((SPAN, HD), jnp.float32)] * (SEQ_LEN // SPAN)
    grad_value = list(grad_key)
    gain_query = jnp.zeros((1, HD), jnp.float32)
    for g in range(HQ // HK):
        at = slice(g * HD, (g + 1) * HD)
        query_low, normed, root = head_forward(query_ref[:, at], gain_ref[0:1, :], cosine, sine)
        grad_query = []
        for start in range(0, SEQ_LEN, SPAN):
            stop = start + SPAN
            weights = span_weights(query_low, key_low, row_ref, col_ref, start)
            grad_out = grad_ref[start:stop, at]
            grad_weights = lax.dot_general(
                value_low[:stop],
                grad_out,
                (((1,), (1,)), ((), ())),
                preferred_element_type=jnp.float32,
            )
            more_value = jnp.dot(
                weights.astype(jnp.bfloat16), grad_out, preferred_element_type=jnp.float32
            )
            product = weights * grad_weights
            grad_scores = (
                weights * (grad_weights - jnp.sum(product, axis=0, keepdims=True))
            ).astype(jnp.bfloat16)
            more_key = jnp.dot(
                grad_scores, query_low[start:stop], preferred_element_type=jnp.float32
            )
            grad_query.append(
                jnp.dot(
                    key_turned[:, :stop], grad_scores, preferred_element_type=jnp.float32
                ).T
            )
            for j in range(stop // SPAN):
                part = slice(j * SPAN, (j + 1) * SPAN)
                grad_key[j] = grad_key[j] + more_key[part]
                grad_value[j] = grad_value[j] + more_value[part]
        raw, more_gain = head_backward(
            jnp.concatenate(grad_query, axis=0) * inv_head,
            normed,
            root,
            gain_ref[0:1, :],
            cosine,
            sine,
        )
        gain_query = gain_query + more_gain
        place = pl.multiple_of((head * (HQ // HK) + g) * HD, HD)
        out_ref[:, pl.ds(place, HD)] = raw.astype(jnp.bfloat16)
    raw, gain_key = head_backward(
        jnp.concatenate(grad_key, axis=0) * inv_head,
        key_normed,
        key_root,
        gain_ref[1:2, :],
        cosine,
        sine,
    )
    out_ref[:, pl.ds(pl.multiple_of((HQ + head) * HD, HD), HD)] = raw.astype(jnp.bfloat16)
    out_ref[:, pl.ds(pl.multiple_of((HQ + HK + head) * HD, HD), HD)] = jnp.concatenate(
        grad_value, axis=0
    ).astype(jnp.bfloat16)
    gain_out_ref[0:1, :] += gain_query
    gain_out_ref[1:2, :] += gain_key


def attention_call(body, projected, tables, segments, gains, grad_out, first, count, base):
    token_rows = projected.shape[0]
    seq_count = token_rows // SEQ_LEN
    groups = HQ // HK
    wide = groups * HD
    full = lambda s, h: (s, 0)
    in_specs = [
        pl.BlockSpec((SEQ_LEN, wide), lambda s, h: (s, first + h)),
        pl.BlockSpec((SEQ_LEN, HD), lambda s, h: (s, HQ + first + h)),
        pl.BlockSpec((SEQ_LEN, HD), lambda s, h: (s, HQ + HK + first + h)),
        pl.BlockSpec((SEQ_LEN, HD), full),
        pl.BlockSpec((SEQ_LEN, HD), full),
        pl.BlockSpec((1, SEQ_LEN), lambda s, h: (0, s)),
        pl.BlockSpec((SEQ_LEN, 1), full),
        pl.BlockSpec((2, HD), lambda s, h: (0, 0)),
    ]
    operands = [
        projected,
        projected,
        projected,
        *tables,
        segments[None, :],
        segments[:, None],
        gains,
    ]
    pairs = token_rows * SEQ_LEN * groups * count
    aliases = {}
    if grad_out is None:
        out_specs = pl.BlockSpec((SEQ_LEN, wide), lambda s, h: (s, first + h))
        out_shape = jax.ShapeDtypeStruct((token_rows, HQ * HD), jnp.bfloat16)
    else:
        columns = projected.shape[1]
        in_specs.append(pl.BlockSpec((SEQ_LEN, wide), lambda s, h: (s, first + h)))
        operands.append(grad_out)
        body = functools.partial(body, first=first)
        if base is not None:
            aliases = {len(operands): 0}
            in_specs.append(pl.BlockSpec((SEQ_LEN, columns), full))
            operands.append(base)
        out_specs = [
            pl.BlockSpec((SEQ_LEN, columns), full),
            pl.BlockSpec((2, HD), lambda s, h: (0, 0)),
        ]
        out_shape = [
            jax.ShapeDtypeStruct((token_rows, columns), jnp.bfloat16),
            jax.ShapeDtypeStruct((2, HD), jnp.float32),
        ]
    return pl.pallas_call(
        body,
        grid=(seq_count, count),
        in_specs=in_specs,
        out_specs=out_specs,
        out_shape=out_shape,
        input_output_aliases=aliases,
        compiler_params=pltpu.CompilerParams(vmem_limit_bytes=48 * 1024 * 1024),
        cost_estimate=pl.CostEstimate(
            flops=(4 if grad_out is None else 10) * pairs * HD * 2,
            bytes_accessed=projected.size * 6,
            transcendentals=pairs,
        ),
    )(*operands)


def gate_up_back(cotangent, full_down, gate_up):
    tokens, columns = cotangent.shape
    block = 512
    steps = FF // block

    def body(cot_ref, down_ref, gate_ref, up_ref, out_ref):
        at = pl.program_id(0) * block
        grad = lax.dot_general(
            cot_ref[...],
            down_ref[...],
            (((1,), (1,)), ((), ())),
            preferred_element_type=jnp.float32,
        )
        gate = gate_ref[...]
        part = jax.nn.sigmoid(gate)
        grad_gate = grad * up_ref[...] * part * (1.0 + gate * (1.0 - part))
        grad_up = grad * gate * part
        out_ref[:, pl.ds(pl.multiple_of(at, block), block)] = grad_gate.astype(jnp.bfloat16)
        out_ref[:, pl.ds(pl.multiple_of(at + FF, block), block)] = grad_up.astype(jnp.bfloat16)

    return pl.pallas_call(
        body,
        grid=(steps,),
        in_specs=[
            pl.BlockSpec((tokens, columns), lambda j: (0, 0)),
            pl.BlockSpec((block, columns), lambda j: (j, 0)),
            pl.BlockSpec((tokens, block), lambda j: (0, j)),
            pl.BlockSpec((tokens, block), lambda j: (0, steps + j)),
        ],
        out_specs=pl.BlockSpec((tokens, 2 * FF), lambda j: (0, 0)),
        out_shape=jax.ShapeDtypeStruct((tokens, 2 * FF), jnp.bfloat16),
        compiler_params=pltpu.CompilerParams(vmem_limit_bytes=48 * 1024 * 1024),
        cost_estimate=pl.CostEstimate(
            flops=2 * tokens * FF * columns,
            bytes_accessed=2 * FF * columns + 12 * tokens * FF,
            transcendentals=tokens * FF,
        ),
    )(cotangent, full_down, gate_up, gate_up)


def on_device(
    tokens,
    segment_ids,
    positions,
    cotangent,
    qkv_weight,
    out_weight,
    gate_up_weight,
    down_weight,
    norm_gains,
    head_gains,
    qkv_moments,
    out_moments,
    gate_up_moments,
    down_moments,
    norm_moments,
    head_moments,
):
    width = norm_gains.shape[1]
    gains_low = jnp.concatenate([norm_gains, head_gains], axis=1).astype(jnp.bfloat16)
    owners = lax.axis_size("group")
    gains_all = gather_small(gains_low).reshape(2, owners, -1)
    full_norm = gains_all[:, :, :width].reshape(2, -1)
    full_head = gains_all[:, :, width:].reshape(2, -1)
    full_qkv, _, order = gather_rows(qkv_weight, None)
    full_out, order, _ = gather_rows(out_weight, order)
    full_gate_up, order, _ = gather_rows(gate_up_weight, order)
    gain_one = full_norm[0].astype(jnp.float32)
    gain_two = full_norm[1].astype(jnp.float32)
    head_gain = full_head.astype(jnp.float32)
    inputs = tokens.astype(jnp.float32)
    root_one = lax.rsqrt(jnp.mean(inputs * inputs, axis=-1, keepdims=True) + EPS_NORM)
    normed_one = inputs * root_one
    hidden_one = (normed_one * gain_one).astype(jnp.bfloat16)
    projected = jnp.dot(hidden_one, full_qkv, preferred_element_type=jnp.float32)
    full_down, _, _ = gather_rows(down_weight, (order, projected))
    tables = rotary_tables(positions, HD)
    mixed_low = attention_call(attend_body, projected, tables, segment_ids, head_gain, None, 0, HK, None)
    attended = jnp.dot(mixed_low, full_out, preferred_element_type=jnp.float32)
    residual = inputs + attended
    root_two = lax.rsqrt(jnp.mean(residual * residual, axis=-1, keepdims=True) + EPS_NORM)
    normed_two = residual * root_two
    hidden_two = (normed_two * gain_two).astype(jnp.bfloat16)
    gate_up = jnp.dot(hidden_two, full_gate_up, preferred_element_type=jnp.float32)
    gate_part = gate_up[:, :FF]
    upward = gate_up[:, FF:]
    sigmoid_gate = jax.nn.sigmoid(gate_part)
    activated = (gate_part * sigmoid_gate * upward).astype(jnp.bfloat16)
    branch = jnp.dot(activated, full_down, preferred_element_type=jnp.float32)
    output = (residual + branch).astype(jnp.bfloat16)
    upstream = cotangent.astype(jnp.float32)
    down_sum = GradSum(activated, cotangent, True)
    grad_gate_up = gate_up_back(after(cotangent, *down_sum.blocks), full_down, gate_up)
    gate_up_sum = GradSum(hidden_two, after(grad_gate_up, *down_sum.advance()), True)
    grad_hidden_two = contract_cols(after(grad_gate_up, *gate_up_sum.blocks), full_gate_up)
    grad_gain_two = jnp.sum(grad_hidden_two * normed_two, axis=0)
    grad_residual = upstream + norm_back(grad_hidden_two, normed_two, root_two, gain_two)
    residual_low = grad_residual.astype(jnp.bfloat16)
    down_sum.hold(residual_low)
    sent = down_sum.advance() + gate_up_sum.advance()
    out_sum = GradSum(mixed_low, after(residual_low, *sent), False)
    down_sum.hold(out_sum.blocks)
    grad_mixed = contract_cols(
        after(residual_low, *out_sum.blocks, *down_sum.advance()), full_out
    ).astype(jnp.bfloat16)
    grad_mixed = after(grad_mixed, *out_sum.advance())
    half = HK // 2
    grad_half, gain_half = attention_call(
        attend_back_body, projected, tables, segment_ids, head_gain, grad_mixed, 0, half, None
    )
    gate_up_sum.hold(grad_half)
    down_sum.hold(grad_half)
    sent = gate_up_sum.advance() + down_sum.advance()
    grad_projected, grad_gain_head = attention_call(
        attend_back_body,
        projected,
        tables,
        segment_ids,
        head_gain,
        grad_mixed,
        half,
        HK - half,
        after(grad_half, *sent),
    )
    grad_gain_head = grad_gain_head + gain_half
    gate_up_sum.hold(grad_projected)
    out_sum.hold(grad_projected)
    sent = gate_up_sum.advance() + out_sum.advance()
    qkv_sum = GradSum(hidden_one, after(grad_projected, *sent), True)
    gate_up_sum.hold(qkv_sum.blocks)
    sent = qkv_sum.advance()
    gate_up_sum.hold(sent)
    out_sum.hold(sent)
    down_sum.hold(sent)
    sent = sent + gate_up_sum.advance() + out_sum.advance()
    grad_hidden_one = contract_cols(after(grad_projected, *qkv_sum.blocks, *sent), full_qkv)
    grad_gain_one = jnp.sum(grad_hidden_one * normed_one, axis=0)
    grad_inputs = grad_residual + norm_back(grad_hidden_one, normed_one, root_one, gain_one)
    tokens_grad = grad_inputs.astype(jnp.bfloat16)
    small = jnp.concatenate(
        [jnp.stack([grad_gain_one, grad_gain_two]), grad_gain_head],
        axis=1,
    )
    owned = tuple(v.finish() for v in (qkv_sum, out_sum, gate_up_sum, down_sum))
    local = sum(jnp.sum(v * v) for v in owned)
    summed = sum_all(
        jnp.concatenate(
            [small, jnp.full((6, small.shape[1]), local, jnp.float32)], axis=0
        )
    )
    small = summed[:2]
    norm_total = small[:, :-HD]
    head_total = small[:, -HD:]
    squares = summed[2, 0] + jnp.sum(small * small)
    clip_limit = math.sqrt(PARAMS)
    factor = clip_limit / jnp.maximum(jnp.sqrt(squares), clip_limit)
    qkv_own, out_own, gate_up_own, down_own = owned
    gathered = [
        gather_grad(after(qkv_own, summed), None),
        gather_grad(out_own, None),
        gather_grad(gate_up_own, summed),
        gather_grad(down_own, None),
    ]
    masters = (qkv_weight, out_weight, gate_up_weight, down_weight)
    moments = (qkv_moments, out_moments, gate_up_moments, down_moments)
    later = after(factor, gathered[0][0][0])
    renewed = [
        adam_blocks(master, moment, blocks, scale, LEARN_RATE, WEIGHT_DECAY)
        for master, moment, blocks, scale in zip(
            masters, moments, gathered, (later, factor, later, later)
        )
    ]
    mine = lax.axis_index("group")
    norm_grad = lax.dynamic_slice_in_dim(
        norm_total, mine * norm_gains.shape[1], norm_gains.shape[1], 1
    )
    head_grad = lax.dynamic_slice_in_dim(
        head_total, mine * head_gains.shape[1], head_gains.shape[1], 1
    )
    renewed.append(adam_update(norm_gains, norm_moments, norm_grad, factor, GAIN_RATE, 0.0))
    renewed.append(adam_update(head_gains, head_moments, head_grad, factor, GAIN_RATE, 0.0))
    return (
        output,
        tokens_grad,
        *owned,
        norm_grad,
        head_grad,
        *[new for new, _ in renewed],
        *[state for _, state in renewed],
    )


def solution(mesh):
    placed = (
        P(("dp", "group"), None),
        P(("dp", "group")),
        P(("dp", "group")),
        P(("dp", "group"), None),
        P("group", None),
        P("group", None),
        P("group", None),
        P("group", None),
        P(None, "group"),
        P(None, "group"),
        P(None, "group", None),
        P(None, "group", None),
        P(None, "group", None),
        P(None, "group", None),
        P(None, None, "group"),
        P(None, None, "group"),
    )
    return jax.shard_map(
        on_device,
        mesh=mesh,
        in_specs=placed,
        out_specs=(
            P(("dp", "group"), None),
            P(("dp", "group"), None),
            P("group", "dp"),
            P("group", "dp"),
            P("group", "dp"),
            P("group", "dp"),
            P(None, "group"),
            P(None, "group"),
            P("group", None),
            P("group", None),
            P("group", None),
            P("group", None),
            P(None, "group"),
            P(None, "group"),
            P(None, "group", None),
            P(None, "group", None),
            P(None, "group", None),
            P(None, "group", None),
            P(None, None, "group"),
            P(None, None, "group"),
        ),
        check_vma=False,
    )
```

```python
import functools
import math

import jax
import jax.numpy as jnp
from jax import lax
from jax.experimental import pallas as pl
from jax.experimental.pallas import tpu as pltpu
from jax.sharding import PartitionSpec as P


HQ = 16
HK = 8
HD = 128
FF = 3072
SEQ_LEN = 512
PARAMS = 15730944


EPS_NORM = 1e-06
ROPE_BASE = 1000000.0
MASKED = -1e30
LEARN_RATE = 0.03
GAIN_RATE = 0.3
WEIGHT_DECAY = 0.1
BETA_ONE = 0.9
BETA_TWO = 0.95
ADAM_EPS = 1e-08
STEP_COUNT = 3.0


def rotary_tables(places, width):
    half_width = width // 2
    frequency = ROPE_BASE ** (-(jnp.arange(half_width, dtype=jnp.float32) * 2.0) / width)
    angles = places.astype(jnp.float32)[:, None] * frequency[None, :]
    cosine, sine = jnp.cos(angles), jnp.sin(angles)
    return (
        jnp.concatenate([cosine, cosine], axis=1),
        jnp.concatenate([-sine, sine], axis=1),
    )


def contract_rows(left_side, right_side):
    return lax.dot_general(
        left_side, right_side, (((0,), (0,)), ((), ())), preferred_element_type=jnp.float32
    )


def contract_cols(left_side, right_side):
    return lax.dot_general(
        left_side, right_side, (((1,), (1,)), ((), ())), preferred_element_type=jnp.float32
    )


def norm_back(grad_out, normed, inv_root, gain):
    scaled = grad_out * gain
    return inv_root * (scaled - normed * jnp.mean(normed * scaled, axis=-1, keepdims=True))


def swap(value, axis, mask):
    count = lax.axis_size(axis)
    return lax.ppermute(value, axis, [(i, i ^ mask) for i in range(count)])


def bit_masks(count):
    return [1 << i for i in range(count.bit_length() - 1)]


def after(value, *others):
    return lax.optimization_barrier((value, others))[0]


def place_rows(pieces, rows, owners):
    columns = pieces[0][0].shape[1]
    kind = pieces[0][0].dtype
    sizes = [v.shape[0] for v, _, _ in pieces]

    def body(*refs):
        count = len(pieces)
        ins, out_ref, held = refs[:count], refs[count], refs[count + 1]
        into, away = refs[count + 2 :]
        mine = lax.axis_index("group")
        here = lax.axis_index("dp")
        arriving, leaving, at = [], [], 0
        for k, (_, delta, offset) in enumerate(pieces):
            slot = held.at[pl.ds(at, sizes[k])]
            start = pl.multiple_of((mine ^ delta) * rows + offset(here), 16)
            arriving.append(pltpu.make_async_copy(ins[k], slot, into.at[k]))
            leaving.append(
                pltpu.make_async_copy(slot, out_ref.at[pl.ds(start, sizes[k])], away.at[k])
            )
            at += sizes[k]
        for copy in arriving:
            copy.start()
        for first, second in zip(arriving, leaving):
            first.wait()
            second.start()
        for copy in leaving:
            copy.wait()

    return pl.pallas_call(
        body,
        out_shape=jax.ShapeDtypeStruct((rows * owners, columns), kind),
        in_specs=[pl.BlockSpec(memory_space=pl.ANY)] * len(pieces),
        out_specs=pl.BlockSpec(memory_space=pl.ANY),
        scratch_shapes=[
            pltpu.VMEM((rows * owners, columns), kind),
            pltpu.SemaphoreType.DMA((len(pieces),)),
            pltpu.SemaphoreType.DMA((len(pieces),)),
        ],
        compiler_params=pltpu.CompilerParams(vmem_limit_bytes=32 * 1024 * 1024),
        cost_estimate=pl.CostEstimate(
            flops=0, bytes_accessed=4 * rows * owners * columns, transcendentals=0
        ),
    )(*[v for v, _, _ in pieces])


def gather_rows(shard, early, late, middle, hold):
    owners = lax.axis_size("group")
    copies = lax.axis_size("dp")
    here = lax.axis_index("dp")
    if early is not None:
        shard = after(shard, early)
    shard = shard.astype(jnp.bfloat16)
    rows, _ = shard.shape

    def none(_):
        return 0

    pieces = [(shard, 0, none)]
    near = order = by_one = by_two = shard
    if owners == 4 and copies % 4 == 0 and rows % 128 == 0:
        quarter, half = rows // 4, rows // 8

        def place(here):
            return (here & 1) * 2 + ((here >> 1) & 1)

        def quarter_at(mask, more=0):
            return lambda here: (place(here) ^ mask) * quarter + more

        near = lax.dynamic_slice_in_dim(shard, place(here) * quarter, quarter, 0)
        if late is not None:
            near = after(near, late)
        order = swap(near, "group", 2)
        passed = order if middle is None else after(order, middle)
        by_one = swap(passed, "dp", 1)
        by_two = swap(passed, "dp", 2)
        pieces += [
            (order, 2, quarter_at(0)),
            (by_one, 2, quarter_at(2)),
            (by_two, 2, quarter_at(1)),
            (swap(by_two[:half], "dp", 1), 2, quarter_at(3)),
            (swap(by_one[half:], "dp", 2), 2, quarter_at(3, half)),
        ]
    else:
        for mask in bit_masks(owners)[1:]:
            pieces += [(swap(v, "group", mask), dg ^ mask, at) for v, dg, at in pieces]
    pieces += [(swap(v, "group", 1), dg ^ 1, at) for v, dg, at in pieces]
    if hold is not None:
        pieces[0] = (after(shard, hold), 0, none)
    return place_rows(pieces, rows, owners), near, order, (by_one, by_two)


def gather_small(shard):
    owners = lax.axis_size("group")
    mine = lax.axis_index("group")
    width = shard.shape[1]
    held = shard[None]
    deltas = [0]
    for mask in reversed(bit_masks(owners)):
        held = jnp.concatenate([held, swap(held, "group", mask)], axis=0)
        deltas += [d ^ mask for d in deltas]
    full = jnp.zeros((shard.shape[0], width * owners), shard.dtype)
    for k, delta in enumerate(deltas):
        full = lax.dynamic_update_slice(full, held[k], (0, (mine ^ delta) * width))
    return full


def sum_all(value):
    owners = lax.axis_size("group")
    copies = lax.axis_size("dp")
    mesh_type = pl.DeviceIdType.MESH

    def body(in_ref, out_ref, near, near_sum, far, near_send, near_recv, far_send, far_recv):
        mine = lax.axis_index("group")
        here = lax.axis_index("dp")
        near_peers = [(here, mine ^ k) for k in range(1, owners)]
        far_peers = [(here ^ k, mine) for k in range(1, copies)]
        barrier = pltpu.get_barrier_semaphore()
        for peer in near_peers + far_peers:
            pl.semaphore_signal(barrier, inc=1, device_id=peer, device_id_type=mesh_type)
        pl.semaphore_wait(barrier, len(near_peers) + len(far_peers))

        def exchange(source, slots, index, peers, sends, recvs):
            slots[index] = source[...]
            copies_out = [
                pltpu.make_async_remote_copy(
                    src_ref=source,
                    dst_ref=slots.at[index],
                    send_sem=sends.at[k],
                    recv_sem=recvs.at[k],
                    device_id=peer,
                    device_id_type=mesh_type,
                )
                for k, peer in enumerate(peers)
            ]
            for copy in copies_out:
                copy.start()
            for copy in copies_out:
                copy.wait()
            total = slots[0]
            for k in range(1, len(peers) + 1):
                total = total + slots[k]
            return total

        near_sum[...] = exchange(in_ref, near, mine, near_peers, near_send, near_recv)
        out_ref[...] = exchange(near_sum, far, here, far_peers, far_send, far_recv)

    shape = value.shape
    return pl.pallas_call(
        body,
        out_shape=jax.ShapeDtypeStruct(shape, jnp.float32),
        in_specs=[pl.BlockSpec(memory_space=pltpu.VMEM)],
        out_specs=pl.BlockSpec(memory_space=pltpu.VMEM),
        scratch_shapes=[
            pltpu.VMEM((owners,) + shape, jnp.float32),
            pltpu.VMEM(shape, jnp.float32),
            pltpu.VMEM((copies,) + shape, jnp.float32),
            pltpu.SemaphoreType.DMA((owners - 1,)),
            pltpu.SemaphoreType.DMA((owners - 1,)),
            pltpu.SemaphoreType.DMA((copies - 1,)),
            pltpu.SemaphoreType.DMA((copies - 1,)),
        ],
        compiler_params=pltpu.CompilerParams(collective_id=0, has_side_effects=True),
    )(value)


def spread_bits(position, masks):
    total = 0
    count = len(masks)
    for i, mask in enumerate(masks):
        total = total + ((position >> (count - 1 - i)) & 1) * mask
    return total


def grad_blocks(left, right):
    tokens, rows = left.shape
    columns = right.shape[1]
    owners = lax.axis_size("group")
    copies = lax.axis_size("dp")
    column_masks = bit_masks(copies)
    later = bit_masks(owners)[1:]
    staying = [spread_bits(p, later) for p in range(1 << len(later))]
    row_sets = [[dg + 1 for dg in staying], staying] if owners > 1 else [[0]]
    row_block = rows // owners
    column_block = columns // copies
    mine = lax.axis_index("group")
    here = lax.axis_index("dp")
    if column_block % 128 or row_block % 16:
        ordered = jnp.concatenate(
            [
                lax.dynamic_slice_in_dim(
                    right, (here ^ spread_bits(p, column_masks)) * column_block, column_block, 1
                )
                for p in range(copies)
            ],
            axis=1,
        )
        return [
            jnp.stack(
                [
                    contract_rows(
                        lax.dynamic_slice_in_dim(left, (mine ^ dg) * row_block, row_block, 1),
                        ordered,
                    ).astype(jnp.bfloat16)
                    for dg in row_set
                ]
            )
            for row_set in row_sets
        ]
    wide = 2 if column_block % 256 and copies % 2 == 0 else 1

    def body(where, left_ref, *rest):
        rights, outs, turned = rest[:wide], rest[wide:-1], rest[-1]

        @pl.when(pl.program_id(0) == 0)
        def _():
            turned[...] = left_ref[...].T

        block = jnp.concatenate([ref[...] for ref in rights], axis=1)
        for out, row_set in zip(outs, row_sets):
            for k, dg in enumerate(row_set):
                start = pl.multiple_of((where[0] ^ dg) * row_block, row_block)
                out[k] = jnp.dot(
                    turned[pl.ds(start, row_block), :],
                    block,
                    preferred_element_type=jnp.float32,
                ).astype(jnp.bfloat16)

    def right_spec(j):
        return pl.BlockSpec(
            (tokens, column_block),
            lambda p, where: (0, where[1] ^ spread_bits(p * wide + j, column_masks)),
        )

    return pl.pallas_call(
        body,
        out_shape=[
            jax.ShapeDtypeStruct((len(row_set), row_block, columns), jnp.bfloat16)
            for row_set in row_sets
        ],
        grid_spec=pltpu.PrefetchScalarGridSpec(
            num_scalar_prefetch=1,
            grid=(copies // wide,),
            in_specs=[pl.BlockSpec((tokens, rows), lambda p, where: (0, 0))]
            + [right_spec(j) for j in range(wide)],
            out_specs=[
                pl.BlockSpec(
                    (len(row_set), row_block, column_block * wide), lambda p, where: (0, 0, p)
                )
                for row_set in row_sets
            ],
            scratch_shapes=[pltpu.VMEM((rows, tokens), jnp.bfloat16)],
        ),
        compiler_params=pltpu.CompilerParams(vmem_limit_bytes=48 * 1024 * 1024),
        cost_estimate=pl.CostEstimate(
            flops=2 * tokens * rows * columns,
            bytes_accessed=2 * (tokens * rows + tokens * columns + rows * columns),
            transcendentals=0,
        ),
    )(jnp.stack([mine, here]).astype(jnp.int32), left, *[right] * wide)


class GradSum:
    def __init__(self, left, right, split):
        blocks = grad_blocks(left, right)
        self.blocks = blocks
        group = [("group", m) for m in bit_masks(lax.axis_size("group"))]
        other = [("dp", m) for m in bit_masks(lax.axis_size("dp"))]
        self.arrays = [blocks[-1]]
        if group:
            self.arrays.append(swap(blocks[0], "group", 1))
        rest = group[1:]
        self.orders = [rest + other]
        if split:
            self.orders.append(other[:1] + rest + other[1:])
        count = len(self.orders)
        deep, tall, width = blocks[-1].shape
        size = tall // count
        self.parts = [
            [(k, [(0, deep), (i * size, (i + 1) * size), (0, width)]) for k in range(len(self.arrays))]
            for i in range(count)
        ]
        self.common = len(rest) + 1
        self.length = len(rest) + len(other)
        self.step = 0

    def hold(self, *others):
        self.arrays = list(lax.optimization_barrier((self.arrays, others))[0])

    def read(self, part):
        total = 0.0
        for k, ranges in part:
            at = tuple(slice(*r) for r in ranges)
            total = total + self.arrays[k][at].astype(jnp.float32)
        return total

    def exchange(self, away, axis, mask):
        self.arrays.append(swap(away, axis, mask))
        return len(self.arrays) - 1

    def advance(self):
        if self.step == self.length:
            return []
        outgoing = []
        for i, order in enumerate(self.orders):
            axis, mask = order[self.step]
            dim = 0 if axis == "group" else 2
            far, near = [], []
            for k, ranges in self.parts[i]:
                start, stop = ranges[dim]
                middle = (start + stop) // 2
                near.append((k, ranges[:dim] + [(start, middle)] + ranges[dim + 1 :]))
                far.append((k, ranges[:dim] + [(middle, stop)] + ranges[dim + 1 :]))
            self.parts[i] = near
            outgoing.append((self.read(far).astype(jnp.bfloat16), axis, mask))
        deep, tall, width = outgoing[0][0].shape
        if self.step >= self.common:
            away = jnp.concatenate([v for v, _, _ in outgoing], axis=1)
            sent = [away]
            k = self.exchange(away, *outgoing[0][1:])
            for i, part in enumerate(self.parts):
                part.append((k, [(0, deep), (i * tall, (i + 1) * tall), (0, width)]))
        else:
            sent = [v for v, _, _ in outgoing]
            for i, (away, axis, mask) in enumerate(outgoing):
                k = self.exchange(away, axis, mask)
                deep, tall, width = away.shape
                self.parts[i].append((k, [(0, deep), (0, tall), (0, width)]))
        self.step += 1
        return sent

    def finish(self):
        while self.step < self.length:
            self.advance()
        return jnp.concatenate([self.read(part)[0] for part in self.parts], axis=0)


def gather_grad(own, last):
    held = own.astype(jnp.bfloat16)[None]
    deltas = [0]
    groups = [(held, deltas)]
    masks = list(reversed(bit_masks(lax.axis_size("dp"))))
    for i, mask in enumerate(masks):
        away = held if last is None or i + 1 < len(masks) else after(held, last)
        got = swap(away, "dp", mask)
        got_deltas = [d ^ mask for d in deltas]
        if i + 1 < len(masks):
            held = jnp.concatenate([held, got], axis=0)
            deltas = deltas + got_deltas
            groups = [(held, deltas)]
        else:
            groups.append((got, got_deltas))
    return groups


def adam_core(master, first_moment, second_moment, clipped, step_rate, decay_rate):
    first_new = BETA_ONE * first_moment + (1.0 - BETA_ONE) * clipped
    second_new = BETA_TWO * second_moment + (1.0 - BETA_TWO) * clipped * clipped
    first_hat = first_new * (1.0 / (1.0 - BETA_ONE**STEP_COUNT))
    second_hat = second_new * (1.0 / (1.0 - BETA_TWO**STEP_COUNT))
    renewed = master - step_rate * (
        first_hat / (jnp.sqrt(second_hat) + ADAM_EPS) + decay_rate * master
    )
    return renewed, first_new, second_new


def adam_blocks(master, moment, blocks, factor, step_rate, decay_rate):
    rows, columns = master.shape
    copies = lax.axis_size("dp")
    here = lax.axis_index("dp")
    width = columns // copies
    if width % 128:
        full = jnp.zeros(master.shape, jnp.float32)
        for value, deltas in blocks:
            for k, dd in enumerate(deltas):
                full = lax.dynamic_update_slice(
                    full, value[k].astype(jnp.float32), (0, (here ^ dd) * width)
                )
        return adam_update(master, moment, full, factor, step_rate, decay_rate)
    tile = rows
    while tile % 32 == 0 and tile * columns > 256 * 1024:
        tile //= 2

    def body(where, factor_ref, master_ref, moment_ref, *rest):
        grads, (new_ref, state_ref) = rest[:-2], rest[-2:]
        scale = factor_ref[0, 0]
        for grad, (_, deltas) in zip(grads, blocks):
            for k, dd in enumerate(deltas):
                at = pl.ds(pl.multiple_of((where[0] ^ dd) * width, 128), width)
                renewed, first_new, second_new = adam_core(
                    master_ref[:, at],
                    moment_ref[0, :, at],
                    moment_ref[1, :, at],
                    grad[k].astype(jnp.float32) * scale,
                    step_rate,
                    decay_rate,
                )
                new_ref[:, at] = renewed
                state_ref[0, :, at] = first_new
                state_ref[1, :, at] = second_new

    return pl.pallas_call(
        body,
        out_shape=[
            jax.ShapeDtypeStruct(master.shape, jnp.float32),
            jax.ShapeDtypeStruct(moment.shape, jnp.float32),
        ],
        grid_spec=pltpu.PrefetchScalarGridSpec(
            num_scalar_prefetch=1,
            grid=(rows // tile,),
            in_specs=[
                pl.BlockSpec(memory_space=pltpu.SMEM),
                pl.BlockSpec((tile, columns), lambda i, where: (i, 0)),
                pl.BlockSpec((2, tile, columns), lambda i, where: (0, i, 0)),
            ]
            + [
                pl.BlockSpec((len(deltas), tile, width), lambda i, where: (0, i, 0))
                for _, deltas in blocks
            ],
            out_specs=[
                pl.BlockSpec((tile, columns), lambda i, where: (i, 0)),
                pl.BlockSpec((2, tile, columns), lambda i, where: (0, i, 0)),
            ],
        ),
        compiler_params=pltpu.CompilerParams(vmem_limit_bytes=48 * 1024 * 1024),
        cost_estimate=pl.CostEstimate(
            flops=20 * rows * columns,
            bytes_accessed=26 * rows * columns,
            transcendentals=rows * columns,
        ),
    )(
        here.reshape(1).astype(jnp.int32),
        factor.reshape(1, 1),
        master,
        moment,
        *[value for value, _ in blocks],
    )


def adam_update(master, moment, gradient, factor, step_rate, decay_rate):
    clipped = gradient * factor
    first_moment = BETA_ONE * moment[0] + (1.0 - BETA_ONE) * clipped
    second = BETA_TWO * moment[1] + (1.0 - BETA_TWO) * clipped * clipped
    first_hat = first_moment / (1.0 - BETA_ONE**STEP_COUNT)
    second_hat = second / (1.0 - BETA_TWO**STEP_COUNT)
    renewed = master - step_rate * (
        first_hat / (jnp.sqrt(second_hat) + ADAM_EPS) + decay_rate * master
    )
    return (renewed, jnp.stack([first_moment, second]))


def head_forward(raw, gain, cosine, sine):
    root = lax.rsqrt(jnp.mean(raw * raw, axis=-1, keepdims=True) + EPS_NORM)
    normed = raw * root
    scaled = normed * gain
    turned = scaled * cosine + pltpu.roll(scaled, HD // 2, 1) * sine
    return turned.astype(jnp.bfloat16), normed, root


def head_backward(grad, normed, root, gain, cosine, sine):
    turned = grad * cosine - pltpu.roll(grad, HD // 2, 1) * sine
    grad_gain = jnp.sum(turned * normed, axis=0, keepdims=True)
    scaled = turned * gain
    raw = root * (scaled - normed * jnp.mean(normed * scaled, axis=-1, keepdims=True))
    return raw, grad_gain


SPAN = 256


def fill_bias(bias_ref, row_ref, col_ref):
    key_at = lax.broadcasted_iota(jnp.int32, (SEQ_LEN, SEQ_LEN), 0)
    query_at = lax.broadcasted_iota(jnp.int32, (SEQ_LEN, SEQ_LEN), 1)
    allowed = (key_at <= query_at) & (col_ref[...] == row_ref[...])
    bias_ref[...] = jnp.where(allowed, 0.0, MASKED)


def span_weights(query_low, key_low, bias_ref, start):
    stop = start + SPAN
    scores = lax.dot_general(
        key_low[:stop],
        query_low[start:stop],
        (((1,), (1,)), ((), ())),
        preferred_element_type=jnp.float32,
    ) * (1.0 / math.sqrt(HD))
    scores = scores + bias_ref[:stop, start:stop]
    raised = jnp.exp(scores - jnp.max(scores, axis=0, keepdims=True))
    return raised * (1.0 / jnp.sum(raised, axis=0, keepdims=True))


def attend_body(
    query_ref, key_ref, value_ref, cos_ref, sin_ref, row_ref, col_ref, gain_ref, out_ref, bias_ref
):
    @pl.when(pl.program_id(1) == 0)
    def _():
        fill_bias(bias_ref, row_ref, col_ref)

    cosine, sine = cos_ref[...], sin_ref[...]
    key_low, _, _ = head_forward(key_ref[...], gain_ref[1:2, :], cosine, sine)
    value_turned = value_ref[...].astype(jnp.bfloat16).T
    for g in range(HQ // HK):
        at = slice(g * HD, (g + 1) * HD)
        query_low, _, _ = head_forward(query_ref[:, at], gain_ref[0:1, :], cosine, sine)
        for start in range(0, SEQ_LEN, SPAN):
            stop = start + SPAN
            weights = span_weights(query_low, key_low, bias_ref, start)
            mixed = jnp.dot(
                value_turned[:, :stop],
                weights.astype(jnp.bfloat16),
                preferred_element_type=jnp.float32,
            )
            out_ref[start:stop, at] = mixed.T.astype(jnp.bfloat16)


def attend_back_body(
    query_ref, key_ref, value_ref, cos_ref, sin_ref, row_ref, col_ref, gain_ref, grad_ref,
    *rest,
    first,
):
    out_ref, gain_out_ref, bias_ref = rest[-3:]
    head = pl.program_id(1) + first

    @pl.when(head == first)
    def _():
        fill_bias(bias_ref, row_ref, col_ref)

    cosine, sine = cos_ref[...], sin_ref[...]
    inv_head = 1.0 / math.sqrt(HD)

    @pl.when((pl.program_id(0) == 0) & (head == first))
    def _():
        gain_out_ref[...] = jnp.zeros_like(gain_out_ref)

    if len(rest) == 4:

        @pl.when(head == first)
        def _():
            out_ref[...] = rest[0][...]

    key_low, key_normed, key_root = head_forward(key_ref[...], gain_ref[1:2, :], cosine, sine)
    value_low = value_ref[...].astype(jnp.bfloat16)
    key_turned = key_low.T
    grad_key = [jnp.zeros((SPAN, HD), jnp.float32)] * (SEQ_LEN // SPAN)
    grad_value = list(grad_key)
    gain_query = jnp.zeros((1, HD), jnp.float32)
    for g in range(HQ // HK):
        at = slice(g * HD, (g + 1) * HD)
        query_low, normed, root = head_forward(query_ref[:, at], gain_ref[0:1, :], cosine, sine)
        grad_query = []
        for start in range(0, SEQ_LEN, SPAN):
            stop = start + SPAN
            weights = span_weights(query_low, key_low, bias_ref, start)
            grad_out = grad_ref[start:stop, at]
            grad_weights = lax.dot_general(
                value_low[:stop],
                grad_out,
                (((1,), (1,)), ((), ())),
                preferred_element_type=jnp.float32,
            )
            more_value = jnp.dot(
                weights.astype(jnp.bfloat16), grad_out, preferred_element_type=jnp.float32
            )
            product = weights * grad_weights
            grad_scores = (
                weights * (grad_weights - jnp.sum(product, axis=0, keepdims=True))
            ).astype(jnp.bfloat16)
            more_key = jnp.dot(
                grad_scores, query_low[start:stop], preferred_element_type=jnp.float32
            )
            grad_query.append(
                jnp.dot(
                    key_turned[:, :stop], grad_scores, preferred_element_type=jnp.float32
                ).T
            )
            for j in range(stop // SPAN):
                part = slice(j * SPAN, (j + 1) * SPAN)
                grad_key[j] = grad_key[j] + more_key[part]
                grad_value[j] = grad_value[j] + more_value[part]
        raw, more_gain = head_backward(
            jnp.concatenate(grad_query, axis=0) * inv_head,
            normed,
            root,
            gain_ref[0:1, :],
            cosine,
            sine,
        )
        gain_query = gain_query + more_gain
        place = pl.multiple_of((head * (HQ // HK) + g) * HD, HD)
        out_ref[:, pl.ds(place, HD)] = raw.astype(jnp.bfloat16)
    raw, gain_key = head_backward(
        jnp.concatenate(grad_key, axis=0) * inv_head,
        key_normed,
        key_root,
        gain_ref[1:2, :],
        cosine,
        sine,
    )
    out_ref[:, pl.ds(pl.multiple_of((HQ + head) * HD, HD), HD)] = raw.astype(jnp.bfloat16)
    out_ref[:, pl.ds(pl.multiple_of((HQ + HK + head) * HD, HD), HD)] = jnp.concatenate(
        grad_value, axis=0
    ).astype(jnp.bfloat16)
    gain_out_ref[0:1, :] += gain_query
    gain_out_ref[1:2, :] += gain_key


def attention_call(body, projected, tables, segments, gains, grad_out, first, count, base):
    token_rows = projected.shape[0]
    seq_count = token_rows // SEQ_LEN
    groups = HQ // HK
    wide = groups * HD
    full = lambda s, h: (s, 0)
    in_specs = [
        pl.BlockSpec((SEQ_LEN, wide), lambda s, h: (s, first + h)),
        pl.BlockSpec((SEQ_LEN, HD), lambda s, h: (s, HQ + first + h)),
        pl.BlockSpec((SEQ_LEN, HD), lambda s, h: (s, HQ + HK + first + h)),
        pl.BlockSpec((SEQ_LEN, HD), full),
        pl.BlockSpec((SEQ_LEN, HD), full),
        pl.BlockSpec((1, SEQ_LEN), lambda s, h: (0, s)),
        pl.BlockSpec((SEQ_LEN, 1), full),
        pl.BlockSpec((2, HD), lambda s, h: (0, 0)),
    ]
    operands = [
        projected,
        projected,
        projected,
        *tables,
        segments[None, :],
        segments[:, None],
        gains,
    ]
    pairs = token_rows * SEQ_LEN * groups * count
    aliases = {}
    if grad_out is None:
        out_specs = pl.BlockSpec((SEQ_LEN, wide), lambda s, h: (s, first + h))
        out_shape = jax.ShapeDtypeStruct((token_rows, HQ * HD), jnp.bfloat16)
    else:
        columns = projected.shape[1]
        in_specs.append(pl.BlockSpec((SEQ_LEN, wide), lambda s, h: (s, first + h)))
        operands.append(grad_out)
        body = functools.partial(body, first=first)
        if base is not None:
            aliases = {len(operands): 0}
            in_specs.append(pl.BlockSpec((SEQ_LEN, columns), full))
            operands.append(base)
        out_specs = [
            pl.BlockSpec((SEQ_LEN, columns), full),
            pl.BlockSpec((2, HD), lambda s, h: (0, 0)),
        ]
        out_shape = [
            jax.ShapeDtypeStruct((token_rows, columns), jnp.bfloat16),
            jax.ShapeDtypeStruct((2, HD), jnp.float32),
        ]
    return pl.pallas_call(
        body,
        grid=(seq_count, count),
        in_specs=in_specs,
        out_specs=out_specs,
        out_shape=out_shape,
        input_output_aliases=aliases,
        scratch_shapes=[pltpu.VMEM((SEQ_LEN, SEQ_LEN), jnp.float32)],
        compiler_params=pltpu.CompilerParams(vmem_limit_bytes=48 * 1024 * 1024),
        cost_estimate=pl.CostEstimate(
            flops=(4 if grad_out is None else 10) * pairs * HD * 2,
            bytes_accessed=projected.size * 6,
            transcendentals=pairs,
        ),
    )(*operands)


def gate_up_back(cotangent, full_down, gate_up):
    tokens, columns = cotangent.shape
    block = 512
    steps = FF // block

    def body(cot_ref, down_ref, gate_ref, up_ref, out_ref):
        at = pl.program_id(0) * block
        grad = lax.dot_general(
            cot_ref[...],
            down_ref[...],
            (((1,), (1,)), ((), ())),
            preferred_element_type=jnp.float32,
        )
        gate = gate_ref[...]
        part = jax.nn.sigmoid(gate)
        grad_gate = grad * up_ref[...] * part * (1.0 + gate * (1.0 - part))
        grad_up = grad * gate * part
        out_ref[:, pl.ds(pl.multiple_of(at, block), block)] = grad_gate.astype(jnp.bfloat16)
        out_ref[:, pl.ds(pl.multiple_of(at + FF, block), block)] = grad_up.astype(jnp.bfloat16)

    return pl.pallas_call(
        body,
        grid=(steps,),
        in_specs=[
            pl.BlockSpec((tokens, columns), lambda j: (0, 0)),
            pl.BlockSpec((block, columns), lambda j: (j, 0)),
            pl.BlockSpec((tokens, block), lambda j: (0, j)),
            pl.BlockSpec((tokens, block), lambda j: (0, steps + j)),
        ],
        out_specs=pl.BlockSpec((tokens, 2 * FF), lambda j: (0, 0)),
        out_shape=jax.ShapeDtypeStruct((tokens, 2 * FF), jnp.bfloat16),
        compiler_params=pltpu.CompilerParams(vmem_limit_bytes=48 * 1024 * 1024),
        cost_estimate=pl.CostEstimate(
            flops=2 * tokens * FF * columns,
            bytes_accessed=2 * FF * columns + 12 * tokens * FF,
            transcendentals=tokens * FF,
        ),
    )(cotangent, full_down, gate_up, gate_up)


def on_device(
    tokens,
    segment_ids,
    positions,
    cotangent,
    qkv_weight,
    out_weight,
    gate_up_weight,
    down_weight,
    norm_gains,
    head_gains,
    qkv_moments,
    out_moments,
    gate_up_moments,
    down_moments,
    norm_moments,
    head_moments,
):
    width = norm_gains.shape[1]
    gains_low = jnp.concatenate([norm_gains, head_gains], axis=1).astype(jnp.bfloat16)
    owners = lax.axis_size("group")
    gains_all = gather_small(gains_low).reshape(2, owners, -1)
    full_norm = gains_all[:, :, :width].reshape(2, -1)
    full_head = gains_all[:, :, width:].reshape(2, -1)
    full_qkv, first, _, late = gather_rows(qkv_weight, None, None, None, None)
    gain_one = full_norm[0].astype(jnp.float32)
    gain_two = full_norm[1].astype(jnp.float32)
    head_gain = full_head.astype(jnp.float32)
    inputs = tokens.astype(jnp.float32)
    root_one = lax.rsqrt(jnp.mean(inputs * inputs, axis=-1, keepdims=True) + EPS_NORM)
    normed_one = inputs * root_one
    hidden_one = (normed_one * gain_one).astype(jnp.bfloat16)
    projected = jnp.dot(hidden_one, full_qkv, preferred_element_type=jnp.float32)
    full_out, _, late, _ = gather_rows(out_weight, first, late, None, projected)
    full_gate_up, _, late, _ = gather_rows(gate_up_weight, first, late, projected, None)
    full_down, _, _, _ = gather_rows(down_weight, first, late, None, None)
    tables = rotary_tables(positions, HD)
    mixed_low = attention_call(attend_body, projected, tables, segment_ids, head_gain, None, 0, HK, None)
    attended = jnp.dot(mixed_low, full_out, preferred_element_type=jnp.float32)
    residual = inputs + attended
    root_two = lax.rsqrt(jnp.mean(residual * residual, axis=-1, keepdims=True) + EPS_NORM)
    normed_two = residual * root_two
    hidden_two = (normed_two * gain_two).astype(jnp.bfloat16)
    gate_up = jnp.dot(hidden_two, full_gate_up, preferred_element_type=jnp.float32)
    gate_part = gate_up[:, :FF]
    upward = gate_up[:, FF:]
    sigmoid_gate = jax.nn.sigmoid(gate_part)
    activated = (gate_part * sigmoid_gate * upward).astype(jnp.bfloat16)
    branch = jnp.dot(activated, full_down, preferred_element_type=jnp.float32)
    output = (residual + branch).astype(jnp.bfloat16)
    upstream = cotangent.astype(jnp.float32)
    down_sum = GradSum(activated, cotangent, True)
    grad_gate_up = gate_up_back(after(cotangent, *down_sum.blocks), full_down, gate_up)
    gate_up_sum = GradSum(hidden_two, after(grad_gate_up, *down_sum.advance()), True)
    grad_hidden_two = contract_cols(after(grad_gate_up, *gate_up_sum.blocks), full_gate_up)
    grad_gain_two = jnp.sum(grad_hidden_two * normed_two, axis=0)
    grad_residual = upstream + norm_back(grad_hidden_two, normed_two, root_two, gain_two)
    residual_low = grad_residual.astype(jnp.bfloat16)
    down_sum.hold(residual_low)
    sent = down_sum.advance() + gate_up_sum.advance()
    out_sum = GradSum(mixed_low, after(residual_low, *sent), True)
    down_sum.hold(out_sum.blocks)
    grad_mixed = contract_cols(
        after(residual_low, *out_sum.blocks, *down_sum.advance()), full_out
    ).astype(jnp.bfloat16)
    grad_mixed = after(grad_mixed, *out_sum.advance())
    half = HK // 2
    grad_half, gain_half = attention_call(
        attend_back_body, projected, tables, segment_ids, head_gain, grad_mixed, 0, half, None
    )
    gate_up_sum.hold(grad_half)
    down_sum.hold(grad_half)
    sent = gate_up_sum.advance() + down_sum.advance()
    grad_projected, grad_gain_head = attention_call(
        attend_back_body,
        projected,
        tables,
        segment_ids,
        head_gain,
        grad_mixed,
        half,
        HK - half,
        after(grad_half, *sent),
    )
    grad_gain_head = grad_gain_head + gain_half
    gate_up_sum.hold(grad_projected)
    out_sum.hold(grad_projected)
    sent = gate_up_sum.advance() + out_sum.advance()
    qkv_sum = GradSum(hidden_one, after(grad_projected, *sent), True)
    gate_up_sum.hold(qkv_sum.blocks)
    sent = qkv_sum.advance()
    gate_up_sum.hold(sent)
    out_sum.hold(sent)
    down_sum.hold(sent)
    sent = sent + gate_up_sum.advance() + out_sum.advance()
    grad_hidden_one = contract_cols(after(grad_projected, *qkv_sum.blocks, *sent), full_qkv)
    grad_gain_one = jnp.sum(grad_hidden_one * normed_one, axis=0)
    grad_inputs = grad_residual + norm_back(grad_hidden_one, normed_one, root_one, gain_one)
    tokens_grad = grad_inputs.astype(jnp.bfloat16)
    small = jnp.concatenate(
        [jnp.stack([grad_gain_one, grad_gain_two]), grad_gain_head],
        axis=1,
    )
    owned = tuple(v.finish() for v in (qkv_sum, out_sum, gate_up_sum, down_sum))
    qkv_own, out_own, gate_up_own, down_own = owned
    down_gathered = gather_grad(down_own, None)
    local = sum(jnp.sum(v * v) for v in owned)
    partial = jnp.concatenate(
        [small, jnp.full((6, small.shape[1]), local, jnp.float32)], axis=0
    )
    summed = sum_all(after(partial, down_gathered[0][0]))
    small = summed[:2]
    norm_total = small[:, :-HD]
    head_total = small[:, -HD:]
    squares = summed[2, 0] + jnp.sum(small * small)
    clip_limit = math.sqrt(PARAMS)
    factor = clip_limit / jnp.maximum(jnp.sqrt(squares), clip_limit)
    gathered = [
        gather_grad(after(qkv_own, summed), None),
        gather_grad(out_own, None),
        gather_grad(gate_up_own, summed),
        down_gathered,
    ]
    masters = (qkv_weight, out_weight, gate_up_weight, down_weight)
    moments = (qkv_moments, out_moments, gate_up_moments, down_moments)
    later = after(factor, gathered[0][0][0])
    renewed = [
        adam_blocks(master, moment, blocks, scale, LEARN_RATE, WEIGHT_DECAY)
        for master, moment, blocks, scale in zip(
            masters, moments, gathered, (later, later, later, factor)
        )
    ]
    mine = lax.axis_index("group")
    norm_grad = lax.dynamic_slice_in_dim(
        norm_total, mine * norm_gains.shape[1], norm_gains.shape[1], 1
    )
    head_grad = lax.dynamic_slice_in_dim(
        head_total, mine * head_gains.shape[1], head_gains.shape[1], 1
    )
    renewed.append(adam_update(norm_gains, norm_moments, norm_grad, factor, GAIN_RATE, 0.0))
    renewed.append(adam_update(head_gains, head_moments, head_grad, factor, GAIN_RATE, 0.0))
    return (
        output,
        tokens_grad,
        *owned,
        norm_grad,
        head_grad,
        *[new for new, _ in renewed],
        *[state for _, state in renewed],
    )


def solution(mesh):
    placed = (
        P(("dp", "group"), None),
        P(("dp", "group")),
        P(("dp", "group")),
        P(("dp", "group"), None),
        P("group", None),
        P("group", None),
        P("group", None),
        P("group", None),
        P(None, "group"),
        P(None, "group"),
        P(None, "group", None),
        P(None, "group", None),
        P(None, "group", None),
        P(None, "group", None),
        P(None, None, "group"),
        P(None, None, "group"),
    )
    return jax.shard_map(
        on_device,
        mesh=mesh,
        in_specs=placed,
        out_specs=(
            P(("dp", "group"), None),
            P(("dp", "group"), None),
            P("group", "dp"),
            P("group", "dp"),
            P("group", "dp"),
            P("group", "dp"),
            P(None, "group"),
            P(None, "group"),
            P("group", None),
            P("group", None),
            P("group", None),
            P("group", None),
            P(None, "group"),
            P(None, "group"),
            P(None, "group", None),
            P(None, "group", None),
            P(None, "group", None),
            P(None, "group", None),
            P(None, None, "group"),
            P(None, None, "group"),
        ),
        check_vma=False,
    )
```

```python
import functools
import math

import jax
import jax.numpy as jnp
from jax import lax
from jax.experimental import pallas as pl
from jax.experimental.pallas import tpu as pltpu
from jax.sharding import PartitionSpec as P


HQ = 16
HK = 8
HD = 128
FF = 3072
SEQ_LEN = 512
PARAMS = 15730944
GROUP = "group"
DP = "dp"


EPS_NORM = 1e-06
ROPE_BASE = 1000000.0
MASKED = -1e30
LEARN_RATE = 0.03
GAIN_RATE = 0.3
WEIGHT_DECAY = 0.1
BETA_ONE = 0.9
BETA_TWO = 0.95
ADAM_EPS = 1e-08
STEP_COUNT = 3.0


def rotary_tables(places, width):
    half_width = width // 2
    frequency = ROPE_BASE ** (-(jnp.arange(half_width, dtype=jnp.float32) * 2.0) / width)
    angles = places.astype(jnp.float32)[:, None] * frequency[None, :]
    cosine, sine = jnp.cos(angles), jnp.sin(angles)
    return (
        jnp.concatenate([cosine, cosine], axis=1),
        jnp.concatenate([-sine, sine], axis=1),
    )


def contract_rows(left_side, right_side):
    return lax.dot_general(
        left_side, right_side, (((0,), (0,)), ((), ())), preferred_element_type=jnp.float32
    )


def contract_cols(left_side, right_side):
    return lax.dot_general(
        left_side, right_side, (((1,), (1,)), ((), ())), preferred_element_type=jnp.float32
    )


def norm_back(grad_out, normed, inv_root, gain):
    scaled = grad_out * gain
    return inv_root * (scaled - normed * jnp.mean(normed * scaled, axis=-1, keepdims=True))


def swap(value, axis, mask):
    count = lax.axis_size(axis)
    return lax.ppermute(value, axis, [(i, i ^ mask) for i in range(count)])


def bit_masks(count):
    return [1 << i for i in range(count.bit_length() - 1)]


def after(value, *others):
    return lax.optimization_barrier((value, others))[0]


def place_rows(pieces, rows, owners):
    columns = pieces[0][0].shape[1]
    kind = pieces[0][0].dtype
    sizes = [v.shape[0] for v, _, _ in pieces]

    def body(*refs):
        count = len(pieces)
        ins, out_ref, held = refs[:count], refs[count], refs[count + 1]
        into, away = refs[count + 2 :]
        mine = lax.axis_index(GROUP)
        here = lax.axis_index(DP)
        arriving, leaving, at = [], [], 0
        for k, (_, delta, offset) in enumerate(pieces):
            slot = held.at[pl.ds(at, sizes[k])]
            start = pl.multiple_of((mine ^ delta) * rows + offset(here), 16)
            arriving.append(pltpu.make_async_copy(ins[k], slot, into.at[k]))
            leaving.append(
                pltpu.make_async_copy(slot, out_ref.at[pl.ds(start, sizes[k])], away.at[k])
            )
            at += sizes[k]
        for copy in arriving:
            copy.start()
        for first, second in zip(arriving, leaving):
            first.wait()
            second.start()
        for copy in leaving:
            copy.wait()

    return pl.pallas_call(
        body,
        out_shape=jax.ShapeDtypeStruct((rows * owners, columns), kind),
        in_specs=[pl.BlockSpec(memory_space=pl.ANY)] * len(pieces),
        out_specs=pl.BlockSpec(memory_space=pl.ANY),
        scratch_shapes=[
            pltpu.VMEM((rows * owners, columns), kind),
            pltpu.SemaphoreType.DMA((len(pieces),)),
            pltpu.SemaphoreType.DMA((len(pieces),)),
        ],
        compiler_params=pltpu.CompilerParams(vmem_limit_bytes=32 * 1024 * 1024),
        cost_estimate=pl.CostEstimate(
            flops=0, bytes_accessed=4 * rows * owners * columns, transcendentals=0
        ),
    )(*[v for v, _, _ in pieces])


def gather_rows(shard, early, late, middle, hold):
    owners = lax.axis_size(GROUP)
    copies = lax.axis_size(DP)
    here = lax.axis_index(DP)
    if early is not None:
        shard = after(shard, early)
    shard = shard.astype(jnp.bfloat16)
    rows, _ = shard.shape

    def none(_):
        return 0

    pieces = [(shard, 0, none)]
    near = order = by_one = by_two = shard
    if owners == 4 and copies % 4 == 0 and rows % 128 == 0:
        quarter, half = rows // 4, rows // 8

        def place(here):
            return (here & 1) * 2 + ((here >> 1) & 1)

        def quarter_at(mask, more=0):
            return lambda here: (place(here) ^ mask) * quarter + more

        near = lax.dynamic_slice_in_dim(shard, place(here) * quarter, quarter, 0)
        if late is not None:
            near = after(near, late)
        order = swap(near, GROUP, 2)
        passed = order if middle is None else after(order, middle)
        by_one = swap(passed, DP, 1)
        by_two = swap(passed, DP, 2)
        last_one = swap(by_two[:half], DP, 1)
        last_two = swap(by_one[half:], DP, 2)
        pieces += [
            (order, 2, quarter_at(0)),
            (by_one, 2, quarter_at(2)),
            (by_two, 2, quarter_at(1)),
            (last_one, 2, quarter_at(3)),
            (last_two, 2, quarter_at(3, half)),
        ]
    else:
        for mask in bit_masks(owners)[1:]:
            pieces += [(swap(v, GROUP, mask), dg ^ mask, at) for v, dg, at in pieces]
    pieces += [(swap(v, GROUP, 1), dg ^ 1, at) for v, dg, at in pieces]
    if hold is not None:
        pieces[0] = (after(shard, hold), 0, none)
    return place_rows(pieces, rows, owners), near, order, (by_one, by_two)


def gather_small(shard):
    owners = lax.axis_size(GROUP)
    mine = lax.axis_index(GROUP)
    width = shard.shape[1]
    held = shard[None]
    deltas = [0]
    for mask in reversed(bit_masks(owners)):
        held = jnp.concatenate([held, swap(held, GROUP, mask)], axis=0)
        deltas += [d ^ mask for d in deltas]
    full = jnp.zeros((shard.shape[0], width * owners), shard.dtype)
    for k, delta in enumerate(deltas):
        full = lax.dynamic_update_slice(full, held[k], (0, (mine ^ delta) * width))
    return full


def sum_all(value):
    owners = lax.axis_size(GROUP)
    copies = lax.axis_size(DP)
    mesh_type = pl.DeviceIdType.MESH

    def body(in_ref, out_ref, near, near_sum, far, near_send, near_recv, far_send, far_recv):
        mine = lax.axis_index(GROUP)
        here = lax.axis_index(DP)
        near_peers = [(here, mine ^ k) for k in range(1, owners)]
        far_peers = [(here ^ k, mine) for k in range(1, copies)]
        barrier = pltpu.get_barrier_semaphore()
        for peer in near_peers + far_peers:
            pl.semaphore_signal(barrier, inc=1, device_id=peer, device_id_type=mesh_type)
        pl.semaphore_wait(barrier, len(near_peers) + len(far_peers))

        def exchange(source, slots, index, peers, sends, recvs):
            slots[index] = source[...]
            copies_out = [
                pltpu.make_async_remote_copy(
                    src_ref=source,
                    dst_ref=slots.at[index],
                    send_sem=sends.at[k],
                    recv_sem=recvs.at[k],
                    device_id=peer,
                    device_id_type=mesh_type,
                )
                for k, peer in enumerate(peers)
            ]
            for copy in copies_out:
                copy.start()
            for copy in copies_out:
                copy.wait()
            total = slots[0]
            for k in range(1, len(peers) + 1):
                total = total + slots[k]
            return total

        near_sum[...] = exchange(in_ref, near, mine, near_peers, near_send, near_recv)
        out_ref[...] = exchange(near_sum, far, here, far_peers, far_send, far_recv)

    shape = value.shape
    return pl.pallas_call(
        body,
        out_shape=jax.ShapeDtypeStruct(shape, jnp.float32),
        in_specs=[pl.BlockSpec(memory_space=pltpu.VMEM)],
        out_specs=pl.BlockSpec(memory_space=pltpu.VMEM),
        scratch_shapes=[
            pltpu.VMEM((owners,) + shape, jnp.float32),
            pltpu.VMEM(shape, jnp.float32),
            pltpu.VMEM((copies,) + shape, jnp.float32),
            pltpu.SemaphoreType.DMA((owners - 1,)),
            pltpu.SemaphoreType.DMA((owners - 1,)),
            pltpu.SemaphoreType.DMA((copies - 1,)),
            pltpu.SemaphoreType.DMA((copies - 1,)),
        ],
        compiler_params=pltpu.CompilerParams(collective_id=0, has_side_effects=True),
    )(value)


def spread_bits(position, masks):
    total = 0
    count = len(masks)
    for i, mask in enumerate(masks):
        total = total + ((position >> (count - 1 - i)) & 1) * mask
    return total


def grad_blocks(left, right):
    tokens, rows = left.shape
    columns = right.shape[1]
    owners = lax.axis_size(GROUP)
    copies = lax.axis_size(DP)
    column_masks = bit_masks(copies)
    later = bit_masks(owners)[1:]
    staying = [spread_bits(p, later) for p in range(1 << len(later))]
    row_sets = [[dg + 1 for dg in staying], staying] if owners > 1 else [[0]]
    row_block = rows // owners
    column_block = columns // copies
    mine = lax.axis_index(GROUP)
    here = lax.axis_index(DP)
    if column_block % 128 or row_block % 16:
        ordered = jnp.concatenate(
            [
                lax.dynamic_slice_in_dim(
                    right, (here ^ spread_bits(p, column_masks)) * column_block, column_block, 1
                )
                for p in range(copies)
            ],
            axis=1,
        )
        return [
            jnp.stack(
                [
                    contract_rows(
                        lax.dynamic_slice_in_dim(left, (mine ^ dg) * row_block, row_block, 1),
                        ordered,
                    ).astype(jnp.bfloat16)
                    for dg in row_set
                ]
            )
            for row_set in row_sets
        ]
    wide = 2 if column_block % 256 and copies % 2 == 0 else 1

    def body(where, left_ref, *rest):
        rights, outs, turned = rest[:wide], rest[wide:-1], rest[-1]

        @pl.when(pl.program_id(0) == 0)
        def _():
            turned[...] = left_ref[...].T

        block = jnp.concatenate([ref[...] for ref in rights], axis=1)
        for out, row_set in zip(outs, row_sets):
            for k, dg in enumerate(row_set):
                start = pl.multiple_of((where[0] ^ dg) * row_block, row_block)
                out[k] = jnp.dot(
                    turned[pl.ds(start, row_block), :],
                    block,
                    preferred_element_type=jnp.float32,
                ).astype(jnp.bfloat16)

    def right_spec(j):
        return pl.BlockSpec(
            (tokens, column_block),
            lambda p, where: (0, where[1] ^ spread_bits(p * wide + j, column_masks)),
        )

    return pl.pallas_call(
        body,
        out_shape=[
            jax.ShapeDtypeStruct((len(row_set), row_block, columns), jnp.bfloat16)
            for row_set in row_sets
        ],
        grid_spec=pltpu.PrefetchScalarGridSpec(
            num_scalar_prefetch=1,
            grid=(copies // wide,),
            in_specs=[pl.BlockSpec((tokens, rows), lambda p, where: (0, 0))]
            + [right_spec(j) for j in range(wide)],
            out_specs=[
                pl.BlockSpec(
                    (len(row_set), row_block, column_block * wide), lambda p, where: (0, 0, p)
                )
                for row_set in row_sets
            ],
            scratch_shapes=[pltpu.VMEM((rows, tokens), jnp.bfloat16)],
        ),
        compiler_params=pltpu.CompilerParams(vmem_limit_bytes=48 * 1024 * 1024),
        cost_estimate=pl.CostEstimate(
            flops=2 * tokens * rows * columns,
            bytes_accessed=2 * (tokens * rows + tokens * columns + rows * columns),
            transcendentals=0,
        ),
    )(jnp.stack([mine, here]).astype(jnp.int32), left, *[right] * wide)


class GradSum:
    def __init__(self, left, right, split):
        blocks = grad_blocks(left, right)
        self.blocks = blocks
        group = [(GROUP, m) for m in bit_masks(lax.axis_size(GROUP))]
        other = [(DP, m) for m in bit_masks(lax.axis_size(DP))]
        self.arrays = [blocks[-1]]
        if group:
            self.arrays.append(swap(blocks[0], GROUP, 1))
        rest = group[1:]
        self.orders = [rest + other]
        if split:
            self.orders.append(other[:1] + rest + other[1:])
        count = len(self.orders)
        deep, tall, width = blocks[-1].shape
        size = tall // count
        self.parts = [
            [(k, [(0, deep), (i * size, (i + 1) * size), (0, width)]) for k in range(len(self.arrays))]
            for i in range(count)
        ]
        self.common = len(rest) + 1
        self.length = len(rest) + len(other)
        self.step = 0

    def hold(self, *others):
        self.arrays = list(lax.optimization_barrier((self.arrays, others))[0])

    def read(self, part):
        total = 0.0
        for k, ranges in part:
            at = tuple(slice(*r) for r in ranges)
            total = total + self.arrays[k][at].astype(jnp.float32)
        return total

    def exchange(self, away, axis, mask):
        self.arrays.append(swap(away, axis, mask))
        return len(self.arrays) - 1

    def advance(self):
        if self.step == self.length:
            return []
        outgoing = []
        for i, order in enumerate(self.orders):
            axis, mask = order[self.step]
            dim = 0 if axis == GROUP else 2
            far, near = [], []
            for k, ranges in self.parts[i]:
                start, stop = ranges[dim]
                middle = (start + stop) // 2
                near.append((k, ranges[:dim] + [(start, middle)] + ranges[dim + 1 :]))
                far.append((k, ranges[:dim] + [(middle, stop)] + ranges[dim + 1 :]))
            self.parts[i] = near
            outgoing.append((self.read(far).astype(jnp.bfloat16), axis, mask))
        deep, tall, width = outgoing[0][0].shape
        if self.step >= self.common:
            away = jnp.concatenate([v for v, _, _ in outgoing], axis=1)
            sent = [away]
            k = self.exchange(away, *outgoing[0][1:])
            for i, part in enumerate(self.parts):
                part.append((k, [(0, deep), (i * tall, (i + 1) * tall), (0, width)]))
        else:
            sent = [v for v, _, _ in outgoing]
            for i, (away, axis, mask) in enumerate(outgoing):
                k = self.exchange(away, axis, mask)
                deep, tall, width = away.shape
                self.parts[i].append((k, [(0, deep), (0, tall), (0, width)]))
        self.step += 1
        return sent

    def finish(self):
        while self.step < self.length:
            self.advance()
        return jnp.concatenate([self.read(part)[0] for part in self.parts], axis=0)


def gather_grad(own, second, last):
    held = own.astype(jnp.bfloat16)[None]
    deltas = [0]
    groups = [(held, deltas)]
    masks = list(reversed(bit_masks(lax.axis_size(DP))))
    for i, mask in enumerate(masks):
        away = held
        if i == 1 and second is not None:
            away = after(away, second)
        if i + 1 == len(masks) and last is not None:
            away = after(away, last)
        got = swap(away, DP, mask)
        got_deltas = [d ^ mask for d in deltas]
        if i + 1 < len(masks):
            held = jnp.concatenate([held, got], axis=0)
            deltas = deltas + got_deltas
            groups = [(held, deltas)]
        else:
            groups.append((got, got_deltas))
    return groups


def adam_core(master, first_moment, second_moment, clipped, step_rate, decay_rate):
    first_new = BETA_ONE * first_moment + (1.0 - BETA_ONE) * clipped
    second_new = BETA_TWO * second_moment + (1.0 - BETA_TWO) * clipped * clipped
    first_hat = first_new * (1.0 / (1.0 - BETA_ONE**STEP_COUNT))
    second_hat = second_new * (1.0 / (1.0 - BETA_TWO**STEP_COUNT))
    renewed = master - step_rate * (
        first_hat / (jnp.sqrt(second_hat) + ADAM_EPS) + decay_rate * master
    )
    return renewed, first_new, second_new


def adam_blocks(master, moment, blocks, factor, step_rate, decay_rate):
    rows, columns = master.shape
    copies = lax.axis_size(DP)
    here = lax.axis_index(DP)
    width = columns // copies
    if width % 128:
        full = jnp.zeros(master.shape, jnp.float32)
        for value, deltas in blocks:
            for k, dd in enumerate(deltas):
                full = lax.dynamic_update_slice(
                    full, value[k].astype(jnp.float32), (0, (here ^ dd) * width)
                )
        return adam_update(master, moment, full, factor, step_rate, decay_rate)
    tile = rows
    while tile % 32 == 0 and tile * columns > 256 * 1024:
        tile //= 2

    def body(where, factor_ref, master_ref, moment_ref, *rest):
        grads, (new_ref, state_ref) = rest[:-2], rest[-2:]
        scale = factor_ref[0, 0]
        for grad, (_, deltas) in zip(grads, blocks):
            for k, dd in enumerate(deltas):
                at = pl.ds(pl.multiple_of((where[0] ^ dd) * width, 128), width)
                renewed, first_new, second_new = adam_core(
                    master_ref[:, at],
                    moment_ref[0, :, at],
                    moment_ref[1, :, at],
                    grad[k].astype(jnp.float32) * scale,
                    step_rate,
                    decay_rate,
                )
                new_ref[:, at] = renewed
                state_ref[0, :, at] = first_new
                state_ref[1, :, at] = second_new

    return pl.pallas_call(
        body,
        out_shape=[
            jax.ShapeDtypeStruct(master.shape, jnp.float32),
            jax.ShapeDtypeStruct(moment.shape, jnp.float32),
        ],
        grid_spec=pltpu.PrefetchScalarGridSpec(
            num_scalar_prefetch=1,
            grid=(rows // tile,),
            in_specs=[
                pl.BlockSpec(memory_space=pltpu.SMEM),
                pl.BlockSpec((tile, columns), lambda i, where: (i, 0)),
                pl.BlockSpec((2, tile, columns), lambda i, where: (0, i, 0)),
            ]
            + [
                pl.BlockSpec((len(deltas), tile, width), lambda i, where: (0, i, 0))
                for _, deltas in blocks
            ],
            out_specs=[
                pl.BlockSpec((tile, columns), lambda i, where: (i, 0)),
                pl.BlockSpec((2, tile, columns), lambda i, where: (0, i, 0)),
            ],
        ),
        compiler_params=pltpu.CompilerParams(vmem_limit_bytes=48 * 1024 * 1024),
        cost_estimate=pl.CostEstimate(
            flops=20 * rows * columns,
            bytes_accessed=26 * rows * columns,
            transcendentals=rows * columns,
        ),
    )(
        here.reshape(1).astype(jnp.int32),
        factor.reshape(1, 1),
        master,
        moment,
        *[value for value, _ in blocks],
    )


def adam_update(master, moment, gradient, factor, step_rate, decay_rate):
    clipped = gradient * factor
    first_moment = BETA_ONE * moment[0] + (1.0 - BETA_ONE) * clipped
    second = BETA_TWO * moment[1] + (1.0 - BETA_TWO) * clipped * clipped
    first_hat = first_moment / (1.0 - BETA_ONE**STEP_COUNT)
    second_hat = second / (1.0 - BETA_TWO**STEP_COUNT)
    renewed = master - step_rate * (
        first_hat / (jnp.sqrt(second_hat) + ADAM_EPS) + decay_rate * master
    )
    return (renewed, jnp.stack([first_moment, second]))


def head_forward(raw, gain, cosine, sine):
    root = lax.rsqrt(jnp.mean(raw * raw, axis=-1, keepdims=True) + EPS_NORM)
    normed = raw * root
    scaled = normed * gain
    turned = scaled * cosine + pltpu.roll(scaled, HD // 2, 1) * sine
    return turned.astype(jnp.bfloat16), normed, root


def head_backward(grad, normed, root, gain, cosine, sine):
    turned = grad * cosine - pltpu.roll(grad, HD // 2, 1) * sine
    grad_gain = jnp.sum(turned * normed, axis=0, keepdims=True)
    scaled = turned * gain
    raw = root * (scaled - normed * jnp.mean(normed * scaled, axis=-1, keepdims=True))
    return raw, grad_gain


SPAN = 256


def fill_bias(bias_ref, row_ref, col_ref):
    key_at = lax.broadcasted_iota(jnp.int32, (SEQ_LEN, SEQ_LEN), 0)
    query_at = lax.broadcasted_iota(jnp.int32, (SEQ_LEN, SEQ_LEN), 1)
    allowed = (key_at <= query_at) & (col_ref[...] == row_ref[...])
    bias_ref[...] = jnp.where(allowed, 0.0, MASKED)


def span_weights(query_low, key_low, bias_ref, start):
    stop = start + SPAN
    scores = lax.dot_general(
        key_low[:stop],
        query_low[start:stop],
        (((1,), (1,)), ((), ())),
        preferred_element_type=jnp.float32,
    ) * (1.0 / math.sqrt(HD))
    scores = scores + bias_ref[:stop, start:stop]
    raised = jnp.exp(scores - jnp.max(scores, axis=0, keepdims=True))
    return raised * (1.0 / jnp.sum(raised, axis=0, keepdims=True))


def attend_body(
    query_ref, key_ref, value_ref, cos_ref, sin_ref, row_ref, col_ref, gain_ref, out_ref, bias_ref
):
    @pl.when(pl.program_id(1) == 0)
    def _():
        fill_bias(bias_ref, row_ref, col_ref)

    cosine, sine = cos_ref[...], sin_ref[...]
    key_low, _, _ = head_forward(key_ref[...], gain_ref[1:2, :], cosine, sine)
    value_turned = value_ref[...].astype(jnp.bfloat16).T
    for g in range(HQ // HK):
        at = slice(g * HD, (g + 1) * HD)
        query_low, _, _ = head_forward(query_ref[:, at], gain_ref[0:1, :], cosine, sine)
        for start in range(0, SEQ_LEN, SPAN):
            stop = start + SPAN
            weights = span_weights(query_low, key_low, bias_ref, start)
            mixed = jnp.dot(
                value_turned[:, :stop],
                weights.astype(jnp.bfloat16),
                preferred_element_type=jnp.float32,
            )
            out_ref[start:stop, at] = mixed.T.astype(jnp.bfloat16)


def attend_back_body(
    query_ref, key_ref, value_ref, cos_ref, sin_ref, row_ref, col_ref, gain_ref, grad_ref,
    *rest,
    first,
):
    out_ref, gain_out_ref, bias_ref = rest[-3:]
    head = pl.program_id(1) + first

    @pl.when(head == first)
    def _():
        fill_bias(bias_ref, row_ref, col_ref)

    cosine, sine = cos_ref[...], sin_ref[...]
    inv_head = 1.0 / math.sqrt(HD)

    @pl.when((pl.program_id(0) == 0) & (head == first))
    def _():
        gain_out_ref[...] = jnp.zeros_like(gain_out_ref)

    if len(rest) == 4:

        @pl.when(head == first)
        def _():
            out_ref[...] = rest[0][...]

    key_low, key_normed, key_root = head_forward(key_ref[...], gain_ref[1:2, :], cosine, sine)
    value_low = value_ref[...].astype(jnp.bfloat16)
    key_turned = key_low.T
    grad_key = [jnp.zeros((SPAN, HD), jnp.float32)] * (SEQ_LEN // SPAN)
    grad_value = list(grad_key)
    gain_query = jnp.zeros((1, HD), jnp.float32)
    for g in range(HQ // HK):
        at = slice(g * HD, (g + 1) * HD)
        query_low, normed, root = head_forward(query_ref[:, at], gain_ref[0:1, :], cosine, sine)
        grad_query = []
        for start in range(0, SEQ_LEN, SPAN):
            stop = start + SPAN
            weights = span_weights(query_low, key_low, bias_ref, start)
            grad_out = grad_ref[start:stop, at]
            grad_weights = lax.dot_general(
                value_low[:stop],
                grad_out,
                (((1,), (1,)), ((), ())),
                preferred_element_type=jnp.float32,
            )
            more_value = jnp.dot(
                weights.astype(jnp.bfloat16), grad_out, preferred_element_type=jnp.float32
            )
            product = weights * grad_weights
            grad_scores = (
                weights * (grad_weights - jnp.sum(product, axis=0, keepdims=True))
            ).astype(jnp.bfloat16)
            more_key = jnp.dot(
                grad_scores, query_low[start:stop], preferred_element_type=jnp.float32
            )
            grad_query.append(
                jnp.dot(
                    key_turned[:, :stop], grad_scores, preferred_element_type=jnp.float32
                ).T
            )
            for j in range(stop // SPAN):
                part = slice(j * SPAN, (j + 1) * SPAN)
                grad_key[j] = grad_key[j] + more_key[part]
                grad_value[j] = grad_value[j] + more_value[part]
        raw, more_gain = head_backward(
            jnp.concatenate(grad_query, axis=0) * inv_head,
            normed,
            root,
            gain_ref[0:1, :],
            cosine,
            sine,
        )
        gain_query = gain_query + more_gain
        place = pl.multiple_of((head * (HQ // HK) + g) * HD, HD)
        out_ref[:, pl.ds(place, HD)] = raw.astype(jnp.bfloat16)
    raw, gain_key = head_backward(
        jnp.concatenate(grad_key, axis=0) * inv_head,
        key_normed,
        key_root,
        gain_ref[1:2, :],
        cosine,
        sine,
    )
    out_ref[:, pl.ds(pl.multiple_of((HQ + head) * HD, HD), HD)] = raw.astype(jnp.bfloat16)
    out_ref[:, pl.ds(pl.multiple_of((HQ + HK + head) * HD, HD), HD)] = jnp.concatenate(
        grad_value, axis=0
    ).astype(jnp.bfloat16)
    gain_out_ref[0:1, :] += gain_query
    gain_out_ref[1:2, :] += gain_key


def attention_call(body, projected, tables, segments, gains, grad_out, first, count, base):
    token_rows = projected.shape[0]
    seq_count = token_rows // SEQ_LEN
    groups = HQ // HK
    wide = groups * HD
    full = lambda s, h: (s, 0)
    in_specs = [
        pl.BlockSpec((SEQ_LEN, wide), lambda s, h: (s, first + h)),
        pl.BlockSpec((SEQ_LEN, HD), lambda s, h: (s, HQ + first + h)),
        pl.BlockSpec((SEQ_LEN, HD), lambda s, h: (s, HQ + HK + first + h)),
        pl.BlockSpec((SEQ_LEN, HD), full),
        pl.BlockSpec((SEQ_LEN, HD), full),
        pl.BlockSpec((1, SEQ_LEN), lambda s, h: (0, s)),
        pl.BlockSpec((SEQ_LEN, 1), full),
        pl.BlockSpec((2, HD), lambda s, h: (0, 0)),
    ]
    operands = [
        projected,
        projected,
        projected,
        *tables,
        segments[None, :],
        segments[:, None],
        gains,
    ]
    pairs = token_rows * SEQ_LEN * groups * count
    aliases = {}
    if grad_out is None:
        out_specs = pl.BlockSpec((SEQ_LEN, wide), lambda s, h: (s, first + h))
        out_shape = jax.ShapeDtypeStruct((token_rows, HQ * HD), jnp.bfloat16)
    else:
        columns = projected.shape[1]
        in_specs.append(pl.BlockSpec((SEQ_LEN, wide), lambda s, h: (s, first + h)))
        operands.append(grad_out)
        body = functools.partial(body, first=first)
        if base is not None:
            aliases = {len(operands): 0}
            in_specs.append(pl.BlockSpec((SEQ_LEN, columns), full))
            operands.append(base)
        out_specs = [
            pl.BlockSpec((SEQ_LEN, columns), full),
            pl.BlockSpec((2, HD), lambda s, h: (0, 0)),
        ]
        out_shape = [
            jax.ShapeDtypeStruct((token_rows, columns), jnp.bfloat16),
            jax.ShapeDtypeStruct((2, HD), jnp.float32),
        ]
    return pl.pallas_call(
        body,
        grid=(seq_count, count),
        in_specs=in_specs,
        out_specs=out_specs,
        out_shape=out_shape,
        input_output_aliases=aliases,
        scratch_shapes=[pltpu.VMEM((SEQ_LEN, SEQ_LEN), jnp.float32)],
        compiler_params=pltpu.CompilerParams(vmem_limit_bytes=48 * 1024 * 1024),
        cost_estimate=pl.CostEstimate(
            flops=(4 if grad_out is None else 10) * pairs * HD * 2,
            bytes_accessed=projected.size * 6,
            transcendentals=pairs,
        ),
    )(*operands)


def gate_up_forward(hidden, full_gate_up):
    tokens, depth = hidden.shape
    block = 512
    steps = FF // block

    def body(hidden_ref, left_ref, right_ref, gate_ref, up_ref, out_ref):
        gate = jnp.dot(hidden_ref[...], left_ref[...], preferred_element_type=jnp.float32)
        upward = jnp.dot(hidden_ref[...], right_ref[...], preferred_element_type=jnp.float32)
        gate_ref[...] = gate
        up_ref[...] = upward
        out_ref[...] = (gate * jax.nn.sigmoid(gate) * upward).astype(jnp.bfloat16)

    wide = pl.BlockSpec((tokens, block), lambda j: (0, j))
    return pl.pallas_call(
        body,
        grid=(steps,),
        in_specs=[
            pl.BlockSpec((tokens, depth), lambda j: (0, 0)),
            pl.BlockSpec((depth, block), lambda j: (0, j)),
            pl.BlockSpec((depth, block), lambda j: (0, steps + j)),
        ],
        out_specs=[wide, wide, wide],
        out_shape=[
            jax.ShapeDtypeStruct((tokens, FF), jnp.float32),
            jax.ShapeDtypeStruct((tokens, FF), jnp.float32),
            jax.ShapeDtypeStruct((tokens, FF), jnp.bfloat16),
        ],
        compiler_params=pltpu.CompilerParams(vmem_limit_bytes=48 * 1024 * 1024),
        cost_estimate=pl.CostEstimate(
            flops=4 * tokens * FF * depth,
            bytes_accessed=4 * FF * depth + 10 * tokens * FF,
            transcendentals=tokens * FF,
        ),
    )(hidden, full_gate_up, full_gate_up)


def project_back(grad_low, weight, value, upstream, gain, whole):
    tokens, width = grad_low.shape
    depth = weight.shape[0]
    block = 1024
    steps = width // block

    def body(grad_ref, weight_ref, value_ref, up_ref, gain_ref, *rest):
        total_ref = rest[-1]
        step = pl.program_id(0)
        more = lax.dot_general(
            grad_ref[...],
            weight_ref[...],
            (((1,), (1,)), ((), ())),
            preferred_element_type=jnp.float32,
        )

        @pl.when(step == 0)
        def _():
            total_ref[...] = more

        @pl.when(step > 0)
        def _():
            total_ref[...] += more

        @pl.when(step == steps - 1)
        def _():
            raw = value_ref[...].astype(jnp.float32)
            root = lax.rsqrt(jnp.mean(raw * raw, axis=-1, keepdims=True) + EPS_NORM)
            normed = raw * root
            grad = total_ref[...]
            rest[1][...] = jnp.sum(grad * normed, axis=0, keepdims=True)
            full = up_ref[...].astype(jnp.float32) + norm_back(grad, normed, root, gain_ref[...])
            rest[0][...] = full.astype(jnp.bfloat16)
            if whole:
                rest[2][...] = full

    fixed = lambda j: (0, 0)
    square = pl.BlockSpec((tokens, depth), fixed)
    row = pl.BlockSpec((1, depth), fixed)
    shapes = [
        jax.ShapeDtypeStruct((tokens, depth), jnp.bfloat16),
        jax.ShapeDtypeStruct((1, depth), jnp.float32),
    ]
    if whole:
        shapes.append(jax.ShapeDtypeStruct((tokens, depth), jnp.float32))
    return pl.pallas_call(
        body,
        grid=(steps,),
        in_specs=[
            pl.BlockSpec((tokens, block), lambda j: (0, j)),
            pl.BlockSpec((depth, block), lambda j: (0, j)),
            square,
            square,
            row,
        ],
        out_specs=[square, row] + [square] * whole,
        out_shape=shapes,
        scratch_shapes=[pltpu.VMEM((tokens, depth), jnp.float32)],
        compiler_params=pltpu.CompilerParams(vmem_limit_bytes=48 * 1024 * 1024),
        cost_estimate=pl.CostEstimate(
            flops=2 * tokens * width * depth,
            bytes_accessed=2 * width * (depth + tokens) + 14 * tokens * depth,
            transcendentals=tokens,
        ),
    )(grad_low, weight, value, upstream, gain)


def gate_up_back(cotangent, full_down, gate_part, upward):
    tokens, columns = cotangent.shape
    block = 512
    steps = FF // block

    def body(cot_ref, down_ref, gate_ref, up_ref, out_ref):
        at = pl.program_id(0) * block
        grad = lax.dot_general(
            cot_ref[...],
            down_ref[...],
            (((1,), (1,)), ((), ())),
            preferred_element_type=jnp.float32,
        )
        gate = gate_ref[...]
        part = jax.nn.sigmoid(gate)
        grad_gate = grad * up_ref[...] * part * (1.0 + gate * (1.0 - part))
        grad_up = grad * gate * part
        out_ref[:, pl.ds(pl.multiple_of(at, block), block)] = grad_gate.astype(jnp.bfloat16)
        out_ref[:, pl.ds(pl.multiple_of(at + FF, block), block)] = grad_up.astype(jnp.bfloat16)

    return pl.pallas_call(
        body,
        grid=(steps,),
        in_specs=[
            pl.BlockSpec((tokens, columns), lambda j: (0, 0)),
            pl.BlockSpec((block, columns), lambda j: (j, 0)),
            pl.BlockSpec((tokens, block), lambda j: (0, j)),
            pl.BlockSpec((tokens, block), lambda j: (0, j)),
        ],
        out_specs=pl.BlockSpec((tokens, 2 * FF), lambda j: (0, 0)),
        out_shape=jax.ShapeDtypeStruct((tokens, 2 * FF), jnp.bfloat16),
        compiler_params=pltpu.CompilerParams(vmem_limit_bytes=48 * 1024 * 1024),
        cost_estimate=pl.CostEstimate(
            flops=2 * tokens * FF * columns,
            bytes_accessed=2 * FF * columns + 12 * tokens * FF,
            transcendentals=tokens * FF,
        ),
    )(cotangent, full_down, gate_part, upward)


def on_device(
    tokens,
    segment_ids,
    positions,
    cotangent,
    qkv_weight,
    out_weight,
    gate_up_weight,
    down_weight,
    norm_gains,
    head_gains,
    qkv_moments,
    out_moments,
    gate_up_moments,
    down_moments,
    norm_moments,
    head_moments,
):
    width = norm_gains.shape[1]
    gains_low = jnp.concatenate([norm_gains, head_gains], axis=1).astype(jnp.bfloat16)
    owners = lax.axis_size(GROUP)
    gains_all = gather_small(gains_low).reshape(2, owners, -1)
    full_norm = gains_all[:, :, :width].reshape(2, -1)
    full_head = gains_all[:, :, width:].reshape(2, -1)
    full_qkv, first, late, _ = gather_rows(qkv_weight, None, None, None, None)
    gain_one = full_norm[0].astype(jnp.float32)
    gain_two = full_norm[1].astype(jnp.float32)
    head_gain = full_head.astype(jnp.float32)
    inputs = tokens.astype(jnp.float32)
    root_one = lax.rsqrt(jnp.mean(inputs * inputs, axis=-1, keepdims=True) + EPS_NORM)
    normed_one = inputs * root_one
    hidden_one = (normed_one * gain_one).astype(jnp.bfloat16)
    projected = jnp.dot(hidden_one, full_qkv, preferred_element_type=jnp.float32)
    full_out, _, down_late, _ = gather_rows(out_weight, first, late, projected, projected)
    full_gate_up, _, more_late, _ = gather_rows(gate_up_weight, first, late, projected, None)
    full_down, _, _, _ = gather_rows(
        down_weight, first, (down_late, more_late, projected), None, None
    )
    tables = rotary_tables(positions, HD)
    mixed_low = attention_call(attend_body, projected, tables, segment_ids, head_gain, None, 0, HK, None)
    attended = jnp.dot(mixed_low, full_out, preferred_element_type=jnp.float32)
    residual = inputs + attended
    root_two = lax.rsqrt(jnp.mean(residual * residual, axis=-1, keepdims=True) + EPS_NORM)
    normed_two = residual * root_two
    hidden_two = (normed_two * gain_two).astype(jnp.bfloat16)
    gate_part, upward, activated = gate_up_forward(hidden_two, full_gate_up)
    down_sum = GradSum(activated, cotangent, True)
    grad_gate_up = gate_up_back(
        after(cotangent, *down_sum.blocks), full_down, gate_part, upward
    )
    gate_up_sum = GradSum(hidden_two, after(grad_gate_up, *down_sum.advance()), True)
    residual_low, grad_gain_two, grad_residual = project_back(
        after(grad_gate_up, *gate_up_sum.blocks),
        full_gate_up,
        residual,
        cotangent,
        gain_two[None],
        True,
    )
    down_sum.hold(residual_low)
    sent = down_sum.advance() + gate_up_sum.advance()
    out_sum = GradSum(mixed_low, after(residual_low, *sent), True)
    down_sum.hold(out_sum.blocks)
    grad_mixed = contract_cols(
        after(residual_low, *out_sum.blocks, *down_sum.advance()), full_out
    ).astype(jnp.bfloat16)
    grad_mixed = after(grad_mixed, *out_sum.advance())
    half = HK // 2
    grad_half, gain_half = attention_call(
        attend_back_body, projected, tables, segment_ids, head_gain, grad_mixed, 0, half, None
    )
    gate_up_sum.hold(grad_half)
    down_sum.hold(grad_half)
    sent = gate_up_sum.advance() + down_sum.advance()
    grad_projected, grad_gain_head = attention_call(
        attend_back_body,
        projected,
        tables,
        segment_ids,
        head_gain,
        grad_mixed,
        half,
        HK - half,
        after(grad_half, *sent),
    )
    grad_gain_head = grad_gain_head + gain_half
    gate_up_sum.hold(grad_projected)
    out_sum.hold(grad_projected)
    sent = gate_up_sum.advance() + out_sum.advance()
    qkv_sum = GradSum(hidden_one, after(grad_projected, *sent), True)
    gate_up_sum.hold(qkv_sum.blocks)
    sent = qkv_sum.advance()
    gate_up_sum.hold(sent)
    out_sum.hold(sent)
    down_sum.hold(sent)
    sent = sent + gate_up_sum.advance() + out_sum.advance()
    branch = jnp.dot(after(activated, *sent), full_down, preferred_element_type=jnp.float32)
    output = (residual + branch).astype(jnp.bfloat16)
    tokens_grad, grad_gain_one = project_back(
        after(grad_projected, *qkv_sum.blocks, *sent),
        full_qkv,
        tokens,
        grad_residual,
        gain_one[None],
        False,
    )
    small = jnp.concatenate(
        [jnp.concatenate([grad_gain_one, grad_gain_two]), grad_gain_head],
        axis=1,
    )
    sent_next = qkv_sum.advance()
    sent_last = qkv_sum.advance()
    qkv_own, out_own, gate_up_own, down_own = owned = tuple(
        v.finish() for v in (qkv_sum, out_sum, gate_up_sum, down_sum)
    )
    down_gathered = gather_grad(after(down_own, *sent_next), None, None)
    local = sum(jnp.sum(v * v) for v in owned)
    partial = jnp.concatenate(
        [small, jnp.full((6, small.shape[1]), local, jnp.float32)], axis=0
    )
    summed = sum_all(after(partial, down_gathered[0][0]))
    small = summed[:2]
    norm_total = small[:, :-HD]
    head_total = small[:, -HD:]
    squares = summed[2, 0] + jnp.sum(small * small)
    clip_limit = math.sqrt(PARAMS)
    factor = clip_limit / jnp.maximum(jnp.sqrt(squares), clip_limit)
    renewed_down = adam_blocks(
        down_weight, down_moments, down_gathered, factor, LEARN_RATE, WEIGHT_DECAY
    )
    gathered = [
        gather_grad(after(qkv_own, summed), renewed_down[0], None),
        gather_grad(after(out_own, *sent_last), None, None),
        gather_grad(after(gate_up_own, *sent_last), None, summed),
    ]
    later = after(factor, gathered[0][0][0])
    renewed_gate_up = adam_blocks(
        gate_up_weight, gate_up_moments, gathered[2], later, LEARN_RATE, WEIGHT_DECAY
    )
    later = after(factor, renewed_gate_up[0])
    renewed_out = adam_blocks(
        out_weight, out_moments, gathered[1], later, LEARN_RATE, WEIGHT_DECAY
    )
    later = after(factor, renewed_out[0])
    renewed_qkv = adam_blocks(
        qkv_weight, qkv_moments, gathered[0], later, LEARN_RATE, WEIGHT_DECAY
    )
    renewed = [renewed_qkv, renewed_out, renewed_gate_up]
    renewed.append(renewed_down)
    mine = lax.axis_index(GROUP)
    norm_grad = lax.dynamic_slice_in_dim(
        norm_total, mine * norm_gains.shape[1], norm_gains.shape[1], 1
    )
    head_grad = lax.dynamic_slice_in_dim(
        head_total, mine * head_gains.shape[1], head_gains.shape[1], 1
    )
    renewed.append(adam_update(norm_gains, norm_moments, norm_grad, factor, GAIN_RATE, 0.0))
    renewed.append(adam_update(head_gains, head_moments, head_grad, factor, GAIN_RATE, 0.0))
    return (
        output,
        tokens_grad,
        *owned,
        norm_grad,
        head_grad,
        *[new for new, _ in renewed],
        *[state for _, state in renewed],
    )


def solution(mesh):
    placed = (
        P((DP, GROUP), None),
        P((DP, GROUP)),
        P((DP, GROUP)),
        P((DP, GROUP), None),
        P(GROUP, None),
        P(GROUP, None),
        P(GROUP, None),
        P(GROUP, None),
        P(None, GROUP),
        P(None, GROUP),
        P(None, GROUP, None),
        P(None, GROUP, None),
        P(None, GROUP, None),
        P(None, GROUP, None),
        P(None, None, GROUP),
        P(None, None, GROUP),
    )
    return jax.shard_map(
        on_device,
        mesh=mesh,
        in_specs=placed,
        out_specs=(
            P((DP, GROUP), None),
            P((DP, GROUP), None),
            P(GROUP, DP),
            P(GROUP, DP),
            P(GROUP, DP),
            P(GROUP, DP),
            P(None, GROUP),
            P(None, GROUP),
            P(GROUP, None),
            P(GROUP, None),
            P(GROUP, None),
            P(GROUP, None),
            P(None, GROUP),
            P(None, GROUP),
            P(None, GROUP, None),
            P(None, GROUP, None),
            P(None, GROUP, None),
            P(None, GROUP, None),
            P(None, None, GROUP),
            P(None, None, GROUP),
        ),
        check_vma=False,
    )
```

```python
import functools
import math

import jax
import jax.numpy as jnp
from jax import lax
from jax.experimental import pallas as pl
from jax.experimental.pallas import tpu as pltpu
from jax.sharding import PartitionSpec as P


HQ = 16
HK = 8
HD = 128
FF = 3072
SEQ_LEN = 512
PARAMS = 15730944
GROUP = "group"
DP = "dp"


EPS_NORM = 1e-06
ROPE_BASE = 1000000.0
MASKED = -1e30
LEARN_RATE = 0.03
GAIN_RATE = 0.3
WEIGHT_DECAY = 0.1
BETA_ONE = 0.9
BETA_TWO = 0.95
ADAM_EPS = 1e-08
STEP_COUNT = 3.0


def rotary_tables(places, width):
    half_width = width // 2
    frequency = ROPE_BASE ** (-(jnp.arange(half_width, dtype=jnp.float32) * 2.0) / width)
    angles = places.astype(jnp.float32)[:, None] * frequency[None, :]
    cosine, sine = jnp.cos(angles), jnp.sin(angles)
    return (
        jnp.concatenate([cosine, cosine], axis=1),
        jnp.concatenate([-sine, sine], axis=1),
    )


def contract_rows(left_side, right_side):
    return lax.dot_general(
        left_side, right_side, (((0,), (0,)), ((), ())), preferred_element_type=jnp.float32
    )


def contract_cols(left_side, right_side):
    return lax.dot_general(
        left_side, right_side, (((1,), (1,)), ((), ())), preferred_element_type=jnp.float32
    )


def norm_back(grad_out, normed, inv_root, gain):
    scaled = grad_out * gain
    return inv_root * (scaled - normed * jnp.mean(normed * scaled, axis=-1, keepdims=True))


def swap(value, axis, mask):
    count = lax.axis_size(axis)
    return lax.ppermute(value, axis, [(i, i ^ mask) for i in range(count)])


def bit_masks(count):
    return [1 << i for i in range(count.bit_length() - 1)]


def after(value, *others):
    return lax.optimization_barrier((value, others))[0]


def place_rows(pieces, rows, owners):
    columns = pieces[0][0].shape[1]
    kind = pieces[0][0].dtype
    sizes = [v.shape[0] for v, _, _ in pieces]

    def body(*refs):
        count = len(pieces)
        ins, out_ref, held = refs[:count], refs[count], refs[count + 1]
        into, away = refs[count + 2 :]
        mine = lax.axis_index(GROUP)
        here = lax.axis_index(DP)
        arriving, leaving, at = [], [], 0
        for k, (_, delta, offset) in enumerate(pieces):
            slot = held.at[pl.ds(at, sizes[k])]
            start = pl.multiple_of((mine ^ delta) * rows + offset(here), 16)
            arriving.append(pltpu.make_async_copy(ins[k], slot, into.at[k]))
            leaving.append(
                pltpu.make_async_copy(slot, out_ref.at[pl.ds(start, sizes[k])], away.at[k])
            )
            at += sizes[k]
        for copy in arriving:
            copy.start()
        for first, second in zip(arriving, leaving):
            first.wait()
            second.start()
        for copy in leaving:
            copy.wait()

    return pl.pallas_call(
        body,
        out_shape=jax.ShapeDtypeStruct((rows * owners, columns), kind),
        in_specs=[pl.BlockSpec(memory_space=pl.ANY)] * len(pieces),
        out_specs=pl.BlockSpec(memory_space=pl.ANY),
        scratch_shapes=[
            pltpu.VMEM((rows * owners, columns), kind),
            pltpu.SemaphoreType.DMA((len(pieces),)),
            pltpu.SemaphoreType.DMA((len(pieces),)),
        ],
        compiler_params=pltpu.CompilerParams(vmem_limit_bytes=32 * 1024 * 1024),
        cost_estimate=pl.CostEstimate(
            flops=0, bytes_accessed=4 * rows * owners * columns, transcendentals=0
        ),
    )(*[v for v, _, _ in pieces])


def gather_rows(shard, early, late, middle, third, hold):
    owners = lax.axis_size(GROUP)
    copies = lax.axis_size(DP)
    here = lax.axis_index(DP)
    if early is not None:
        shard = after(shard, early)
    shard = shard.astype(jnp.bfloat16)
    rows, _ = shard.shape

    def none(_):
        return 0

    pieces = [(shard, 0, none)]
    near = order = by_one = by_two = shard
    if owners == 4 and copies % 4 == 0 and rows % 128 == 0:
        quarter, half = rows // 4, rows // 8

        def place(here):
            return (here & 1) * 2 + ((here >> 1) & 1)

        def quarter_at(mask, more=0):
            return lambda here: (place(here) ^ mask) * quarter + more

        near = lax.dynamic_slice_in_dim(shard, place(here) * quarter, quarter, 0)
        if late is not None:
            near = after(near, late)
        order = swap(near, GROUP, 2)
        passed = order if middle is None else after(order, middle)
        by_one = swap(passed, DP, 1)
        by_two = swap(passed, DP, 2)
        go_one, go_two = by_one, by_two
        if third is not None:
            go_one, go_two = after((by_one, by_two), third)
        last_one = swap(go_two[:half], DP, 1)
        last_two = swap(go_one[half:], DP, 2)
        if hold is not None:
            last_one, last_two = after((last_one, last_two), hold)
        pieces += [
            (order, 2, quarter_at(0)),
            (by_one, 2, quarter_at(2)),
            (by_two, 2, quarter_at(1)),
            (last_one, 2, quarter_at(3)),
            (last_two, 2, quarter_at(3, half)),
        ]
    else:
        for mask in bit_masks(owners)[1:]:
            pieces += [(swap(v, GROUP, mask), dg ^ mask, at) for v, dg, at in pieces]
    pieces += [(swap(v, GROUP, 1), dg ^ 1, at) for v, dg, at in pieces]
    if hold is not None:
        pieces[0] = (after(shard, hold), 0, none)
    return place_rows(pieces, rows, owners), near, order, (by_one, by_two)


def gather_small(shard):
    owners = lax.axis_size(GROUP)
    mine = lax.axis_index(GROUP)
    width = shard.shape[1]
    held = shard[None]
    deltas = [0]
    for mask in reversed(bit_masks(owners)):
        held = jnp.concatenate([held, swap(held, GROUP, mask)], axis=0)
        deltas += [d ^ mask for d in deltas]
    full = jnp.zeros((shard.shape[0], width * owners), shard.dtype)
    for k, delta in enumerate(deltas):
        full = lax.dynamic_update_slice(full, held[k], (0, (mine ^ delta) * width))
    return full


def sum_all(value):
    owners = lax.axis_size(GROUP)
    copies = lax.axis_size(DP)
    mesh_type = pl.DeviceIdType.MESH

    def body(in_ref, out_ref, near, near_sum, far, near_send, near_recv, far_send, far_recv):
        mine = lax.axis_index(GROUP)
        here = lax.axis_index(DP)
        near_peers = [(here, mine ^ k) for k in range(1, owners)]
        far_peers = [(here ^ k, mine) for k in range(1, copies)]
        barrier = pltpu.get_barrier_semaphore()
        for peer in near_peers + far_peers:
            pl.semaphore_signal(barrier, inc=1, device_id=peer, device_id_type=mesh_type)
        pl.semaphore_wait(barrier, len(near_peers) + len(far_peers))

        def exchange(source, slots, index, peers, sends, recvs):
            slots[index] = source[...]
            copies_out = [
                pltpu.make_async_remote_copy(
                    src_ref=source,
                    dst_ref=slots.at[index],
                    send_sem=sends.at[k],
                    recv_sem=recvs.at[k],
                    device_id=peer,
                    device_id_type=mesh_type,
                )
                for k, peer in enumerate(peers)
            ]
            for copy in copies_out:
                copy.start()
            for copy in copies_out:
                copy.wait()
            total = slots[0]
            for k in range(1, len(peers) + 1):
                total = total + slots[k]
            return total

        near_sum[...] = exchange(in_ref, near, mine, near_peers, near_send, near_recv)
        out_ref[...] = exchange(near_sum, far, here, far_peers, far_send, far_recv)

    shape = value.shape
    return pl.pallas_call(
        body,
        out_shape=jax.ShapeDtypeStruct(shape, jnp.float32),
        in_specs=[pl.BlockSpec(memory_space=pltpu.VMEM)],
        out_specs=pl.BlockSpec(memory_space=pltpu.VMEM),
        scratch_shapes=[
            pltpu.VMEM((owners,) + shape, jnp.float32),
            pltpu.VMEM(shape, jnp.float32),
            pltpu.VMEM((copies,) + shape, jnp.float32),
            pltpu.SemaphoreType.DMA((owners - 1,)),
            pltpu.SemaphoreType.DMA((owners - 1,)),
            pltpu.SemaphoreType.DMA((copies - 1,)),
            pltpu.SemaphoreType.DMA((copies - 1,)),
        ],
        compiler_params=pltpu.CompilerParams(collective_id=0, has_side_effects=True),
    )(value)


def spread_bits(position, masks):
    total = 0
    count = len(masks)
    for i, mask in enumerate(masks):
        total = total + ((position >> (count - 1 - i)) & 1) * mask
    return total


def grad_blocks(left, right):
    tokens, rows = left.shape
    columns = right.shape[1]
    owners = lax.axis_size(GROUP)
    copies = lax.axis_size(DP)
    column_masks = bit_masks(copies)
    later = bit_masks(owners)[1:]
    staying = [spread_bits(p, later) for p in range(1 << len(later))]
    row_sets = [[dg + 1 for dg in staying], staying] if owners > 1 else [[0]]
    row_block = rows // owners
    column_block = columns // copies
    mine = lax.axis_index(GROUP)
    here = lax.axis_index(DP)
    if column_block % 128 or row_block % 16:
        ordered = jnp.concatenate(
            [
                lax.dynamic_slice_in_dim(
                    right, (here ^ spread_bits(p, column_masks)) * column_block, column_block, 1
                )
                for p in range(copies)
            ],
            axis=1,
        )
        return [
            jnp.stack(
                [
                    contract_rows(
                        lax.dynamic_slice_in_dim(left, (mine ^ dg) * row_block, row_block, 1),
                        ordered,
                    ).astype(jnp.bfloat16)
                    for dg in row_set
                ]
            )
            for row_set in row_sets
        ]
    wide = 2 if column_block % 256 and copies % 2 == 0 else 1

    def body(where, left_ref, *rest):
        rights, outs, turned = rest[:wide], rest[wide:-1], rest[-1]

        @pl.when(pl.program_id(0) == 0)
        def _():
            turned[...] = left_ref[...].T

        block = jnp.concatenate([ref[...] for ref in rights], axis=1)
        for out, row_set in zip(outs, row_sets):
            for k, dg in enumerate(row_set):
                start = pl.multiple_of((where[0] ^ dg) * row_block, row_block)
                out[k] = jnp.dot(
                    turned[pl.ds(start, row_block), :],
                    block,
                    preferred_element_type=jnp.float32,
                ).astype(jnp.bfloat16)

    def right_spec(j):
        return pl.BlockSpec(
            (tokens, column_block),
            lambda p, where: (0, where[1] ^ spread_bits(p * wide + j, column_masks)),
        )

    return pl.pallas_call(
        body,
        out_shape=[
            jax.ShapeDtypeStruct((len(row_set), row_block, columns), jnp.bfloat16)
            for row_set in row_sets
        ],
        grid_spec=pltpu.PrefetchScalarGridSpec(
            num_scalar_prefetch=1,
            grid=(copies // wide,),
            in_specs=[pl.BlockSpec((tokens, rows), lambda p, where: (0, 0))]
            + [right_spec(j) for j in range(wide)],
            out_specs=[
                pl.BlockSpec(
                    (len(row_set), row_block, column_block * wide), lambda p, where: (0, 0, p)
                )
                for row_set in row_sets
            ],
            scratch_shapes=[pltpu.VMEM((rows, tokens), jnp.bfloat16)],
        ),
        compiler_params=pltpu.CompilerParams(vmem_limit_bytes=48 * 1024 * 1024),
        cost_estimate=pl.CostEstimate(
            flops=2 * tokens * rows * columns,
            bytes_accessed=2 * (tokens * rows + tokens * columns + rows * columns),
            transcendentals=0,
        ),
    )(jnp.stack([mine, here]).astype(jnp.int32), left, *[right] * wide)


class GradSum:
    def __init__(self, left, right, split):
        blocks = grad_blocks(left, right)
        self.blocks = blocks
        group = [(GROUP, m) for m in bit_masks(lax.axis_size(GROUP))]
        other = [(DP, m) for m in bit_masks(lax.axis_size(DP))]
        self.arrays = [blocks[-1]]
        if group:
            self.arrays.append(swap(blocks[0], GROUP, 1))
        rest = group[1:]
        self.orders = [rest + other]
        if split:
            self.orders.append(other[:1] + rest + other[1:])
        count = len(self.orders)
        deep, tall, width = blocks[-1].shape
        size = tall // count
        self.parts = [
            [(k, [(0, deep), (i * size, (i + 1) * size), (0, width)]) for k in range(len(self.arrays))]
            for i in range(count)
        ]
        self.common = len(rest) + 1
        self.length = len(rest) + len(other)
        self.step = 0

    def hold(self, *others):
        self.arrays = list(lax.optimization_barrier((self.arrays, others))[0])

    def read(self, part):
        total = 0.0
        for k, ranges in part:
            at = tuple(slice(*r) for r in ranges)
            total = total + self.arrays[k][at].astype(jnp.float32)
        return total

    def exchange(self, away, axis, mask):
        self.arrays.append(swap(away, axis, mask))
        return len(self.arrays) - 1

    def advance(self):
        if self.step == self.length:
            return []
        outgoing = []
        for i, order in enumerate(self.orders):
            axis, mask = order[self.step]
            dim = 0 if axis == GROUP else 2
            far, near = [], []
            for k, ranges in self.parts[i]:
                start, stop = ranges[dim]
                middle = (start + stop) // 2
                near.append((k, ranges[:dim] + [(start, middle)] + ranges[dim + 1 :]))
                far.append((k, ranges[:dim] + [(middle, stop)] + ranges[dim + 1 :]))
            self.parts[i] = near
            outgoing.append((self.read(far).astype(jnp.bfloat16), axis, mask))
        deep, tall, width = outgoing[0][0].shape
        if self.step >= self.common:
            away = jnp.concatenate([v for v, _, _ in outgoing], axis=1)
            sent = [away]
            k = self.exchange(away, *outgoing[0][1:])
            for i, part in enumerate(self.parts):
                part.append((k, [(0, deep), (i * tall, (i + 1) * tall), (0, width)]))
        else:
            sent = [v for v, _, _ in outgoing]
            for i, (away, axis, mask) in enumerate(outgoing):
                k = self.exchange(away, axis, mask)
                deep, tall, width = away.shape
                self.parts[i].append((k, [(0, deep), (0, tall), (0, width)]))
        self.step += 1
        return sent

    def finish(self):
        while self.step < self.length:
            self.advance()
        return jnp.concatenate([self.read(part)[0] for part in self.parts], axis=0)


def gather_grad(own, second, last):
    held = own.astype(jnp.bfloat16)[None]
    deltas = [0]
    groups = [(held, deltas)]
    masks = list(reversed(bit_masks(lax.axis_size(DP))))
    for i, mask in enumerate(masks):
        away = held
        if i == 1 and second is not None:
            away = after(away, second)
        if i + 1 == len(masks) and last is not None:
            away = after(away, last)
        got = swap(away, DP, mask)
        got_deltas = [d ^ mask for d in deltas]
        if i + 1 < len(masks):
            held = jnp.concatenate([held, got], axis=0)
            deltas = deltas + got_deltas
            groups = [(held, deltas)]
        else:
            groups.append((got, got_deltas))
    return groups


def adam_core(master, first_moment, second_moment, clipped, step_rate, decay_rate):
    first_new = BETA_ONE * first_moment + (1.0 - BETA_ONE) * clipped
    second_new = BETA_TWO * second_moment + (1.0 - BETA_TWO) * clipped * clipped
    first_hat = first_new * (1.0 / (1.0 - BETA_ONE**STEP_COUNT))
    second_hat = second_new * (1.0 / (1.0 - BETA_TWO**STEP_COUNT))
    renewed = master - step_rate * (
        first_hat / (jnp.sqrt(second_hat) + ADAM_EPS) + decay_rate * master
    )
    return renewed, first_new, second_new


def adam_blocks(master, moment, blocks, factor, step_rate, decay_rate):
    rows, columns = master.shape
    copies = lax.axis_size(DP)
    here = lax.axis_index(DP)
    width = columns // copies
    if width % 128:
        full = jnp.zeros(master.shape, jnp.float32)
        for value, deltas in blocks:
            for k, dd in enumerate(deltas):
                full = lax.dynamic_update_slice(
                    full, value[k].astype(jnp.float32), (0, (here ^ dd) * width)
                )
        return adam_update(master, moment, full, factor, step_rate, decay_rate)
    tile = rows
    while tile % 32 == 0 and tile * columns > 256 * 1024:
        tile //= 2

    def body(where, factor_ref, master_ref, moment_ref, *rest):
        grads, (new_ref, state_ref) = rest[:-2], rest[-2:]
        scale = factor_ref[0, 0]
        for grad, (_, deltas) in zip(grads, blocks):
            for k, dd in enumerate(deltas):
                at = pl.ds(pl.multiple_of((where[0] ^ dd) * width, 128), width)
                renewed, first_new, second_new = adam_core(
                    master_ref[:, at],
                    moment_ref[0, :, at],
                    moment_ref[1, :, at],
                    grad[k].astype(jnp.float32) * scale,
                    step_rate,
                    decay_rate,
                )
                new_ref[:, at] = renewed
                state_ref[0, :, at] = first_new
                state_ref[1, :, at] = second_new

    return pl.pallas_call(
        body,
        out_shape=[
            jax.ShapeDtypeStruct(master.shape, jnp.float32),
            jax.ShapeDtypeStruct(moment.shape, jnp.float32),
        ],
        grid_spec=pltpu.PrefetchScalarGridSpec(
            num_scalar_prefetch=1,
            grid=(rows // tile,),
            in_specs=[
                pl.BlockSpec(memory_space=pltpu.SMEM),
                pl.BlockSpec((tile, columns), lambda i, where: (i, 0)),
                pl.BlockSpec((2, tile, columns), lambda i, where: (0, i, 0)),
            ]
            + [
                pl.BlockSpec((len(deltas), tile, width), lambda i, where: (0, i, 0))
                for _, deltas in blocks
            ],
            out_specs=[
                pl.BlockSpec((tile, columns), lambda i, where: (i, 0)),
                pl.BlockSpec((2, tile, columns), lambda i, where: (0, i, 0)),
            ],
        ),
        compiler_params=pltpu.CompilerParams(vmem_limit_bytes=48 * 1024 * 1024),
        cost_estimate=pl.CostEstimate(
            flops=20 * rows * columns,
            bytes_accessed=26 * rows * columns,
            transcendentals=rows * columns,
        ),
    )(
        here.reshape(1).astype(jnp.int32),
        factor.reshape(1, 1),
        master,
        moment,
        *[value for value, _ in blocks],
    )


def adam_update(master, moment, gradient, factor, step_rate, decay_rate):
    clipped = gradient * factor
    first_moment = BETA_ONE * moment[0] + (1.0 - BETA_ONE) * clipped
    second = BETA_TWO * moment[1] + (1.0 - BETA_TWO) * clipped * clipped
    first_hat = first_moment / (1.0 - BETA_ONE**STEP_COUNT)
    second_hat = second / (1.0 - BETA_TWO**STEP_COUNT)
    renewed = master - step_rate * (
        first_hat / (jnp.sqrt(second_hat) + ADAM_EPS) + decay_rate * master
    )
    return (renewed, jnp.stack([first_moment, second]))


def head_forward(raw, gain, cosine, sine):
    root = lax.rsqrt(jnp.mean(raw * raw, axis=-1, keepdims=True) + EPS_NORM)
    normed = raw * root
    scaled = normed * gain
    turned = scaled * cosine + pltpu.roll(scaled, HD // 2, 1) * sine
    return turned.astype(jnp.bfloat16), normed, root


def head_backward(grad, normed, root, gain, cosine, sine):
    turned = grad * cosine - pltpu.roll(grad, HD // 2, 1) * sine
    grad_gain = jnp.sum(turned * normed, axis=0, keepdims=True)
    scaled = turned * gain
    raw = root * (scaled - normed * jnp.mean(normed * scaled, axis=-1, keepdims=True))
    return raw, grad_gain


SPAN = 256


def fill_bias(bias_ref, row_ref, col_ref):
    key_at = lax.broadcasted_iota(jnp.int32, (SEQ_LEN, SEQ_LEN), 0)
    query_at = lax.broadcasted_iota(jnp.int32, (SEQ_LEN, SEQ_LEN), 1)
    allowed = (key_at <= query_at) & (col_ref[...] == row_ref[...])
    bias_ref[...] = jnp.where(allowed, 0.0, MASKED)


def span_weights(query_low, key_low, bias_ref, start):
    stop = start + SPAN
    scores = lax.dot_general(
        key_low[:stop],
        query_low[start:stop],
        (((1,), (1,)), ((), ())),
        preferred_element_type=jnp.float32,
    ) * (1.0 / math.sqrt(HD))
    scores = scores + bias_ref[:stop, start:stop]
    raised = jnp.exp(scores - jnp.max(scores, axis=0, keepdims=True))
    return raised * (1.0 / jnp.sum(raised, axis=0, keepdims=True))


def attend_body(
    query_ref, key_ref, value_ref, cos_ref, sin_ref, row_ref, col_ref, gain_ref, out_ref, bias_ref
):
    @pl.when(pl.program_id(1) == 0)
    def _():
        fill_bias(bias_ref, row_ref, col_ref)

    cosine, sine = cos_ref[...], sin_ref[...]
    key_low, _, _ = head_forward(key_ref[...], gain_ref[1:2, :], cosine, sine)
    value_turned = value_ref[...].astype(jnp.bfloat16).T
    for g in range(HQ // HK):
        at = slice(g * HD, (g + 1) * HD)
        query_low, _, _ = head_forward(query_ref[:, at], gain_ref[0:1, :], cosine, sine)
        for start in range(0, SEQ_LEN, SPAN):
            stop = start + SPAN
            weights = span_weights(query_low, key_low, bias_ref, start)
            mixed = jnp.dot(
                value_turned[:, :stop],
                weights.astype(jnp.bfloat16),
                preferred_element_type=jnp.float32,
            )
            out_ref[start:stop, at] = mixed.T.astype(jnp.bfloat16)


def attend_back_body(
    query_ref, key_ref, value_ref, cos_ref, sin_ref, row_ref, col_ref, gain_ref, grad_ref,
    *rest,
    first,
):
    out_ref, gain_out_ref, bias_ref = rest[-3:]
    head = pl.program_id(1) + first

    @pl.when(head == first)
    def _():
        fill_bias(bias_ref, row_ref, col_ref)

    cosine, sine = cos_ref[...], sin_ref[...]
    inv_head = 1.0 / math.sqrt(HD)

    @pl.when((pl.program_id(0) == 0) & (head == first))
    def _():
        gain_out_ref[...] = jnp.zeros_like(gain_out_ref)

    if len(rest) == 4:

        @pl.when(head == first)
        def _():
            out_ref[...] = rest[0][...]

    key_low, key_normed, key_root = head_forward(key_ref[...], gain_ref[1:2, :], cosine, sine)
    value_low = value_ref[...].astype(jnp.bfloat16)
    key_turned = key_low.T
    grad_key = [jnp.zeros((SPAN, HD), jnp.float32)] * (SEQ_LEN // SPAN)
    grad_value = list(grad_key)
    gain_query = jnp.zeros((1, HD), jnp.float32)
    for g in range(HQ // HK):
        at = slice(g * HD, (g + 1) * HD)
        query_low, normed, root = head_forward(query_ref[:, at], gain_ref[0:1, :], cosine, sine)
        grad_query = []
        for start in range(0, SEQ_LEN, SPAN):
            stop = start + SPAN
            weights = span_weights(query_low, key_low, bias_ref, start)
            grad_out = grad_ref[start:stop, at]
            grad_weights = lax.dot_general(
                value_low[:stop],
                grad_out,
                (((1,), (1,)), ((), ())),
                preferred_element_type=jnp.float32,
            )
            more_value = jnp.dot(
                weights.astype(jnp.bfloat16), grad_out, preferred_element_type=jnp.float32
            )
            product = weights * grad_weights
            grad_scores = (
                weights * (grad_weights - jnp.sum(product, axis=0, keepdims=True))
            ).astype(jnp.bfloat16)
            more_key = jnp.dot(
                grad_scores, query_low[start:stop], preferred_element_type=jnp.float32
            )
            grad_query.append(
                jnp.dot(
                    key_turned[:, :stop], grad_scores, preferred_element_type=jnp.float32
                ).T
            )
            for j in range(stop // SPAN):
                part = slice(j * SPAN, (j + 1) * SPAN)
                grad_key[j] = grad_key[j] + more_key[part]
                grad_value[j] = grad_value[j] + more_value[part]
        raw, more_gain = head_backward(
            jnp.concatenate(grad_query, axis=0) * inv_head,
            normed,
            root,
            gain_ref[0:1, :],
            cosine,
            sine,
        )
        gain_query = gain_query + more_gain
        place = pl.multiple_of((head * (HQ // HK) + g) * HD, HD)
        out_ref[:, pl.ds(place, HD)] = raw.astype(jnp.bfloat16)
    raw, gain_key = head_backward(
        jnp.concatenate(grad_key, axis=0) * inv_head,
        key_normed,
        key_root,
        gain_ref[1:2, :],
        cosine,
        sine,
    )
    out_ref[:, pl.ds(pl.multiple_of((HQ + head) * HD, HD), HD)] = raw.astype(jnp.bfloat16)
    out_ref[:, pl.ds(pl.multiple_of((HQ + HK + head) * HD, HD), HD)] = jnp.concatenate(
        grad_value, axis=0
    ).astype(jnp.bfloat16)
    gain_out_ref[0:1, :] += gain_query
    gain_out_ref[1:2, :] += gain_key


def attention_call(body, projected, tables, segments, gains, grad_out, first, count, base):
    token_rows = projected.shape[0]
    seq_count = token_rows // SEQ_LEN
    groups = HQ // HK
    wide = groups * HD
    full = lambda s, h: (s, 0)
    in_specs = [
        pl.BlockSpec((SEQ_LEN, wide), lambda s, h: (s, first + h)),
        pl.BlockSpec((SEQ_LEN, HD), lambda s, h: (s, HQ + first + h)),
        pl.BlockSpec((SEQ_LEN, HD), lambda s, h: (s, HQ + HK + first + h)),
        pl.BlockSpec((SEQ_LEN, HD), full),
        pl.BlockSpec((SEQ_LEN, HD), full),
        pl.BlockSpec((1, SEQ_LEN), lambda s, h: (0, s)),
        pl.BlockSpec((SEQ_LEN, 1), full),
        pl.BlockSpec((2, HD), lambda s, h: (0, 0)),
    ]
    operands = [
        projected,
        projected,
        projected,
        *tables,
        segments[None, :],
        segments[:, None],
        gains,
    ]
    pairs = token_rows * SEQ_LEN * groups * count
    aliases = {}
    if grad_out is None:
        out_specs = pl.BlockSpec((SEQ_LEN, wide), lambda s, h: (s, first + h))
        out_shape = jax.ShapeDtypeStruct((token_rows, HQ * HD), jnp.bfloat16)
    else:
        columns = projected.shape[1]
        in_specs.append(pl.BlockSpec((SEQ_LEN, wide), lambda s, h: (s, first + h)))
        operands.append(grad_out)
        body = functools.partial(body, first=first)
        if base is not None:
            aliases = {len(operands): 0}
            in_specs.append(pl.BlockSpec((SEQ_LEN, columns), full))
            operands.append(base)
        out_specs = [
            pl.BlockSpec((SEQ_LEN, columns), full),
            pl.BlockSpec((2, HD), lambda s, h: (0, 0)),
        ]
        out_shape = [
            jax.ShapeDtypeStruct((token_rows, columns), jnp.bfloat16),
            jax.ShapeDtypeStruct((2, HD), jnp.float32),
        ]
    return pl.pallas_call(
        body,
        grid=(seq_count, count),
        in_specs=in_specs,
        out_specs=out_specs,
        out_shape=out_shape,
        input_output_aliases=aliases,
        scratch_shapes=[pltpu.VMEM((SEQ_LEN, SEQ_LEN), jnp.float32)],
        compiler_params=pltpu.CompilerParams(vmem_limit_bytes=48 * 1024 * 1024),
        cost_estimate=pl.CostEstimate(
            flops=(4 if grad_out is None else 10) * pairs * HD * 2,
            bytes_accessed=projected.size * 6,
            transcendentals=pairs,
        ),
    )(*operands)


def gate_up_forward(hidden, full_gate_up):
    tokens, depth = hidden.shape
    block = 512
    steps = FF // block

    def body(hidden_ref, left_ref, right_ref, gate_ref, up_ref, out_ref):
        gate = jnp.dot(hidden_ref[...], left_ref[...], preferred_element_type=jnp.float32)
        upward = jnp.dot(hidden_ref[...], right_ref[...], preferred_element_type=jnp.float32)
        gate_ref[...] = gate
        up_ref[...] = upward
        out_ref[...] = (gate * jax.nn.sigmoid(gate) * upward).astype(jnp.bfloat16)

    wide = pl.BlockSpec((tokens, block), lambda j: (0, j))
    return pl.pallas_call(
        body,
        grid=(steps,),
        in_specs=[
            pl.BlockSpec((tokens, depth), lambda j: (0, 0)),
            pl.BlockSpec((depth, block), lambda j: (0, j)),
            pl.BlockSpec((depth, block), lambda j: (0, steps + j)),
        ],
        out_specs=[wide, wide, wide],
        out_shape=[
            jax.ShapeDtypeStruct((tokens, FF), jnp.float32),
            jax.ShapeDtypeStruct((tokens, FF), jnp.float32),
            jax.ShapeDtypeStruct((tokens, FF), jnp.bfloat16),
        ],
        compiler_params=pltpu.CompilerParams(vmem_limit_bytes=48 * 1024 * 1024),
        cost_estimate=pl.CostEstimate(
            flops=4 * tokens * FF * depth,
            bytes_accessed=4 * FF * depth + 10 * tokens * FF,
            transcendentals=tokens * FF,
        ),
    )(hidden, full_gate_up, full_gate_up)


def project_back(grad_low, weight, value, upstream, gain, whole):
    tokens, width = grad_low.shape
    depth = weight.shape[0]
    block = 1024
    steps = width // block

    def body(grad_ref, weight_ref, value_ref, up_ref, gain_ref, *rest):
        total_ref = rest[-1]
        step = pl.program_id(0)
        more = lax.dot_general(
            grad_ref[...],
            weight_ref[...],
            (((1,), (1,)), ((), ())),
            preferred_element_type=jnp.float32,
        )

        @pl.when(step == 0)
        def _():
            total_ref[...] = more

        @pl.when(step > 0)
        def _():
            total_ref[...] += more

        @pl.when(step == steps - 1)
        def _():
            raw = value_ref[...].astype(jnp.float32)
            root = lax.rsqrt(jnp.mean(raw * raw, axis=-1, keepdims=True) + EPS_NORM)
            normed = raw * root
            grad = total_ref[...]
            rest[1][...] = jnp.sum(grad * normed, axis=0, keepdims=True)
            full = up_ref[...].astype(jnp.float32) + norm_back(grad, normed, root, gain_ref[...])
            rest[0][...] = full.astype(jnp.bfloat16)
            if whole:
                rest[2][...] = full

    fixed = lambda j: (0, 0)
    square = pl.BlockSpec((tokens, depth), fixed)
    row = pl.BlockSpec((1, depth), fixed)
    shapes = [
        jax.ShapeDtypeStruct((tokens, depth), jnp.bfloat16),
        jax.ShapeDtypeStruct((1, depth), jnp.float32),
    ]
    if whole:
        shapes.append(jax.ShapeDtypeStruct((tokens, depth), jnp.float32))
    return pl.pallas_call(
        body,
        grid=(steps,),
        in_specs=[
            pl.BlockSpec((tokens, block), lambda j: (0, j)),
            pl.BlockSpec((depth, block), lambda j: (0, j)),
            square,
            square,
            row,
        ],
        out_specs=[square, row] + [square] * whole,
        out_shape=shapes,
        scratch_shapes=[pltpu.VMEM((tokens, depth), jnp.float32)],
        compiler_params=pltpu.CompilerParams(vmem_limit_bytes=48 * 1024 * 1024),
        cost_estimate=pl.CostEstimate(
            flops=2 * tokens * width * depth,
            bytes_accessed=2 * width * (depth + tokens) + 14 * tokens * depth,
            transcendentals=tokens,
        ),
    )(grad_low, weight, value, upstream, gain)


def gate_up_back(cotangent, full_down, gate_part, upward):
    tokens, columns = cotangent.shape
    block = 512
    steps = FF // block

    def body(cot_ref, down_ref, gate_ref, up_ref, out_ref):
        at = pl.program_id(0) * block
        grad = lax.dot_general(
            cot_ref[...],
            down_ref[...],
            (((1,), (1,)), ((), ())),
            preferred_element_type=jnp.float32,
        )
        gate = gate_ref[...]
        part = jax.nn.sigmoid(gate)
        grad_gate = grad * up_ref[...] * part * (1.0 + gate * (1.0 - part))
        grad_up = grad * gate * part
        out_ref[:, pl.ds(pl.multiple_of(at, block), block)] = grad_gate.astype(jnp.bfloat16)
        out_ref[:, pl.ds(pl.multiple_of(at + FF, block), block)] = grad_up.astype(jnp.bfloat16)

    return pl.pallas_call(
        body,
        grid=(steps,),
        in_specs=[
            pl.BlockSpec((tokens, columns), lambda j: (0, 0)),
            pl.BlockSpec((block, columns), lambda j: (j, 0)),
            pl.BlockSpec((tokens, block), lambda j: (0, j)),
            pl.BlockSpec((tokens, block), lambda j: (0, j)),
        ],
        out_specs=pl.BlockSpec((tokens, 2 * FF), lambda j: (0, 0)),
        out_shape=jax.ShapeDtypeStruct((tokens, 2 * FF), jnp.bfloat16),
        compiler_params=pltpu.CompilerParams(vmem_limit_bytes=48 * 1024 * 1024),
        cost_estimate=pl.CostEstimate(
            flops=2 * tokens * FF * columns,
            bytes_accessed=2 * FF * columns + 12 * tokens * FF,
            transcendentals=tokens * FF,
        ),
    )(cotangent, full_down, gate_part, upward)


def on_device(
    tokens,
    segment_ids,
    positions,
    cotangent,
    qkv_weight,
    out_weight,
    gate_up_weight,
    down_weight,
    norm_gains,
    head_gains,
    qkv_moments,
    out_moments,
    gate_up_moments,
    down_moments,
    norm_moments,
    head_moments,
):
    width = norm_gains.shape[1]
    gains_low = jnp.concatenate([norm_gains, head_gains], axis=1).astype(jnp.bfloat16)
    owners = lax.axis_size(GROUP)
    gains_all = gather_small(gains_low).reshape(2, owners, -1)
    full_norm = gains_all[:, :, :width].reshape(2, -1)
    full_head = gains_all[:, :, width:].reshape(2, -1)
    full_qkv, first, late, _ = gather_rows(qkv_weight, None, None, None, None, None)
    gain_one = full_norm[0].astype(jnp.float32)
    gain_two = full_norm[1].astype(jnp.float32)
    head_gain = full_head.astype(jnp.float32)
    inputs = tokens.astype(jnp.float32)
    root_one = lax.rsqrt(jnp.mean(inputs * inputs, axis=-1, keepdims=True) + EPS_NORM)
    normed_one = inputs * root_one
    hidden_one = (normed_one * gain_one).astype(jnp.bfloat16)
    projected = jnp.dot(hidden_one, full_qkv, preferred_element_type=jnp.float32)
    tables = rotary_tables(positions, HD)
    mixed_low = attention_call(attend_body, projected, tables, segment_ids, head_gain, None, 0, HK, None)
    full_out, _, down_late, _ = gather_rows(out_weight, first, late, None, projected, mixed_low)
    full_gate_up, _, more_late, _ = gather_rows(gate_up_weight, first, late, projected, None, None)
    full_down, _, _, _ = gather_rows(
        down_weight, first, (down_late, more_late, projected), None, None, None
    )
    attended = jnp.dot(mixed_low, full_out, preferred_element_type=jnp.float32)
    residual = inputs + attended
    root_two = lax.rsqrt(jnp.mean(residual * residual, axis=-1, keepdims=True) + EPS_NORM)
    normed_two = residual * root_two
    hidden_two = (normed_two * gain_two).astype(jnp.bfloat16)
    gate_part, upward, activated = gate_up_forward(hidden_two, full_gate_up)
    down_sum = GradSum(activated, cotangent, True)
    grad_gate_up = gate_up_back(
        after(cotangent, *down_sum.blocks), full_down, gate_part, upward
    )
    gate_up_sum = GradSum(hidden_two, after(grad_gate_up, *down_sum.advance()), True)
    residual_low, grad_gain_two, grad_residual = project_back(
        after(grad_gate_up, *gate_up_sum.blocks),
        full_gate_up,
        residual,
        cotangent,
        gain_two[None],
        True,
    )
    down_sum.hold(residual_low)
    sent = down_sum.advance() + gate_up_sum.advance()
    out_sum = GradSum(mixed_low, after(residual_low, *sent), True)
    down_sum.hold(out_sum.blocks)
    grad_mixed = contract_cols(
        after(residual_low, *out_sum.blocks, *down_sum.advance()), full_out
    ).astype(jnp.bfloat16)
    grad_mixed = after(grad_mixed, *out_sum.advance())
    half = HK // 2
    grad_half, gain_half = attention_call(
        attend_back_body, projected, tables, segment_ids, head_gain, grad_mixed, 0, half, None
    )
    gate_up_sum.hold(grad_half)
    down_sum.hold(grad_half)
    sent = gate_up_sum.advance() + down_sum.advance()
    grad_projected, grad_gain_head = attention_call(
        attend_back_body,
        projected,
        tables,
        segment_ids,
        head_gain,
        grad_mixed,
        half,
        HK - half,
        after(grad_half, *sent),
    )
    grad_gain_head = grad_gain_head + gain_half
    gate_up_sum.hold(grad_projected)
    out_sum.hold(grad_projected)
    sent = gate_up_sum.advance() + out_sum.advance()
    qkv_sum = GradSum(hidden_one, after(grad_projected, *sent), True)
    gate_up_sum.hold(qkv_sum.blocks)
    sent = qkv_sum.advance()
    gate_up_sum.hold(sent)
    out_sum.hold(sent)
    down_sum.hold(sent)
    sent = sent + gate_up_sum.advance() + out_sum.advance()
    branch = jnp.dot(after(activated, *sent), full_down, preferred_element_type=jnp.float32)
    output = (residual + branch).astype(jnp.bfloat16)
    tokens_grad, grad_gain_one = project_back(
        after(grad_projected, *qkv_sum.blocks, *sent),
        full_qkv,
        tokens,
        grad_residual,
        gain_one[None],
        False,
    )
    small = jnp.concatenate(
        [jnp.concatenate([grad_gain_one, grad_gain_two]), grad_gain_head],
        axis=1,
    )
    sent_next = qkv_sum.advance()
    qkv_sum.advance()
    sent_last = qkv_sum.advance()
    qkv_own, out_own, gate_up_own, down_own = owned = tuple(
        v.finish() for v in (qkv_sum, out_sum, gate_up_sum, down_sum)
    )
    down_gathered = gather_grad(after(down_own, *sent_next), None, None)
    local = sum(jnp.sum(v * v) for v in owned)
    partial = jnp.concatenate(
        [small, jnp.full((6, small.shape[1]), local, jnp.float32)], axis=0
    )
    summed = sum_all(after(partial, down_gathered[0][0]))
    small = summed[:2]
    norm_total = small[:, :-HD]
    head_total = small[:, -HD:]
    squares = summed[2, 0] + jnp.sum(small * small)
    clip_limit = math.sqrt(PARAMS)
    factor = clip_limit / jnp.maximum(jnp.sqrt(squares), clip_limit)
    renewed_down = adam_blocks(
        down_weight, down_moments, down_gathered, factor, LEARN_RATE, WEIGHT_DECAY
    )
    gathered = [
        gather_grad(after(qkv_own, summed), renewed_down[0], None),
        gather_grad(after(out_own, *sent_last), None, None),
        gather_grad(after(gate_up_own, *sent_last), summed, None),
    ]
    later = after(factor, gathered[0][0][0])
    renewed_gate_up = adam_blocks(
        gate_up_weight, gate_up_moments, gathered[2], later, LEARN_RATE, WEIGHT_DECAY
    )
    later = after(factor, renewed_gate_up[0])
    renewed_out = adam_blocks(
        out_weight, out_moments, gathered[1], later, LEARN_RATE, WEIGHT_DECAY
    )
    later = after(factor, renewed_out[0])
    renewed_qkv = adam_blocks(
        qkv_weight, qkv_moments, gathered[0], later, LEARN_RATE, WEIGHT_DECAY
    )
    renewed = [renewed_qkv, renewed_out, renewed_gate_up]
    renewed.append(renewed_down)
    mine = lax.axis_index(GROUP)
    norm_grad = lax.dynamic_slice_in_dim(
        norm_total, mine * norm_gains.shape[1], norm_gains.shape[1], 1
    )
    head_grad = lax.dynamic_slice_in_dim(
        head_total, mine * head_gains.shape[1], head_gains.shape[1], 1
    )
    renewed.append(adam_update(norm_gains, norm_moments, norm_grad, factor, GAIN_RATE, 0.0))
    renewed.append(adam_update(head_gains, head_moments, head_grad, factor, GAIN_RATE, 0.0))
    return (
        output,
        tokens_grad,
        *owned,
        norm_grad,
        head_grad,
        *[new for new, _ in renewed],
        *[state for _, state in renewed],
    )


def solution(mesh):
    placed = (
        P((DP, GROUP), None),
        P((DP, GROUP)),
        P((DP, GROUP)),
        P((DP, GROUP), None),
        P(GROUP, None),
        P(GROUP, None),
        P(GROUP, None),
        P(GROUP, None),
        P(None, GROUP),
        P(None, GROUP),
        P(None, GROUP, None),
        P(None, GROUP, None),
        P(None, GROUP, None),
        P(None, GROUP, None),
        P(None, None, GROUP),
        P(None, None, GROUP),
    )
    return jax.shard_map(
        on_device,
        mesh=mesh,
        in_specs=placed,
        out_specs=(
            P((DP, GROUP), None),
            P((DP, GROUP), None),
            P(GROUP, DP),
            P(GROUP, DP),
            P(GROUP, DP),
            P(GROUP, DP),
            P(None, GROUP),
            P(None, GROUP),
            P(GROUP, None),
            P(GROUP, None),
            P(GROUP, None),
            P(GROUP, None),
            P(None, GROUP),
            P(None, GROUP),
            P(None, GROUP, None),
            P(None, GROUP, None),
            P(None, GROUP, None),
            P(None, GROUP, None),
            P(None, None, GROUP),
            P(None, None, GROUP),
        ),
        check_vma=False,
    )
```

```python
import functools
import math

import jax
import jax.numpy as jnp
from jax import lax
from jax.experimental import pallas as pl
from jax.experimental.pallas import tpu as pltpu
from jax.sharding import PartitionSpec as P


HQ = 16
HK = 8
HD = 128
FF = 3072
SEQ_LEN = 512
PARAMS = 15730944
GROUP = "group"
DP = "dp"


EPS_NORM = 1e-06
ROPE_BASE = 1000000.0
MASKED = -1e30
LEARN_RATE = 0.03
GAIN_RATE = 0.3
WEIGHT_DECAY = 0.1
BETA_ONE = 0.9
BETA_TWO = 0.95
ADAM_EPS = 1e-08
STEP_COUNT = 3.0


def rotary_tables(places, width):
    half_width = width // 2
    frequency = ROPE_BASE ** (-(jnp.arange(half_width, dtype=jnp.float32) * 2.0) / width)
    angles = places.astype(jnp.float32)[:, None] * frequency[None, :]
    cosine, sine = jnp.cos(angles), jnp.sin(angles)
    return (
        jnp.concatenate([cosine, cosine], axis=1),
        jnp.concatenate([-sine, sine], axis=1),
    )


def contract_rows(left_side, right_side):
    return lax.dot_general(
        left_side, right_side, (((0,), (0,)), ((), ())), preferred_element_type=jnp.float32
    )


def contract_cols(left_side, right_side):
    return lax.dot_general(
        left_side, right_side, (((1,), (1,)), ((), ())), preferred_element_type=jnp.float32
    )


def norm_back(grad_out, normed, inv_root, gain):
    scaled = grad_out * gain
    return inv_root * (scaled - normed * jnp.mean(normed * scaled, axis=-1, keepdims=True))


def swap(value, axis, mask):
    count = lax.axis_size(axis)
    return lax.ppermute(value, axis, [(i, i ^ mask) for i in range(count)])


def bit_masks(count):
    return [1 << i for i in range(count.bit_length() - 1)]


def after(value, *others):
    return lax.optimization_barrier((value, others))[0]


def place_rows(pieces, rows, owners):
    columns = pieces[0][0].shape[1]
    kind = pieces[0][0].dtype
    sizes = [v.shape[0] for v, _, _ in pieces]

    def body(*refs):
        count = len(pieces)
        ins, out_ref, held = refs[:count], refs[count], refs[count + 1]
        into, away = refs[count + 2 :]
        mine = lax.axis_index(GROUP)
        here = lax.axis_index(DP)
        arriving, leaving, at = [], [], 0
        for k, (_, delta, offset) in enumerate(pieces):
            slot = held.at[pl.ds(at, sizes[k])]
            start = pl.multiple_of((mine ^ delta) * rows + offset(here), 16)
            arriving.append(pltpu.make_async_copy(ins[k], slot, into.at[k]))
            leaving.append(
                pltpu.make_async_copy(slot, out_ref.at[pl.ds(start, sizes[k])], away.at[k])
            )
            at += sizes[k]
        for copy in arriving:
            copy.start()
        for first, second in zip(arriving, leaving):
            first.wait()
            second.start()
        for copy in leaving:
            copy.wait()

    return pl.pallas_call(
        body,
        out_shape=jax.ShapeDtypeStruct((rows * owners, columns), kind),
        in_specs=[pl.BlockSpec(memory_space=pl.ANY)] * len(pieces),
        out_specs=pl.BlockSpec(memory_space=pl.ANY),
        scratch_shapes=[
            pltpu.VMEM((rows * owners, columns), kind),
            pltpu.SemaphoreType.DMA((len(pieces),)),
            pltpu.SemaphoreType.DMA((len(pieces),)),
        ],
        compiler_params=pltpu.CompilerParams(vmem_limit_bytes=32 * 1024 * 1024),
        cost_estimate=pl.CostEstimate(
            flops=0, bytes_accessed=4 * rows * owners * columns, transcendentals=0
        ),
    )(*[v for v, _, _ in pieces])


def gather_rows(shard, early, late, middle, third, hold):
    owners = lax.axis_size(GROUP)
    copies = lax.axis_size(DP)
    here = lax.axis_index(DP)
    if early is not None:
        shard = after(shard, early)
    shard = shard.astype(jnp.bfloat16)
    rows, _ = shard.shape

    def none(_):
        return 0

    pieces = [(shard, 0, none)]
    near = order = by_one = by_two = shard
    if owners == 4 and copies % 4 == 0 and rows % 128 == 0:
        quarter, half = rows // 4, rows // 8

        def place(here):
            return (here & 1) * 2 + ((here >> 1) & 1)

        def quarter_at(mask, more=0):
            return lambda here: (place(here) ^ mask) * quarter + more

        near = lax.dynamic_slice_in_dim(shard, place(here) * quarter, quarter, 0)
        if late is not None:
            near = after(near, late)
        order = swap(near, GROUP, 2)
        passed = order if middle is None else after(order, middle)
        by_one = swap(passed, DP, 1)
        by_two = swap(passed, DP, 2)
        go_one, go_two = by_one, by_two
        if third is not None:
            go_one, go_two = after((by_one, by_two), third)
        last_one = swap(go_two[:half], DP, 1)
        last_two = swap(go_one[half:], DP, 2)
        if hold is not None:
            last_one, last_two = after((last_one, last_two), hold)
        pieces += [
            (order, 2, quarter_at(0)),
            (by_one, 2, quarter_at(2)),
            (by_two, 2, quarter_at(1)),
            (last_one, 2, quarter_at(3)),
            (last_two, 2, quarter_at(3, half)),
        ]
    else:
        for mask in bit_masks(owners)[1:]:
            pieces += [(swap(v, GROUP, mask), dg ^ mask, at) for v, dg, at in pieces]
    pieces += [(swap(v, GROUP, 1), dg ^ 1, at) for v, dg, at in pieces]
    if hold is not None:
        pieces[0] = (after(shard, hold), 0, none)
    full = place_rows(pieces, rows, owners)
    return full, near, order, (by_one, by_two)


def gather_small(shard):
    owners = lax.axis_size(GROUP)
    mine = lax.axis_index(GROUP)
    width = shard.shape[1]
    held = shard[None]
    deltas = [0]
    for mask in reversed(bit_masks(owners)):
        held = jnp.concatenate([held, swap(held, GROUP, mask)], axis=0)
        deltas += [d ^ mask for d in deltas]
    full = jnp.zeros((shard.shape[0], width * owners), shard.dtype)
    for k, delta in enumerate(deltas):
        full = lax.dynamic_update_slice(full, held[k], (0, (mine ^ delta) * width))
    return full


def sum_all(value):
    owners = lax.axis_size(GROUP)
    copies = lax.axis_size(DP)
    mesh_type = pl.DeviceIdType.MESH

    def body(in_ref, out_ref, near, near_sum, far, near_send, near_recv, far_send, far_recv):
        mine = lax.axis_index(GROUP)
        here = lax.axis_index(DP)
        near_peers = [(here, mine ^ k) for k in range(1, owners)]
        far_peers = [(here ^ k, mine) for k in range(1, copies)]
        barrier = pltpu.get_barrier_semaphore()
        for peer in near_peers + far_peers:
            pl.semaphore_signal(barrier, inc=1, device_id=peer, device_id_type=mesh_type)
        pl.semaphore_wait(barrier, len(near_peers) + len(far_peers))

        def exchange(source, slots, index, peers, sends, recvs):
            slots[index] = source[...]
            copies_out = [
                pltpu.make_async_remote_copy(
                    src_ref=source,
                    dst_ref=slots.at[index],
                    send_sem=sends.at[k],
                    recv_sem=recvs.at[k],
                    device_id=peer,
                    device_id_type=mesh_type,
                )
                for k, peer in enumerate(peers)
            ]
            for copy in copies_out:
                copy.start()
            for copy in copies_out:
                copy.wait()
            total = slots[0]
            for k in range(1, len(peers) + 1):
                total = total + slots[k]
            return total

        near_sum[...] = exchange(in_ref, near, mine, near_peers, near_send, near_recv)
        out_ref[...] = exchange(near_sum, far, here, far_peers, far_send, far_recv)

    shape = value.shape
    return pl.pallas_call(
        body,
        out_shape=jax.ShapeDtypeStruct(shape, jnp.float32),
        in_specs=[pl.BlockSpec(memory_space=pltpu.VMEM)],
        out_specs=pl.BlockSpec(memory_space=pltpu.VMEM),
        scratch_shapes=[
            pltpu.VMEM((owners,) + shape, jnp.float32),
            pltpu.VMEM(shape, jnp.float32),
            pltpu.VMEM((copies,) + shape, jnp.float32),
            pltpu.SemaphoreType.DMA((owners - 1,)),
            pltpu.SemaphoreType.DMA((owners - 1,)),
            pltpu.SemaphoreType.DMA((copies - 1,)),
            pltpu.SemaphoreType.DMA((copies - 1,)),
        ],
        compiler_params=pltpu.CompilerParams(collective_id=0, has_side_effects=True),
    )(value)


def spread_bits(position, masks):
    total = 0
    count = len(masks)
    for i, mask in enumerate(masks):
        total = total + ((position >> (count - 1 - i)) & 1) * mask
    return total


def grad_blocks(left, right):
    tokens, rows = left.shape
    columns = right.shape[1]
    owners = lax.axis_size(GROUP)
    copies = lax.axis_size(DP)
    column_masks = bit_masks(copies)
    later = bit_masks(owners)[1:]
    staying = [spread_bits(p, later) for p in range(1 << len(later))]
    row_sets = [[dg + 1 for dg in staying], staying] if owners > 1 else [[0]]
    row_block = rows // owners
    column_block = columns // copies
    mine = lax.axis_index(GROUP)
    here = lax.axis_index(DP)
    if column_block % 128 or row_block % 16:
        ordered = jnp.concatenate(
            [
                lax.dynamic_slice_in_dim(
                    right, (here ^ spread_bits(p, column_masks)) * column_block, column_block, 1
                )
                for p in range(copies)
            ],
            axis=1,
        )
        return [
            jnp.stack(
                [
                    contract_rows(
                        lax.dynamic_slice_in_dim(left, (mine ^ dg) * row_block, row_block, 1),
                        ordered,
                    ).astype(jnp.bfloat16)
                    for dg in row_set
                ]
            )
            for row_set in row_sets
        ]
    wide = 2 if column_block % 256 and copies % 2 == 0 else 1

    def body(where, left_ref, *rest):
        rights, outs, turned = rest[:wide], rest[wide:-1], rest[-1]

        @pl.when(pl.program_id(0) == 0)
        def _():
            turned[...] = left_ref[...].T

        block = jnp.concatenate([ref[...] for ref in rights], axis=1)
        for out, row_set in zip(outs, row_sets):
            for k, dg in enumerate(row_set):
                start = pl.multiple_of((where[0] ^ dg) * row_block, row_block)
                out[k] = jnp.dot(
                    turned[pl.ds(start, row_block), :],
                    block,
                    preferred_element_type=jnp.float32,
                ).astype(jnp.bfloat16)

    def right_spec(j):
        return pl.BlockSpec(
            (tokens, column_block),
            lambda p, where: (0, where[1] ^ spread_bits(p * wide + j, column_masks)),
        )

    return pl.pallas_call(
        body,
        out_shape=[
            jax.ShapeDtypeStruct((len(row_set), row_block, columns), jnp.bfloat16)
            for row_set in row_sets
        ],
        grid_spec=pltpu.PrefetchScalarGridSpec(
            num_scalar_prefetch=1,
            grid=(copies // wide,),
            in_specs=[pl.BlockSpec((tokens, rows), lambda p, where: (0, 0))]
            + [right_spec(j) for j in range(wide)],
            out_specs=[
                pl.BlockSpec(
                    (len(row_set), row_block, column_block * wide), lambda p, where: (0, 0, p)
                )
                for row_set in row_sets
            ],
            scratch_shapes=[pltpu.VMEM((rows, tokens), jnp.bfloat16)],
        ),
        compiler_params=pltpu.CompilerParams(vmem_limit_bytes=48 * 1024 * 1024),
        cost_estimate=pl.CostEstimate(
            flops=2 * tokens * rows * columns,
            bytes_accessed=2 * (tokens * rows + tokens * columns + rows * columns),
            transcendentals=0,
        ),
    )(jnp.stack([mine, here]).astype(jnp.int32), left, *[right] * wide)


class GradSum:
    def __init__(self, left, right, split):
        blocks = grad_blocks(left, right)
        self.blocks = blocks
        group = [(GROUP, m) for m in bit_masks(lax.axis_size(GROUP))]
        other = [(DP, m) for m in bit_masks(lax.axis_size(DP))]
        self.arrays = [blocks[-1]]
        if group:
            self.arrays.append(swap(blocks[0], GROUP, 1))
        rest = group[1:]
        self.orders = [rest + other]
        if split:
            self.orders.append(other[:1] + rest + other[1:])
        count = len(self.orders)
        deep, tall, width = blocks[-1].shape
        size = tall // count
        self.parts = [
            [(k, [(0, deep), (i * size, (i + 1) * size), (0, width)]) for k in range(len(self.arrays))]
            for i in range(count)
        ]
        self.common = len(rest) + 1
        self.length = len(rest) + len(other)
        self.step = 0

    def hold(self, *others):
        self.arrays = list(lax.optimization_barrier((self.arrays, others))[0])

    def read(self, part):
        total = 0.0
        for k, ranges in part:
            at = tuple(slice(*r) for r in ranges)
            total = total + self.arrays[k][at].astype(jnp.float32)
        return total

    def exchange(self, away, axis, mask):
        self.arrays.append(swap(away, axis, mask))
        return len(self.arrays) - 1

    def advance(self):
        if self.step == self.length:
            return []
        outgoing = []
        for i, order in enumerate(self.orders):
            axis, mask = order[self.step]
            dim = 0 if axis == GROUP else 2
            far, near = [], []
            for k, ranges in self.parts[i]:
                start, stop = ranges[dim]
                middle = (start + stop) // 2
                near.append((k, ranges[:dim] + [(start, middle)] + ranges[dim + 1 :]))
                far.append((k, ranges[:dim] + [(middle, stop)] + ranges[dim + 1 :]))
            self.parts[i] = near
            outgoing.append((self.read(far).astype(jnp.bfloat16), axis, mask))
        deep, tall, width = outgoing[0][0].shape
        if self.step >= self.common:
            away = jnp.concatenate([v for v, _, _ in outgoing], axis=1)
            sent = [away]
            k = self.exchange(away, *outgoing[0][1:])
            for i, part in enumerate(self.parts):
                part.append((k, [(0, deep), (i * tall, (i + 1) * tall), (0, width)]))
        else:
            sent = [v for v, _, _ in outgoing]
            for i, (away, axis, mask) in enumerate(outgoing):
                k = self.exchange(away, axis, mask)
                deep, tall, width = away.shape
                self.parts[i].append((k, [(0, deep), (0, tall), (0, width)]))
        self.step += 1
        return sent

    def finish(self):
        while self.step < self.length:
            self.advance()
        return jnp.concatenate([self.read(part)[0] for part in self.parts], axis=0)


def gather_grad(own, second, last):
    held = own.astype(jnp.bfloat16)[None]
    deltas = [0]
    groups = [(held, deltas)]
    masks = list(reversed(bit_masks(lax.axis_size(DP))))
    for i, mask in enumerate(masks):
        away = held
        if i == 1 and second is not None:
            away = after(away, second)
        if i + 1 == len(masks) and last is not None:
            away = after(away, last)
        got = swap(away, DP, mask)
        got_deltas = [d ^ mask for d in deltas]
        if i + 1 < len(masks):
            held = jnp.concatenate([held, got], axis=0)
            deltas = deltas + got_deltas
            groups = [(held, deltas)]
        else:
            groups.append((got, got_deltas))
    return groups


def adam_core(master, first_moment, second_moment, clipped, step_rate, decay_rate):
    first_new = BETA_ONE * first_moment + (1.0 - BETA_ONE) * clipped
    second_new = BETA_TWO * second_moment + (1.0 - BETA_TWO) * clipped * clipped
    first_hat = first_new * (1.0 / (1.0 - BETA_ONE**STEP_COUNT))
    second_hat = second_new * (1.0 / (1.0 - BETA_TWO**STEP_COUNT))
    renewed = master - step_rate * (
        first_hat / (jnp.sqrt(second_hat) + ADAM_EPS) + decay_rate * master
    )
    return renewed, first_new, second_new


def adam_blocks(master, moment, blocks, factor, step_rate, decay_rate):
    rows, columns = master.shape
    copies = lax.axis_size(DP)
    here = lax.axis_index(DP)
    width = columns // copies
    if width % 128:
        full = jnp.zeros(master.shape, jnp.float32)
        for value, deltas in blocks:
            for k, dd in enumerate(deltas):
                full = lax.dynamic_update_slice(
                    full, value[k].astype(jnp.float32), (0, (here ^ dd) * width)
                )
        return adam_update(master, moment, full, factor, step_rate, decay_rate)
    tile = rows
    while tile % 32 == 0 and tile * columns > 256 * 1024:
        tile //= 2

    def body(where, factor_ref, master_ref, moment_ref, *rest):
        grads, (new_ref, state_ref) = rest[:-2], rest[-2:]
        scale = factor_ref[0, 0]
        for grad, (_, deltas) in zip(grads, blocks):
            for k, dd in enumerate(deltas):
                at = pl.ds(pl.multiple_of((where[0] ^ dd) * width, 128), width)
                renewed, first_new, second_new = adam_core(
                    master_ref[:, at],
                    moment_ref[0, :, at],
                    moment_ref[1, :, at],
                    grad[k].astype(jnp.float32) * scale,
                    step_rate,
                    decay_rate,
                )
                new_ref[:, at] = renewed
                state_ref[0, :, at] = first_new
                state_ref[1, :, at] = second_new

    return pl.pallas_call(
        body,
        out_shape=[
            jax.ShapeDtypeStruct(master.shape, jnp.float32),
            jax.ShapeDtypeStruct(moment.shape, jnp.float32),
        ],
        grid_spec=pltpu.PrefetchScalarGridSpec(
            num_scalar_prefetch=1,
            grid=(rows // tile,),
            in_specs=[
                pl.BlockSpec(memory_space=pltpu.SMEM),
                pl.BlockSpec((tile, columns), lambda i, where: (i, 0)),
                pl.BlockSpec((2, tile, columns), lambda i, where: (0, i, 0)),
            ]
            + [
                pl.BlockSpec((len(deltas), tile, width), lambda i, where: (0, i, 0))
                for _, deltas in blocks
            ],
            out_specs=[
                pl.BlockSpec((tile, columns), lambda i, where: (i, 0)),
                pl.BlockSpec((2, tile, columns), lambda i, where: (0, i, 0)),
            ],
        ),
        compiler_params=pltpu.CompilerParams(vmem_limit_bytes=48 * 1024 * 1024),
        cost_estimate=pl.CostEstimate(
            flops=20 * rows * columns,
            bytes_accessed=26 * rows * columns,
            transcendentals=rows * columns,
        ),
    )(
        here.reshape(1).astype(jnp.int32),
        factor.reshape(1, 1),
        master,
        moment,
        *[value for value, _ in blocks],
    )


def adam_update(master, moment, gradient, factor, step_rate, decay_rate):
    clipped = gradient * factor
    first_moment = BETA_ONE * moment[0] + (1.0 - BETA_ONE) * clipped
    second = BETA_TWO * moment[1] + (1.0 - BETA_TWO) * clipped * clipped
    first_hat = first_moment / (1.0 - BETA_ONE**STEP_COUNT)
    second_hat = second / (1.0 - BETA_TWO**STEP_COUNT)
    renewed = master - step_rate * (
        first_hat / (jnp.sqrt(second_hat) + ADAM_EPS) + decay_rate * master
    )
    return (renewed, jnp.stack([first_moment, second]))


def head_forward(raw, gain, cosine, sine):
    root = lax.rsqrt(jnp.mean(raw * raw, axis=-1, keepdims=True) + EPS_NORM)
    normed = raw * root
    scaled = normed * gain
    turned = scaled * cosine + pltpu.roll(scaled, HD // 2, 1) * sine
    return turned.astype(jnp.bfloat16), normed, root


def head_backward(grad, normed, root, gain, cosine, sine):
    turned = grad * cosine - pltpu.roll(grad, HD // 2, 1) * sine
    grad_gain = jnp.sum(turned * normed, axis=0, keepdims=True)
    scaled = turned * gain
    raw = root * (scaled - normed * jnp.mean(normed * scaled, axis=-1, keepdims=True))
    return raw, grad_gain


SPAN = 256


def fill_bias(bias_ref, row_ref, col_ref):
    key_at = lax.broadcasted_iota(jnp.int32, (SEQ_LEN, SEQ_LEN), 0)
    query_at = lax.broadcasted_iota(jnp.int32, (SEQ_LEN, SEQ_LEN), 1)
    allowed = (key_at <= query_at) & (col_ref[...] == row_ref[...])
    bias_ref[...] = jnp.where(allowed, 0.0, MASKED)


def span_weights(query_low, key_low, bias_ref, start):
    stop = start + SPAN
    scores = lax.dot_general(
        key_low[:stop],
        query_low[start:stop],
        (((1,), (1,)), ((), ())),
        preferred_element_type=jnp.float32,
    ) * (1.0 / math.sqrt(HD))
    scores = scores + bias_ref[:stop, start:stop]
    raised = jnp.exp(scores - jnp.max(scores, axis=0, keepdims=True))
    return raised * (1.0 / jnp.sum(raised, axis=0, keepdims=True))


def attend_body(
    query_ref, key_ref, value_ref, cos_ref, sin_ref, row_ref, col_ref, gain_ref, out_ref, bias_ref
):
    @pl.when(pl.program_id(1) == 0)
    def _():
        fill_bias(bias_ref, row_ref, col_ref)

    cosine, sine = cos_ref[...], sin_ref[...]
    key_low, _, _ = head_forward(key_ref[...], gain_ref[1:2, :], cosine, sine)
    value_turned = value_ref[...].astype(jnp.bfloat16).T
    for g in range(HQ // HK):
        at = slice(g * HD, (g + 1) * HD)
        query_low, _, _ = head_forward(query_ref[:, at], gain_ref[0:1, :], cosine, sine)
        for start in range(0, SEQ_LEN, SPAN):
            stop = start + SPAN
            weights = span_weights(query_low, key_low, bias_ref, start)
            mixed = jnp.dot(
                value_turned[:, :stop],
                weights.astype(jnp.bfloat16),
                preferred_element_type=jnp.float32,
            )
            out_ref[start:stop, at] = mixed.T.astype(jnp.bfloat16)


def attend_back_body(
    query_ref, key_ref, value_ref, cos_ref, sin_ref, row_ref, col_ref, gain_ref, grad_ref,
    *rest,
    first,
):
    out_ref, gain_out_ref, bias_ref = rest[-3:]
    head = pl.program_id(1) + first

    @pl.when(head == first)
    def _():
        fill_bias(bias_ref, row_ref, col_ref)

    cosine, sine = cos_ref[...], sin_ref[...]
    inv_head = 1.0 / math.sqrt(HD)

    @pl.when((pl.program_id(0) == 0) & (head == first))
    def _():
        gain_out_ref[...] = jnp.zeros_like(gain_out_ref)

    if len(rest) == 4:

        @pl.when(head == first)
        def _():
            out_ref[...] = rest[0][...]

    key_low, key_normed, key_root = head_forward(key_ref[...], gain_ref[1:2, :], cosine, sine)
    value_low = value_ref[...].astype(jnp.bfloat16)
    key_turned = key_low.T
    grad_key = [jnp.zeros((SPAN, HD), jnp.float32)] * (SEQ_LEN // SPAN)
    grad_value = list(grad_key)
    gain_query = jnp.zeros((1, HD), jnp.float32)
    for g in range(HQ // HK):
        at = slice(g * HD, (g + 1) * HD)
        query_low, normed, root = head_forward(query_ref[:, at], gain_ref[0:1, :], cosine, sine)
        grad_query = []
        for start in range(0, SEQ_LEN, SPAN):
            stop = start + SPAN
            weights = span_weights(query_low, key_low, bias_ref, start)
            grad_out = grad_ref[start:stop, at]
            grad_weights = lax.dot_general(
                value_low[:stop],
                grad_out,
                (((1,), (1,)), ((), ())),
                preferred_element_type=jnp.float32,
            )
            more_value = jnp.dot(
                weights.astype(jnp.bfloat16), grad_out, preferred_element_type=jnp.float32
            )
            product = weights * grad_weights
            grad_scores = (
                weights * (grad_weights - jnp.sum(product, axis=0, keepdims=True))
            ).astype(jnp.bfloat16)
            more_key = jnp.dot(
                grad_scores, query_low[start:stop], preferred_element_type=jnp.float32
            )
            grad_query.append(
                jnp.dot(
                    key_turned[:, :stop], grad_scores, preferred_element_type=jnp.float32
                ).T
            )
            for j in range(stop // SPAN):
                part = slice(j * SPAN, (j + 1) * SPAN)
                grad_key[j] = grad_key[j] + more_key[part]
                grad_value[j] = grad_value[j] + more_value[part]
        raw, more_gain = head_backward(
            jnp.concatenate(grad_query, axis=0) * inv_head,
            normed,
            root,
            gain_ref[0:1, :],
            cosine,
            sine,
        )
        gain_query = gain_query + more_gain
        place = pl.multiple_of((head * (HQ // HK) + g) * HD, HD)
        out_ref[:, pl.ds(place, HD)] = raw.astype(jnp.bfloat16)
    raw, gain_key = head_backward(
        jnp.concatenate(grad_key, axis=0) * inv_head,
        key_normed,
        key_root,
        gain_ref[1:2, :],
        cosine,
        sine,
    )
    out_ref[:, pl.ds(pl.multiple_of((HQ + head) * HD, HD), HD)] = raw.astype(jnp.bfloat16)
    out_ref[:, pl.ds(pl.multiple_of((HQ + HK + head) * HD, HD), HD)] = jnp.concatenate(
        grad_value, axis=0
    ).astype(jnp.bfloat16)
    gain_out_ref[0:1, :] += gain_query
    gain_out_ref[1:2, :] += gain_key


def attention_call(body, projected, tables, segments, gains, grad_out, first, count, base):
    token_rows = projected.shape[0]
    seq_count = token_rows // SEQ_LEN
    groups = HQ // HK
    wide = groups * HD
    full = lambda s, h: (s, 0)
    in_specs = [
        pl.BlockSpec((SEQ_LEN, wide), lambda s, h: (s, first + h)),
        pl.BlockSpec((SEQ_LEN, HD), lambda s, h: (s, HQ + first + h)),
        pl.BlockSpec((SEQ_LEN, HD), lambda s, h: (s, HQ + HK + first + h)),
        pl.BlockSpec((SEQ_LEN, HD), full),
        pl.BlockSpec((SEQ_LEN, HD), full),
        pl.BlockSpec((1, SEQ_LEN), lambda s, h: (0, s)),
        pl.BlockSpec((SEQ_LEN, 1), full),
        pl.BlockSpec((2, HD), lambda s, h: (0, 0)),
    ]
    operands = [
        projected,
        projected,
        projected,
        *tables,
        segments[None, :],
        segments[:, None],
        gains,
    ]
    pairs = token_rows * SEQ_LEN * groups * count
    aliases = {}
    if grad_out is None:
        out_specs = pl.BlockSpec((SEQ_LEN, wide), lambda s, h: (s, first + h))
        out_shape = jax.ShapeDtypeStruct((token_rows, HQ * HD), jnp.bfloat16)
    else:
        columns = projected.shape[1]
        in_specs.append(pl.BlockSpec((SEQ_LEN, wide), lambda s, h: (s, first + h)))
        operands.append(grad_out)
        body = functools.partial(body, first=first)
        if base is not None:
            aliases = {len(operands): 0}
            in_specs.append(pl.BlockSpec((SEQ_LEN, columns), full))
            operands.append(base)
        out_specs = [
            pl.BlockSpec((SEQ_LEN, columns), full),
            pl.BlockSpec((2, HD), lambda s, h: (0, 0)),
        ]
        out_shape = [
            jax.ShapeDtypeStruct((token_rows, columns), jnp.bfloat16),
            jax.ShapeDtypeStruct((2, HD), jnp.float32),
        ]
    return pl.pallas_call(
        body,
        grid=(seq_count, count),
        in_specs=in_specs,
        out_specs=out_specs,
        out_shape=out_shape,
        input_output_aliases=aliases,
        scratch_shapes=[pltpu.VMEM((SEQ_LEN, SEQ_LEN), jnp.float32)],
        compiler_params=pltpu.CompilerParams(vmem_limit_bytes=48 * 1024 * 1024),
        cost_estimate=pl.CostEstimate(
            flops=(4 if grad_out is None else 10) * pairs * HD * 2,
            bytes_accessed=projected.size * 6,
            transcendentals=pairs,
        ),
    )(*operands)


def gate_up_forward(hidden, full_gate_up):
    tokens, depth = hidden.shape
    block = 512
    steps = FF // block

    def body(hidden_ref, left_ref, right_ref, gate_ref, up_ref, out_ref):
        gate = jnp.dot(hidden_ref[...], left_ref[...], preferred_element_type=jnp.float32)
        upward = jnp.dot(hidden_ref[...], right_ref[...], preferred_element_type=jnp.float32)
        gate_ref[...] = gate
        up_ref[...] = upward
        out_ref[...] = (gate * jax.nn.sigmoid(gate) * upward).astype(jnp.bfloat16)

    wide = pl.BlockSpec((tokens, block), lambda j: (0, j))
    return pl.pallas_call(
        body,
        grid=(steps,),
        in_specs=[
            pl.BlockSpec((tokens, depth), lambda j: (0, 0)),
            pl.BlockSpec((depth, block), lambda j: (0, j)),
            pl.BlockSpec((depth, block), lambda j: (0, steps + j)),
        ],
        out_specs=[wide, wide, wide],
        out_shape=[
            jax.ShapeDtypeStruct((tokens, FF), jnp.float32),
            jax.ShapeDtypeStruct((tokens, FF), jnp.float32),
            jax.ShapeDtypeStruct((tokens, FF), jnp.bfloat16),
        ],
        compiler_params=pltpu.CompilerParams(vmem_limit_bytes=48 * 1024 * 1024),
        cost_estimate=pl.CostEstimate(
            flops=4 * tokens * FF * depth,
            bytes_accessed=4 * FF * depth + 10 * tokens * FF,
            transcendentals=tokens * FF,
        ),
    )(hidden, full_gate_up, full_gate_up)


def project_back(grad_low, weight, value, upstream, gain, whole):
    tokens, width = grad_low.shape
    depth = weight.shape[0]
    block = 1024
    steps = width // block

    def body(grad_ref, weight_ref, value_ref, up_ref, gain_ref, *rest):
        total_ref = rest[-1]
        step = pl.program_id(0)
        more = lax.dot_general(
            grad_ref[...],
            weight_ref[...],
            (((1,), (1,)), ((), ())),
            preferred_element_type=jnp.float32,
        )

        @pl.when(step == 0)
        def _():
            total_ref[...] = more

        @pl.when(step > 0)
        def _():
            total_ref[...] += more

        @pl.when(step == steps - 1)
        def _():
            raw = value_ref[...].astype(jnp.float32)
            root = lax.rsqrt(jnp.mean(raw * raw, axis=-1, keepdims=True) + EPS_NORM)
            normed = raw * root
            grad = total_ref[...]
            rest[1][...] = jnp.sum(grad * normed, axis=0, keepdims=True)
            full = up_ref[...].astype(jnp.float32) + norm_back(grad, normed, root, gain_ref[...])
            rest[0][...] = full.astype(jnp.bfloat16)
            if whole:
                rest[2][...] = full

    fixed = lambda j: (0, 0)
    square = pl.BlockSpec((tokens, depth), fixed)
    row = pl.BlockSpec((1, depth), fixed)
    shapes = [
        jax.ShapeDtypeStruct((tokens, depth), jnp.bfloat16),
        jax.ShapeDtypeStruct((1, depth), jnp.float32),
    ]
    if whole:
        shapes.append(jax.ShapeDtypeStruct((tokens, depth), jnp.float32))
    return pl.pallas_call(
        body,
        grid=(steps,),
        in_specs=[
            pl.BlockSpec((tokens, block), lambda j: (0, j)),
            pl.BlockSpec((depth, block), lambda j: (0, j)),
            square,
            square,
            row,
        ],
        out_specs=[square, row] + [square] * whole,
        out_shape=shapes,
        scratch_shapes=[pltpu.VMEM((tokens, depth), jnp.float32)],
        compiler_params=pltpu.CompilerParams(vmem_limit_bytes=48 * 1024 * 1024),
        cost_estimate=pl.CostEstimate(
            flops=2 * tokens * width * depth,
            bytes_accessed=2 * width * (depth + tokens) + 14 * tokens * depth,
            transcendentals=tokens,
        ),
    )(grad_low, weight, value, upstream, gain)


def gate_up_back(cotangent, full_down, gate_part, upward):
    tokens, columns = cotangent.shape
    block = 512
    steps = FF // block

    def body(cot_ref, down_ref, gate_ref, up_ref, out_ref):
        at = pl.program_id(0) * block
        grad = lax.dot_general(
            cot_ref[...],
            down_ref[...],
            (((1,), (1,)), ((), ())),
            preferred_element_type=jnp.float32,
        )
        gate = gate_ref[...]
        part = jax.nn.sigmoid(gate)
        grad_gate = grad * up_ref[...] * part * (1.0 + gate * (1.0 - part))
        grad_up = grad * gate * part
        out_ref[:, pl.ds(pl.multiple_of(at, block), block)] = grad_gate.astype(jnp.bfloat16)
        out_ref[:, pl.ds(pl.multiple_of(at + FF, block), block)] = grad_up.astype(jnp.bfloat16)

    return pl.pallas_call(
        body,
        grid=(steps,),
        in_specs=[
            pl.BlockSpec((tokens, columns), lambda j: (0, 0)),
            pl.BlockSpec((block, columns), lambda j: (j, 0)),
            pl.BlockSpec((tokens, block), lambda j: (0, j)),
            pl.BlockSpec((tokens, block), lambda j: (0, j)),
        ],
        out_specs=pl.BlockSpec((tokens, 2 * FF), lambda j: (0, 0)),
        out_shape=jax.ShapeDtypeStruct((tokens, 2 * FF), jnp.bfloat16),
        compiler_params=pltpu.CompilerParams(vmem_limit_bytes=48 * 1024 * 1024),
        cost_estimate=pl.CostEstimate(
            flops=2 * tokens * FF * columns,
            bytes_accessed=2 * FF * columns + 12 * tokens * FF,
            transcendentals=tokens * FF,
        ),
    )(cotangent, full_down, gate_part, upward)


def on_device(
    tokens,
    segment_ids,
    positions,
    cotangent,
    qkv_weight,
    out_weight,
    gate_up_weight,
    down_weight,
    norm_gains,
    head_gains,
    qkv_moments,
    out_moments,
    gate_up_moments,
    down_moments,
    norm_moments,
    head_moments,
):
    width = norm_gains.shape[1]
    gains_low = jnp.concatenate([norm_gains, head_gains], axis=1).astype(jnp.bfloat16)
    owners = lax.axis_size(GROUP)
    gains_all = gather_small(gains_low).reshape(2, owners, -1)
    full_norm = gains_all[:, :, :width].reshape(2, -1)
    full_head = gains_all[:, :, width:].reshape(2, -1)
    full_qkv, first, late, _ = gather_rows(qkv_weight, None, None, None, None, None)
    gain_one = full_norm[0].astype(jnp.float32)
    gain_two = full_norm[1].astype(jnp.float32)
    head_gain = full_head.astype(jnp.float32)
    inputs = tokens.astype(jnp.float32)
    root_one = lax.rsqrt(jnp.mean(inputs * inputs, axis=-1, keepdims=True) + EPS_NORM)
    normed_one = inputs * root_one
    hidden_one = (normed_one * gain_one).astype(jnp.bfloat16)
    projected = jnp.dot(hidden_one, full_qkv, preferred_element_type=jnp.float32)
    tables = rotary_tables(positions, HD)
    mixed_low = attention_call(attend_body, projected, tables, segment_ids, head_gain, None, 0, HK, None)
    full_out, _, down_late, _ = gather_rows(out_weight, first, late, None, projected, mixed_low)
    full_gate_up, _, more_late, _ = gather_rows(gate_up_weight, first, late, projected, None, None)
    attended = jnp.dot(mixed_low, full_out, preferred_element_type=jnp.float32)
    residual = inputs + attended
    root_two = lax.rsqrt(jnp.mean(residual * residual, axis=-1, keepdims=True) + EPS_NORM)
    normed_two = residual * root_two
    hidden_two = (normed_two * gain_two).astype(jnp.bfloat16)
    gate_part, upward, activated = gate_up_forward(hidden_two, full_gate_up)
    full_down, _, _, _ = gather_rows(
        down_weight, first, (down_late, more_late, projected), None, full_gate_up, activated
    )
    down_sum = GradSum(activated, cotangent, True)
    grad_gate_up = gate_up_back(
        after(cotangent, *down_sum.blocks), full_down, gate_part, upward
    )
    gate_up_sum = GradSum(hidden_two, after(grad_gate_up, *down_sum.advance()), True)
    residual_low, grad_gain_two, grad_residual = project_back(
        after(grad_gate_up, *gate_up_sum.blocks),
        full_gate_up,
        residual,
        cotangent,
        gain_two[None],
        True,
    )
    down_sum.hold(residual_low)
    sent = down_sum.advance() + gate_up_sum.advance()
    out_sum = GradSum(mixed_low, after(residual_low, *sent), True)
    down_sum.hold(out_sum.blocks)
    grad_mixed = contract_cols(
        after(residual_low, *out_sum.blocks, *down_sum.advance()), full_out
    ).astype(jnp.bfloat16)
    grad_mixed = after(grad_mixed, *out_sum.advance())
    half = HK // 2
    grad_half, gain_half = attention_call(
        attend_back_body, projected, tables, segment_ids, head_gain, grad_mixed, 0, half, None
    )
    gate_up_sum.hold(grad_half)
    down_sum.hold(grad_half)
    sent = gate_up_sum.advance() + down_sum.advance()
    grad_projected, grad_gain_head = attention_call(
        attend_back_body,
        projected,
        tables,
        segment_ids,
        head_gain,
        grad_mixed,
        half,
        HK - half,
        after(grad_half, *sent),
    )
    grad_gain_head = grad_gain_head + gain_half
    gate_up_sum.hold(grad_projected)
    out_sum.hold(grad_projected)
    sent = gate_up_sum.advance() + out_sum.advance()
    qkv_sum = GradSum(hidden_one, after(grad_projected, *sent), True)
    gate_up_sum.hold(qkv_sum.blocks)
    sent = qkv_sum.advance()
    gate_up_sum.hold(sent)
    out_sum.hold(sent)
    down_sum.hold(sent)
    sent = sent + gate_up_sum.advance() + out_sum.advance()
    branch = jnp.dot(after(activated, *sent), full_down, preferred_element_type=jnp.float32)
    output = (residual + branch).astype(jnp.bfloat16)
    tokens_grad, grad_gain_one = project_back(
        after(grad_projected, *qkv_sum.blocks, *sent),
        full_qkv,
        tokens,
        grad_residual,
        gain_one[None],
        False,
    )
    small = jnp.concatenate(
        [jnp.concatenate([grad_gain_one, grad_gain_two]), grad_gain_head],
        axis=1,
    )
    sent_next = qkv_sum.advance()
    qkv_own, out_own, gate_up_own, down_own = owned = tuple(
        v.finish() for v in (qkv_sum, out_sum, gate_up_sum, down_sum)
    )
    down_gathered = gather_grad(after(down_own, *sent_next), None, None)
    local = sum(jnp.sum(v * v) for v in owned)
    partial = jnp.concatenate(
        [small, jnp.full((6, small.shape[1]), local, jnp.float32)], axis=0
    )
    summed = sum_all(after(partial, down_gathered[0][0]))
    small = summed[:2]
    norm_total = small[:, :-HD]
    head_total = small[:, -HD:]
    squares = summed[2, 0] + jnp.sum(small * small)
    clip_limit = math.sqrt(PARAMS)
    factor = clip_limit / jnp.maximum(jnp.sqrt(squares), clip_limit)
    renewed_down = adam_blocks(
        down_weight, down_moments, down_gathered, factor, LEARN_RATE, WEIGHT_DECAY
    )
    gathered = [
        gather_grad(after(qkv_own, summed), renewed_down[0], None),
        gather_grad(after(out_own, *sent_next), None, None),
        gather_grad(after(gate_up_own, *sent_next), None, summed),
    ]
    later = after(factor, gathered[0][0][0])
    renewed_gate_up = adam_blocks(
        gate_up_weight, gate_up_moments, gathered[2], later, LEARN_RATE, WEIGHT_DECAY
    )
    later = after(factor, renewed_gate_up[0])
    renewed_out = adam_blocks(
        out_weight, out_moments, gathered[1], later, LEARN_RATE, WEIGHT_DECAY
    )
    later = after(factor, renewed_out[0])
    renewed_qkv = adam_blocks(
        qkv_weight, qkv_moments, gathered[0], later, LEARN_RATE, WEIGHT_DECAY
    )
    renewed = [renewed_qkv, renewed_out, renewed_gate_up]
    renewed.append(renewed_down)
    mine = lax.axis_index(GROUP)
    norm_grad = lax.dynamic_slice_in_dim(
        norm_total, mine * norm_gains.shape[1], norm_gains.shape[1], 1
    )
    head_grad = lax.dynamic_slice_in_dim(
        head_total, mine * head_gains.shape[1], head_gains.shape[1], 1
    )
    renewed.append(adam_update(norm_gains, norm_moments, norm_grad, factor, GAIN_RATE, 0.0))
    renewed.append(adam_update(head_gains, head_moments, head_grad, factor, GAIN_RATE, 0.0))
    return (
        output,
        tokens_grad,
        *owned,
        norm_grad,
        head_grad,
        *[new for new, _ in renewed],
        *[state for _, state in renewed],
    )


def solution(mesh):
    placed = (
        P((DP, GROUP), None),
        P((DP, GROUP)),
        P((DP, GROUP)),
        P((DP, GROUP), None),
        P(GROUP, None),
        P(GROUP, None),
        P(GROUP, None),
        P(GROUP, None),
        P(None, GROUP),
        P(None, GROUP),
        P(None, GROUP, None),
        P(None, GROUP, None),
        P(None, GROUP, None),
        P(None, GROUP, None),
        P(None, None, GROUP),
        P(None, None, GROUP),
    )
    return jax.shard_map(
        on_device,
        mesh=mesh,
        in_specs=placed,
        out_specs=(
            P((DP, GROUP), None),
            P((DP, GROUP), None),
            P(GROUP, DP),
            P(GROUP, DP),
            P(GROUP, DP),
            P(GROUP, DP),
            P(None, GROUP),
            P(None, GROUP),
            P(GROUP, None),
            P(GROUP, None),
            P(GROUP, None),
            P(GROUP, None),
            P(None, GROUP),
            P(None, GROUP),
            P(None, GROUP, None),
            P(None, GROUP, None),
            P(None, GROUP, None),
            P(None, GROUP, None),
            P(None, None, GROUP),
            P(None, None, GROUP),
        ),
        check_vma=False,
    )
```

```python
import functools
import math

import jax
import jax.numpy as jnp
from jax import lax
from jax.experimental import pallas as pl
from jax.experimental.pallas import tpu as pltpu
from jax.sharding import PartitionSpec as P


HQ = 16
HK = 8
HD = 128
FF = 3072
SEQ_LEN = 512
PARAMS = 15730944
GROUP = "group"
DP = "dp"


EPS_NORM = 1e-06
ROPE_BASE = 1000000.0
MASKED = -1e30
LEARN_RATE = 0.03
GAIN_RATE = 0.3
WEIGHT_DECAY = 0.1
BETA_ONE = 0.9
BETA_TWO = 0.95
ADAM_EPS = 1e-08
STEP_COUNT = 3.0


def rotary_tables(places, width):
    half_width = width // 2
    frequency = ROPE_BASE ** (-(jnp.arange(half_width, dtype=jnp.float32) * 2.0) / width)
    angles = places.astype(jnp.float32)[:, None] * frequency[None, :]
    cosine, sine = jnp.cos(angles), jnp.sin(angles)
    return (
        jnp.concatenate([cosine, cosine], axis=1),
        jnp.concatenate([-sine, sine], axis=1),
    )


def contract_rows(left_side, right_side):
    return lax.dot_general(
        left_side, right_side, (((0,), (0,)), ((), ())), preferred_element_type=jnp.float32
    )


def contract_cols(left_side, right_side):
    return lax.dot_general(
        left_side, right_side, (((1,), (1,)), ((), ())), preferred_element_type=jnp.float32
    )


def norm_back(grad_out, normed, inv_root, gain):
    scaled = grad_out * gain
    return inv_root * (scaled - normed * jnp.mean(normed * scaled, axis=-1, keepdims=True))


def swap(value, axis, mask):
    count = lax.axis_size(axis)
    return lax.ppermute(value, axis, [(i, i ^ mask) for i in range(count)])


def bit_masks(count):
    return [1 << i for i in range(count.bit_length() - 1)]


def after(value, *others):
    return lax.optimization_barrier((value, others))[0]


def place_rows(pieces, rows, owners):
    columns = pieces[0][0].shape[1]
    kind = pieces[0][0].dtype
    sizes = [v.shape[0] for v, _, _ in pieces]

    def body(*refs):
        count = len(pieces)
        ins, out_ref, held = refs[:count], refs[count], refs[count + 1]
        into, away = refs[count + 2 :]
        mine = lax.axis_index(GROUP)
        here = lax.axis_index(DP)
        arriving, leaving, at = [], [], 0
        for k, (_, delta, offset) in enumerate(pieces):
            slot = held.at[pl.ds(at, sizes[k])]
            start = pl.multiple_of((mine ^ delta) * rows + offset(here), 16)
            arriving.append(pltpu.make_async_copy(ins[k], slot, into.at[k]))
            leaving.append(
                pltpu.make_async_copy(slot, out_ref.at[pl.ds(start, sizes[k])], away.at[k])
            )
            at += sizes[k]
        for copy in arriving:
            copy.start()
        for first, second in zip(arriving, leaving):
            first.wait()
            second.start()
        for copy in leaving:
            copy.wait()

    return pl.pallas_call(
        body,
        out_shape=jax.ShapeDtypeStruct((rows * owners, columns), kind),
        in_specs=[pl.BlockSpec(memory_space=pl.ANY)] * len(pieces),
        out_specs=pl.BlockSpec(memory_space=pl.ANY),
        scratch_shapes=[
            pltpu.VMEM((rows * owners, columns), kind),
            pltpu.SemaphoreType.DMA((len(pieces),)),
            pltpu.SemaphoreType.DMA((len(pieces),)),
        ],
        compiler_params=pltpu.CompilerParams(vmem_limit_bytes=32 * 1024 * 1024),
        cost_estimate=pl.CostEstimate(
            flops=0, bytes_accessed=4 * rows * owners * columns, transcendentals=0
        ),
    )(*[v for v, _, _ in pieces])


def gather_rows(shard, early, late, middle, third, hold):
    owners = lax.axis_size(GROUP)
    copies = lax.axis_size(DP)
    here = lax.axis_index(DP)
    if early is not None:
        shard = after(shard, early)
    shard = shard.astype(jnp.bfloat16)
    rows, _ = shard.shape

    def none(_):
        return 0

    pieces = [(shard, 0, none)]
    near = order = by_one = by_two = shard
    if owners == 4 and copies % 4 == 0 and rows % 128 == 0:
        quarter, half = rows // 4, rows // 8

        def place(here):
            return (here & 1) * 2 + ((here >> 1) & 1)

        def quarter_at(mask, more=0):
            return lambda here: (place(here) ^ mask) * quarter + more

        near = lax.dynamic_slice_in_dim(shard, place(here) * quarter, quarter, 0)
        if late is not None:
            near = after(near, late)
        order = swap(near, GROUP, 2)
        passed = order if middle is None else after(order, middle)
        by_one = swap(passed, DP, 1)
        by_two = swap(passed, DP, 2)
        go_one, go_two = by_one, by_two
        if third is not None:
            go_one, go_two = after((by_one, by_two), third)
        last_one = swap(go_two[:half], DP, 1)
        last_two = swap(go_one[half:], DP, 2)
        if hold is not None:
            last_one, last_two = after((last_one, last_two), hold)
        pieces += [
            (order, 2, quarter_at(0)),
            (go_one, 2, quarter_at(2)),
            (go_two, 2, quarter_at(1)),
            (last_one, 2, quarter_at(3)),
            (last_two, 2, quarter_at(3, half)),
        ]
    else:
        for mask in bit_masks(owners)[1:]:
            pieces += [(swap(v, GROUP, mask), dg ^ mask, at) for v, dg, at in pieces]
    pieces += [(swap(v, GROUP, 1), dg ^ 1, at) for v, dg, at in pieces]
    if hold is not None:
        pieces[0] = (after(shard, hold), 0, none)
    full = place_rows(pieces, rows, owners)
    return full, near, order, (by_one, by_two)


def gather_small(shard):
    owners = lax.axis_size(GROUP)
    mine = lax.axis_index(GROUP)
    width = shard.shape[1]
    held = shard[None]
    deltas = [0]
    for mask in reversed(bit_masks(owners)):
        held = jnp.concatenate([held, swap(held, GROUP, mask)], axis=0)
        deltas += [d ^ mask for d in deltas]
    full = jnp.zeros((shard.shape[0], width * owners), shard.dtype)
    for k, delta in enumerate(deltas):
        full = lax.dynamic_update_slice(full, held[k], (0, (mine ^ delta) * width))
    return full


def sum_all(value):
    owners = lax.axis_size(GROUP)
    copies = lax.axis_size(DP)
    mesh_type = pl.DeviceIdType.MESH

    def body(in_ref, out_ref, near, near_sum, far, near_send, near_recv, far_send, far_recv):
        mine = lax.axis_index(GROUP)
        here = lax.axis_index(DP)
        near_peers = [(here, mine ^ k) for k in range(1, owners)]
        far_peers = [(here ^ k, mine) for k in range(1, copies)]
        barrier = pltpu.get_barrier_semaphore()
        for peer in near_peers + far_peers:
            pl.semaphore_signal(barrier, inc=1, device_id=peer, device_id_type=mesh_type)
        pl.semaphore_wait(barrier, len(near_peers) + len(far_peers))

        def exchange(source, slots, index, peers, sends, recvs):
            slots[index] = source[...]
            copies_out = [
                pltpu.make_async_remote_copy(
                    src_ref=source,
                    dst_ref=slots.at[index],
                    send_sem=sends.at[k],
                    recv_sem=recvs.at[k],
                    device_id=peer,
                    device_id_type=mesh_type,
                )
                for k, peer in enumerate(peers)
            ]
            for copy in copies_out:
                copy.start()
            for copy in copies_out:
                copy.wait()
            total = slots[0]
            for k in range(1, len(peers) + 1):
                total = total + slots[k]
            return total

        near_sum[...] = exchange(in_ref, near, mine, near_peers, near_send, near_recv)
        out_ref[...] = exchange(near_sum, far, here, far_peers, far_send, far_recv)

    shape = value.shape
    return pl.pallas_call(
        body,
        out_shape=jax.ShapeDtypeStruct(shape, jnp.float32),
        in_specs=[pl.BlockSpec(memory_space=pltpu.VMEM)],
        out_specs=pl.BlockSpec(memory_space=pltpu.VMEM),
        scratch_shapes=[
            pltpu.VMEM((owners,) + shape, jnp.float32),
            pltpu.VMEM(shape, jnp.float32),
            pltpu.VMEM((copies,) + shape, jnp.float32),
            pltpu.SemaphoreType.DMA((owners - 1,)),
            pltpu.SemaphoreType.DMA((owners - 1,)),
            pltpu.SemaphoreType.DMA((copies - 1,)),
            pltpu.SemaphoreType.DMA((copies - 1,)),
        ],
        compiler_params=pltpu.CompilerParams(collective_id=0, has_side_effects=True),
    )(value)


def spread_bits(position, masks):
    total = 0
    count = len(masks)
    for i, mask in enumerate(masks):
        total = total + ((position >> (count - 1 - i)) & 1) * mask
    return total


def grad_blocks(left, right):
    tokens, rows = left.shape
    columns = right.shape[1]
    owners = lax.axis_size(GROUP)
    copies = lax.axis_size(DP)
    column_masks = bit_masks(copies)
    later = bit_masks(owners)[1:]
    staying = [spread_bits(p, later) for p in range(1 << len(later))]
    row_sets = [[dg + 1 for dg in staying], staying] if owners > 1 else [[0]]
    row_block = rows // owners
    column_block = columns // copies
    mine = lax.axis_index(GROUP)
    here = lax.axis_index(DP)
    if column_block % 128 or row_block % 16:
        ordered = jnp.concatenate(
            [
                lax.dynamic_slice_in_dim(
                    right, (here ^ spread_bits(p, column_masks)) * column_block, column_block, 1
                )
                for p in range(copies)
            ],
            axis=1,
        )
        return [
            jnp.stack(
                [
                    contract_rows(
                        lax.dynamic_slice_in_dim(left, (mine ^ dg) * row_block, row_block, 1),
                        ordered,
                    ).astype(jnp.bfloat16)
                    for dg in row_set
                ]
            )
            for row_set in row_sets
        ]
    wide = 2 if column_block % 256 and copies % 2 == 0 else 1

    def body(where, left_ref, *rest):
        rights, outs, turned = rest[:wide], rest[wide:-1], rest[-1]

        @pl.when(pl.program_id(0) == 0)
        def _():
            turned[...] = left_ref[...].T

        block = jnp.concatenate([ref[...] for ref in rights], axis=1)
        for out, row_set in zip(outs, row_sets):
            for k, dg in enumerate(row_set):
                start = pl.multiple_of((where[0] ^ dg) * row_block, row_block)
                out[k] = jnp.dot(
                    turned[pl.ds(start, row_block), :],
                    block,
                    preferred_element_type=jnp.float32,
                ).astype(jnp.bfloat16)

    def right_spec(j):
        return pl.BlockSpec(
            (tokens, column_block),
            lambda p, where: (0, where[1] ^ spread_bits(p * wide + j, column_masks)),
        )

    return pl.pallas_call(
        body,
        out_shape=[
            jax.ShapeDtypeStruct((len(row_set), row_block, columns), jnp.bfloat16)
            for row_set in row_sets
        ],
        grid_spec=pltpu.PrefetchScalarGridSpec(
            num_scalar_prefetch=1,
            grid=(copies // wide,),
            in_specs=[pl.BlockSpec((tokens, rows), lambda p, where: (0, 0))]
            + [right_spec(j) for j in range(wide)],
            out_specs=[
                pl.BlockSpec(
                    (len(row_set), row_block, column_block * wide), lambda p, where: (0, 0, p)
                )
                for row_set in row_sets
            ],
            scratch_shapes=[pltpu.VMEM((rows, tokens), jnp.bfloat16)],
        ),
        compiler_params=pltpu.CompilerParams(vmem_limit_bytes=48 * 1024 * 1024),
        cost_estimate=pl.CostEstimate(
            flops=2 * tokens * rows * columns,
            bytes_accessed=2 * (tokens * rows + tokens * columns + rows * columns),
            transcendentals=0,
        ),
    )(jnp.stack([mine, here]).astype(jnp.int32), left, *[right] * wide)


class GradSum:
    def __init__(self, left, right, split):
        blocks = grad_blocks(left, right)
        self.blocks = blocks
        group = [(GROUP, m) for m in bit_masks(lax.axis_size(GROUP))]
        other = [(DP, m) for m in bit_masks(lax.axis_size(DP))]
        self.arrays = [blocks[-1]]
        if group:
            self.arrays.append(swap(blocks[0], GROUP, 1))
        rest = group[1:]
        self.orders = [rest + other]
        if split:
            self.orders.append(other[:1] + rest + other[1:])
        count = len(self.orders)
        deep, tall, width = blocks[-1].shape
        size = tall // count
        self.parts = [
            [(k, [(0, deep), (i * size, (i + 1) * size), (0, width)]) for k in range(len(self.arrays))]
            for i in range(count)
        ]
        self.common = len(rest) + 1
        self.length = len(rest) + len(other)
        self.step = 0

    def hold(self, *others):
        self.arrays = list(lax.optimization_barrier((self.arrays, others))[0])

    def read(self, part):
        total = 0.0
        for k, ranges in part:
            at = tuple(slice(*r) for r in ranges)
            total = total + self.arrays[k][at].astype(jnp.float32)
        return total

    def exchange(self, away, axis, mask):
        self.arrays.append(swap(away, axis, mask))
        return len(self.arrays) - 1

    def advance(self):
        if self.step == self.length:
            return []
        outgoing = []
        for i, order in enumerate(self.orders):
            axis, mask = order[self.step]
            dim = 0 if axis == GROUP else 2
            far, near = [], []
            for k, ranges in self.parts[i]:
                start, stop = ranges[dim]
                middle = (start + stop) // 2
                near.append((k, ranges[:dim] + [(start, middle)] + ranges[dim + 1 :]))
                far.append((k, ranges[:dim] + [(middle, stop)] + ranges[dim + 1 :]))
            self.parts[i] = near
            outgoing.append((self.read(far).astype(jnp.bfloat16), axis, mask))
        deep, tall, width = outgoing[0][0].shape
        if self.step >= self.common:
            away = jnp.concatenate([v for v, _, _ in outgoing], axis=1)
            sent = [away]
            k = self.exchange(away, *outgoing[0][1:])
            for i, part in enumerate(self.parts):
                part.append((k, [(0, deep), (i * tall, (i + 1) * tall), (0, width)]))
        else:
            sent = [v for v, _, _ in outgoing]
            for i, (away, axis, mask) in enumerate(outgoing):
                k = self.exchange(away, axis, mask)
                deep, tall, width = away.shape
                self.parts[i].append((k, [(0, deep), (0, tall), (0, width)]))
        self.step += 1
        return sent

    def finish(self):
        while self.step < self.length:
            self.advance()
        return jnp.concatenate([self.read(part)[0] for part in self.parts], axis=0)


def gather_grad(own, second, last):
    held = own.astype(jnp.bfloat16)[None]
    deltas = [0]
    groups = [(held, deltas)]
    masks = list(reversed(bit_masks(lax.axis_size(DP))))
    for i, mask in enumerate(masks):
        away = held
        if i == 1 and second is not None:
            away = after(away, second)
        if i + 1 == len(masks) and last is not None:
            away = after(away, last)
        got = swap(away, DP, mask)
        got_deltas = [d ^ mask for d in deltas]
        if i + 1 < len(masks):
            held = jnp.concatenate([held, got], axis=0)
            deltas = deltas + got_deltas
            groups = [(held, deltas)]
        else:
            groups.append((got, got_deltas))
    return groups


def adam_core(master, first_moment, second_moment, clipped, step_rate, decay_rate):
    first_new = BETA_ONE * first_moment + (1.0 - BETA_ONE) * clipped
    second_new = BETA_TWO * second_moment + (1.0 - BETA_TWO) * clipped * clipped
    first_hat = first_new * (1.0 / (1.0 - BETA_ONE**STEP_COUNT))
    second_hat = second_new * (1.0 / (1.0 - BETA_TWO**STEP_COUNT))
    renewed = master - step_rate * (
        first_hat / (jnp.sqrt(second_hat) + ADAM_EPS) + decay_rate * master
    )
    return renewed, first_new, second_new


def adam_blocks(master, moment, blocks, factor, step_rate, decay_rate):
    rows, columns = master.shape
    copies = lax.axis_size(DP)
    here = lax.axis_index(DP)
    width = columns // copies
    if width % 128:
        full = jnp.zeros(master.shape, jnp.float32)
        for value, deltas in blocks:
            for k, dd in enumerate(deltas):
                full = lax.dynamic_update_slice(
                    full, value[k].astype(jnp.float32), (0, (here ^ dd) * width)
                )
        return adam_update(master, moment, full, factor, step_rate, decay_rate)
    tile = rows
    while tile % 32 == 0 and tile * columns > 256 * 1024:
        tile //= 2

    def body(where, factor_ref, master_ref, moment_ref, *rest):
        grads, (new_ref, state_ref) = rest[:-2], rest[-2:]
        scale = factor_ref[0, 0]
        for grad, (_, deltas) in zip(grads, blocks):
            for k, dd in enumerate(deltas):
                at = pl.ds(pl.multiple_of((where[0] ^ dd) * width, 128), width)
                renewed, first_new, second_new = adam_core(
                    master_ref[:, at],
                    moment_ref[0, :, at],
                    moment_ref[1, :, at],
                    grad[k].astype(jnp.float32) * scale,
                    step_rate,
                    decay_rate,
                )
                new_ref[:, at] = renewed
                state_ref[0, :, at] = first_new
                state_ref[1, :, at] = second_new

    return pl.pallas_call(
        body,
        out_shape=[
            jax.ShapeDtypeStruct(master.shape, jnp.float32),
            jax.ShapeDtypeStruct(moment.shape, jnp.float32),
        ],
        grid_spec=pltpu.PrefetchScalarGridSpec(
            num_scalar_prefetch=1,
            grid=(rows // tile,),
            in_specs=[
                pl.BlockSpec(memory_space=pltpu.SMEM),
                pl.BlockSpec((tile, columns), lambda i, where: (i, 0)),
                pl.BlockSpec((2, tile, columns), lambda i, where: (0, i, 0)),
            ]
            + [
                pl.BlockSpec((len(deltas), tile, width), lambda i, where: (0, i, 0))
                for _, deltas in blocks
            ],
            out_specs=[
                pl.BlockSpec((tile, columns), lambda i, where: (i, 0)),
                pl.BlockSpec((2, tile, columns), lambda i, where: (0, i, 0)),
            ],
        ),
        compiler_params=pltpu.CompilerParams(vmem_limit_bytes=48 * 1024 * 1024),
        cost_estimate=pl.CostEstimate(
            flops=20 * rows * columns,
            bytes_accessed=26 * rows * columns,
            transcendentals=rows * columns,
        ),
    )(
        here.reshape(1).astype(jnp.int32),
        factor.reshape(1, 1),
        master,
        moment,
        *[value for value, _ in blocks],
    )


def adam_update(master, moment, gradient, factor, step_rate, decay_rate):
    clipped = gradient * factor
    first_moment = BETA_ONE * moment[0] + (1.0 - BETA_ONE) * clipped
    second = BETA_TWO * moment[1] + (1.0 - BETA_TWO) * clipped * clipped
    first_hat = first_moment / (1.0 - BETA_ONE**STEP_COUNT)
    second_hat = second / (1.0 - BETA_TWO**STEP_COUNT)
    renewed = master - step_rate * (
        first_hat / (jnp.sqrt(second_hat) + ADAM_EPS) + decay_rate * master
    )
    return (renewed, jnp.stack([first_moment, second]))


def head_forward(raw, gain, cosine, sine):
    root = lax.rsqrt(jnp.mean(raw * raw, axis=-1, keepdims=True) + EPS_NORM)
    normed = raw * root
    scaled = normed * gain
    turned = scaled * cosine + pltpu.roll(scaled, HD // 2, 1) * sine
    return turned.astype(jnp.bfloat16), normed, root


def head_backward(grad, normed, root, gain, cosine, sine):
    turned = grad * cosine - pltpu.roll(grad, HD // 2, 1) * sine
    grad_gain = jnp.sum(turned * normed, axis=0, keepdims=True)
    scaled = turned * gain
    raw = root * (scaled - normed * jnp.mean(normed * scaled, axis=-1, keepdims=True))
    return raw, grad_gain


SPAN = 256


def fill_bias(bias_ref, row_ref, col_ref):
    key_at = lax.broadcasted_iota(jnp.int32, (SEQ_LEN, SEQ_LEN), 0)
    query_at = lax.broadcasted_iota(jnp.int32, (SEQ_LEN, SEQ_LEN), 1)
    allowed = (key_at <= query_at) & (col_ref[...] == row_ref[...])
    bias_ref[...] = jnp.where(allowed, 0.0, MASKED)


def span_weights(query_low, key_low, bias_ref, start):
    stop = start + SPAN
    scores = lax.dot_general(
        key_low[:stop],
        query_low[start:stop],
        (((1,), (1,)), ((), ())),
        preferred_element_type=jnp.float32,
    ) * (1.0 / math.sqrt(HD))
    scores = scores + bias_ref[:stop, start:stop]
    raised = jnp.exp(scores - jnp.max(scores, axis=0, keepdims=True))
    return raised * (1.0 / jnp.sum(raised, axis=0, keepdims=True))


def attend_body(
    query_ref, key_ref, value_ref, cos_ref, sin_ref, row_ref, col_ref, gain_ref, out_ref, bias_ref
):
    @pl.when(pl.program_id(1) == 0)
    def _():
        fill_bias(bias_ref, row_ref, col_ref)

    cosine, sine = cos_ref[...], sin_ref[...]
    key_low, _, _ = head_forward(key_ref[...], gain_ref[1:2, :], cosine, sine)
    value_turned = value_ref[...].astype(jnp.bfloat16).T
    for g in range(HQ // HK):
        at = slice(g * HD, (g + 1) * HD)
        query_low, _, _ = head_forward(query_ref[:, at], gain_ref[0:1, :], cosine, sine)
        for start in range(0, SEQ_LEN, SPAN):
            stop = start + SPAN
            weights = span_weights(query_low, key_low, bias_ref, start)
            mixed = jnp.dot(
                value_turned[:, :stop],
                weights.astype(jnp.bfloat16),
                preferred_element_type=jnp.float32,
            )
            out_ref[start:stop, at] = mixed.T.astype(jnp.bfloat16)


def attend_back_body(
    query_ref, key_ref, value_ref, cos_ref, sin_ref, row_ref, col_ref, gain_ref, grad_ref,
    *rest,
    first,
):
    out_ref, gain_out_ref, bias_ref = rest[-3:]
    head = pl.program_id(1) + first

    @pl.when(head == first)
    def _():
        fill_bias(bias_ref, row_ref, col_ref)

    cosine, sine = cos_ref[...], sin_ref[...]
    inv_head = 1.0 / math.sqrt(HD)

    @pl.when((pl.program_id(0) == 0) & (head == first))
    def _():
        gain_out_ref[...] = jnp.zeros_like(gain_out_ref)

    if len(rest) == 4:

        @pl.when(head == first)
        def _():
            out_ref[...] = rest[0][...]

    key_low, key_normed, key_root = head_forward(key_ref[...], gain_ref[1:2, :], cosine, sine)
    value_low = value_ref[...].astype(jnp.bfloat16)
    key_turned = key_low.T
    grad_key = [jnp.zeros((SPAN, HD), jnp.float32)] * (SEQ_LEN // SPAN)
    grad_value = list(grad_key)
    gain_query = jnp.zeros((1, HD), jnp.float32)
    for g in range(HQ // HK):
        at = slice(g * HD, (g + 1) * HD)
        query_low, normed, root = head_forward(query_ref[:, at], gain_ref[0:1, :], cosine, sine)
        grad_query = []
        for start in range(0, SEQ_LEN, SPAN):
            stop = start + SPAN
            weights = span_weights(query_low, key_low, bias_ref, start)
            grad_out = grad_ref[start:stop, at]
            grad_weights = lax.dot_general(
                value_low[:stop],
                grad_out,
                (((1,), (1,)), ((), ())),
                preferred_element_type=jnp.float32,
            )
            more_value = jnp.dot(
                weights.astype(jnp.bfloat16), grad_out, preferred_element_type=jnp.float32
            )
            product = weights * grad_weights
            grad_scores = (
                weights * (grad_weights - jnp.sum(product, axis=0, keepdims=True))
            ).astype(jnp.bfloat16)
            more_key = jnp.dot(
                grad_scores, query_low[start:stop], preferred_element_type=jnp.float32
            )
            grad_query.append(
                jnp.dot(
                    key_turned[:, :stop], grad_scores, preferred_element_type=jnp.float32
                ).T
            )
            for j in range(stop // SPAN):
                part = slice(j * SPAN, (j + 1) * SPAN)
                grad_key[j] = grad_key[j] + more_key[part]
                grad_value[j] = grad_value[j] + more_value[part]
        raw, more_gain = head_backward(
            jnp.concatenate(grad_query, axis=0) * inv_head,
            normed,
            root,
            gain_ref[0:1, :],
            cosine,
            sine,
        )
        gain_query = gain_query + more_gain
        place = pl.multiple_of((head * (HQ // HK) + g) * HD, HD)
        out_ref[:, pl.ds(place, HD)] = raw.astype(jnp.bfloat16)
    raw, gain_key = head_backward(
        jnp.concatenate(grad_key, axis=0) * inv_head,
        key_normed,
        key_root,
        gain_ref[1:2, :],
        cosine,
        sine,
    )
    out_ref[:, pl.ds(pl.multiple_of((HQ + head) * HD, HD), HD)] = raw.astype(jnp.bfloat16)
    out_ref[:, pl.ds(pl.multiple_of((HQ + HK + head) * HD, HD), HD)] = jnp.concatenate(
        grad_value, axis=0
    ).astype(jnp.bfloat16)
    gain_out_ref[0:1, :] += gain_query
    gain_out_ref[1:2, :] += gain_key


def attention_call(body, projected, tables, segments, gains, grad_out, first, count, base):
    token_rows = projected.shape[0]
    seq_count = token_rows // SEQ_LEN
    groups = HQ // HK
    wide = groups * HD
    full = lambda s, h: (s, 0)
    in_specs = [
        pl.BlockSpec((SEQ_LEN, wide), lambda s, h: (s, first + h)),
        pl.BlockSpec((SEQ_LEN, HD), lambda s, h: (s, HQ + first + h)),
        pl.BlockSpec((SEQ_LEN, HD), lambda s, h: (s, HQ + HK + first + h)),
        pl.BlockSpec((SEQ_LEN, HD), full),
        pl.BlockSpec((SEQ_LEN, HD), full),
        pl.BlockSpec((1, SEQ_LEN), lambda s, h: (0, s)),
        pl.BlockSpec((SEQ_LEN, 1), full),
        pl.BlockSpec((2, HD), lambda s, h: (0, 0)),
    ]
    operands = [
        projected,
        projected,
        projected,
        *tables,
        segments[None, :],
        segments[:, None],
        gains,
    ]
    pairs = token_rows * SEQ_LEN * groups * count
    aliases = {}
    if grad_out is None:
        out_specs = pl.BlockSpec((SEQ_LEN, wide), lambda s, h: (s, first + h))
        out_shape = jax.ShapeDtypeStruct((token_rows, HQ * HD), jnp.bfloat16)
    else:
        columns = projected.shape[1]
        in_specs.append(pl.BlockSpec((SEQ_LEN, wide), lambda s, h: (s, first + h)))
        operands.append(grad_out)
        body = functools.partial(body, first=first)
        if base is not None:
            aliases = {len(operands): 0}
            in_specs.append(pl.BlockSpec((SEQ_LEN, columns), full))
            operands.append(base)
        out_specs = [
            pl.BlockSpec((SEQ_LEN, columns), full),
            pl.BlockSpec((2, HD), lambda s, h: (0, 0)),
        ]
        out_shape = [
            jax.ShapeDtypeStruct((token_rows, columns), jnp.bfloat16),
            jax.ShapeDtypeStruct((2, HD), jnp.float32),
        ]
    return pl.pallas_call(
        body,
        grid=(seq_count, count),
        in_specs=in_specs,
        out_specs=out_specs,
        out_shape=out_shape,
        input_output_aliases=aliases,
        scratch_shapes=[pltpu.VMEM((SEQ_LEN, SEQ_LEN), jnp.float32)],
        compiler_params=pltpu.CompilerParams(vmem_limit_bytes=48 * 1024 * 1024),
        cost_estimate=pl.CostEstimate(
            flops=(4 if grad_out is None else 10) * pairs * HD * 2,
            bytes_accessed=projected.size * 6,
            transcendentals=pairs,
        ),
    )(*operands)


def gate_up_forward(hidden, full_gate_up):
    tokens, depth = hidden.shape
    block = 512
    steps = FF // block

    def body(hidden_ref, left_ref, right_ref, gate_ref, up_ref, out_ref):
        gate = jnp.dot(hidden_ref[...], left_ref[...], preferred_element_type=jnp.float32)
        upward = jnp.dot(hidden_ref[...], right_ref[...], preferred_element_type=jnp.float32)
        gate_ref[...] = gate
        up_ref[...] = upward
        out_ref[...] = (gate * jax.nn.sigmoid(gate) * upward).astype(jnp.bfloat16)

    wide = pl.BlockSpec((tokens, block), lambda j: (0, j))
    return pl.pallas_call(
        body,
        grid=(steps,),
        in_specs=[
            pl.BlockSpec((tokens, depth), lambda j: (0, 0)),
            pl.BlockSpec((depth, block), lambda j: (0, j)),
            pl.BlockSpec((depth, block), lambda j: (0, steps + j)),
        ],
        out_specs=[wide, wide, wide],
        out_shape=[
            jax.ShapeDtypeStruct((tokens, FF), jnp.float32),
            jax.ShapeDtypeStruct((tokens, FF), jnp.float32),
            jax.ShapeDtypeStruct((tokens, FF), jnp.bfloat16),
        ],
        compiler_params=pltpu.CompilerParams(vmem_limit_bytes=48 * 1024 * 1024),
        cost_estimate=pl.CostEstimate(
            flops=4 * tokens * FF * depth,
            bytes_accessed=4 * FF * depth + 10 * tokens * FF,
            transcendentals=tokens * FF,
        ),
    )(hidden, full_gate_up, full_gate_up)


def project_back(grad_low, weight, value, upstream, gain, whole):
    tokens, width = grad_low.shape
    depth = weight.shape[0]
    block = 1024
    steps = width // block

    def body(grad_ref, weight_ref, value_ref, up_ref, gain_ref, *rest):
        total_ref = rest[-1]
        step = pl.program_id(0)
        more = lax.dot_general(
            grad_ref[...],
            weight_ref[...],
            (((1,), (1,)), ((), ())),
            preferred_element_type=jnp.float32,
        )

        @pl.when(step == 0)
        def _():
            total_ref[...] = more

        @pl.when(step > 0)
        def _():
            total_ref[...] += more

        @pl.when(step == steps - 1)
        def _():
            raw = value_ref[...].astype(jnp.float32)
            root = lax.rsqrt(jnp.mean(raw * raw, axis=-1, keepdims=True) + EPS_NORM)
            normed = raw * root
            grad = total_ref[...]
            rest[1][...] = jnp.sum(grad * normed, axis=0, keepdims=True)
            full = up_ref[...].astype(jnp.float32) + norm_back(grad, normed, root, gain_ref[...])
            rest[0][...] = full.astype(jnp.bfloat16)
            if whole:
                rest[2][...] = full

    fixed = lambda j: (0, 0)
    square = pl.BlockSpec((tokens, depth), fixed)
    row = pl.BlockSpec((1, depth), fixed)
    shapes = [
        jax.ShapeDtypeStruct((tokens, depth), jnp.bfloat16),
        jax.ShapeDtypeStruct((1, depth), jnp.float32),
    ]
    if whole:
        shapes.append(jax.ShapeDtypeStruct((tokens, depth), jnp.float32))
    return pl.pallas_call(
        body,
        grid=(steps,),
        in_specs=[
            pl.BlockSpec((tokens, block), lambda j: (0, j)),
            pl.BlockSpec((depth, block), lambda j: (0, j)),
            square,
            square,
            row,
        ],
        out_specs=[square, row] + [square] * whole,
        out_shape=shapes,
        scratch_shapes=[pltpu.VMEM((tokens, depth), jnp.float32)],
        compiler_params=pltpu.CompilerParams(vmem_limit_bytes=48 * 1024 * 1024),
        cost_estimate=pl.CostEstimate(
            flops=2 * tokens * width * depth,
            bytes_accessed=2 * width * (depth + tokens) + 14 * tokens * depth,
            transcendentals=tokens,
        ),
    )(grad_low, weight, value, upstream, gain)


def gate_up_back(cotangent, full_down, gate_part, upward):
    tokens, columns = cotangent.shape
    block = 512
    steps = FF // block

    def body(cot_ref, down_ref, gate_ref, up_ref, out_ref):
        at = pl.program_id(0) * block
        grad = lax.dot_general(
            cot_ref[...],
            down_ref[...],
            (((1,), (1,)), ((), ())),
            preferred_element_type=jnp.float32,
        )
        gate = gate_ref[...]
        part = jax.nn.sigmoid(gate)
        grad_gate = grad * up_ref[...] * part * (1.0 + gate * (1.0 - part))
        grad_up = grad * gate * part
        out_ref[:, pl.ds(pl.multiple_of(at, block), block)] = grad_gate.astype(jnp.bfloat16)
        out_ref[:, pl.ds(pl.multiple_of(at + FF, block), block)] = grad_up.astype(jnp.bfloat16)

    return pl.pallas_call(
        body,
        grid=(steps,),
        in_specs=[
            pl.BlockSpec((tokens, columns), lambda j: (0, 0)),
            pl.BlockSpec((block, columns), lambda j: (j, 0)),
            pl.BlockSpec((tokens, block), lambda j: (0, j)),
            pl.BlockSpec((tokens, block), lambda j: (0, j)),
        ],
        out_specs=pl.BlockSpec((tokens, 2 * FF), lambda j: (0, 0)),
        out_shape=jax.ShapeDtypeStruct((tokens, 2 * FF), jnp.bfloat16),
        compiler_params=pltpu.CompilerParams(vmem_limit_bytes=48 * 1024 * 1024),
        cost_estimate=pl.CostEstimate(
            flops=2 * tokens * FF * columns,
            bytes_accessed=2 * FF * columns + 12 * tokens * FF,
            transcendentals=tokens * FF,
        ),
    )(cotangent, full_down, gate_part, upward)


def on_device(
    tokens,
    segment_ids,
    positions,
    cotangent,
    qkv_weight,
    out_weight,
    gate_up_weight,
    down_weight,
    norm_gains,
    head_gains,
    qkv_moments,
    out_moments,
    gate_up_moments,
    down_moments,
    norm_moments,
    head_moments,
):
    width = norm_gains.shape[1]
    gains_low = jnp.concatenate([norm_gains, head_gains], axis=1).astype(jnp.bfloat16)
    owners = lax.axis_size(GROUP)
    gains_all = gather_small(gains_low).reshape(2, owners, -1)
    full_norm = gains_all[:, :, :width].reshape(2, -1)
    full_head = gains_all[:, :, width:].reshape(2, -1)
    full_qkv, first, late, _ = gather_rows(qkv_weight, None, None, None, None, None)
    gain_one = full_norm[0].astype(jnp.float32)
    gain_two = full_norm[1].astype(jnp.float32)
    head_gain = full_head.astype(jnp.float32)
    inputs = tokens.astype(jnp.float32)
    root_one = lax.rsqrt(jnp.mean(inputs * inputs, axis=-1, keepdims=True) + EPS_NORM)
    normed_one = inputs * root_one
    hidden_one = (normed_one * gain_one).astype(jnp.bfloat16)
    projected = jnp.dot(hidden_one, full_qkv, preferred_element_type=jnp.float32)
    tables = rotary_tables(positions, HD)
    mixed_low = attention_call(attend_body, projected, tables, segment_ids, head_gain, None, 0, HK, None)
    full_out, _, down_late, _ = gather_rows(out_weight, first, late, None, projected, mixed_low)
    full_gate_up, _, more_late, _ = gather_rows(gate_up_weight, first, late, projected, None, None)
    attended = jnp.dot(mixed_low, full_out, preferred_element_type=jnp.float32)
    residual = inputs + attended
    root_two = lax.rsqrt(jnp.mean(residual * residual, axis=-1, keepdims=True) + EPS_NORM)
    normed_two = residual * root_two
    hidden_two = (normed_two * gain_two).astype(jnp.bfloat16)
    gate_part, upward, activated = gate_up_forward(hidden_two, full_gate_up)
    full_down, _, _, _ = gather_rows(
        down_weight, first, (down_late, more_late, projected), None, full_gate_up, activated
    )
    down_sum = GradSum(activated, cotangent, True)
    grad_gate_up = gate_up_back(
        after(cotangent, *down_sum.blocks), full_down, gate_part, upward
    )
    gate_up_sum = GradSum(hidden_two, after(grad_gate_up, *down_sum.advance()), True)
    residual_low, grad_gain_two, grad_residual = project_back(
        after(grad_gate_up, *gate_up_sum.blocks),
        full_gate_up,
        residual,
        cotangent,
        gain_two[None],
        True,
    )
    down_sum.hold(residual_low)
    sent = down_sum.advance() + gate_up_sum.advance()
    out_sum = GradSum(mixed_low, after(residual_low, *sent), True)
    down_sum.hold(out_sum.blocks)
    grad_mixed = contract_cols(
        after(residual_low, *out_sum.blocks, *down_sum.advance()), full_out
    ).astype(jnp.bfloat16)
    grad_mixed = after(grad_mixed, *out_sum.advance())
    half = HK // 2
    grad_half, gain_half = attention_call(
        attend_back_body, projected, tables, segment_ids, head_gain, grad_mixed, 0, half, None
    )
    gate_up_sum.hold(grad_half)
    down_sum.hold(grad_half)
    sent = gate_up_sum.advance() + down_sum.advance()
    grad_projected, grad_gain_head = attention_call(
        attend_back_body,
        projected,
        tables,
        segment_ids,
        head_gain,
        grad_mixed,
        half,
        HK - half,
        after(grad_half, *sent),
    )
    grad_gain_head = grad_gain_head + gain_half
    gate_up_sum.hold(grad_projected)
    out_sum.hold(grad_projected)
    sent = gate_up_sum.advance() + out_sum.advance()
    qkv_sum = GradSum(hidden_one, after(grad_projected, *sent), True)
    gate_up_sum.hold(qkv_sum.blocks)
    sent = qkv_sum.advance()
    gate_up_sum.hold(sent)
    out_sum.hold(sent)
    down_sum.hold(sent)
    sent = sent + gate_up_sum.advance() + out_sum.advance()
    branch = jnp.dot(after(activated, *sent), full_down, preferred_element_type=jnp.float32)
    output = (residual + branch).astype(jnp.bfloat16)
    tokens_grad, grad_gain_one = project_back(
        after(grad_projected, *qkv_sum.blocks, *sent),
        full_qkv,
        tokens,
        grad_residual,
        gain_one[None],
        False,
    )
    small = jnp.concatenate(
        [jnp.concatenate([grad_gain_one, grad_gain_two]), grad_gain_head],
        axis=1,
    )
    sent_next = qkv_sum.advance()
    sent_two = qkv_sum.advance()
    qkv_own, out_own, gate_up_own, down_own = owned = tuple(
        v.finish() for v in (qkv_sum, out_sum, gate_up_sum, down_sum)
    )
    down_gathered = gather_grad(down_own, None, sent_two)
    local = sum(jnp.sum(v * v) for v in owned)
    partial = jnp.concatenate(
        [small, jnp.full((6, small.shape[1]), local, jnp.float32)], axis=0
    )
    summed = sum_all(partial)
    small = summed[:2]
    norm_total = small[:, :-HD]
    head_total = small[:, -HD:]
    squares = summed[2, 0] + jnp.sum(small * small)
    clip_limit = math.sqrt(PARAMS)
    factor = clip_limit / jnp.maximum(jnp.sqrt(squares), clip_limit)
    renewed_down = adam_blocks(
        down_weight, down_moments, down_gathered, factor, LEARN_RATE, WEIGHT_DECAY
    )
    gathered = [
        gather_grad(after(qkv_own, summed), renewed_down[0], None),
        gather_grad(after(out_own, *sent_next), None, None),
        gather_grad(after(gate_up_own, *sent_next), None, summed),
    ]
    later = after(factor, gathered[0][0][0])
    renewed_gate_up = adam_blocks(
        gate_up_weight, gate_up_moments, gathered[2], later, LEARN_RATE, WEIGHT_DECAY
    )
    later = after(factor, renewed_gate_up[0])
    renewed_out = adam_blocks(
        out_weight, out_moments, gathered[1], later, LEARN_RATE, WEIGHT_DECAY
    )
    later = after(factor, renewed_out[0])
    renewed_qkv = adam_blocks(
        qkv_weight, qkv_moments, gathered[0], later, LEARN_RATE, WEIGHT_DECAY
    )
    renewed = [renewed_qkv, renewed_out, renewed_gate_up]
    renewed.append(renewed_down)
    mine = lax.axis_index(GROUP)
    norm_grad = lax.dynamic_slice_in_dim(
        norm_total, mine * norm_gains.shape[1], norm_gains.shape[1], 1
    )
    head_grad = lax.dynamic_slice_in_dim(
        head_total, mine * head_gains.shape[1], head_gains.shape[1], 1
    )
    renewed.append(adam_update(norm_gains, norm_moments, norm_grad, factor, GAIN_RATE, 0.0))
    renewed.append(adam_update(head_gains, head_moments, head_grad, factor, GAIN_RATE, 0.0))
    return (
        output,
        tokens_grad,
        *owned,
        norm_grad,
        head_grad,
        *[new for new, _ in renewed],
        *[state for _, state in renewed],
    )


def solution(mesh):
    placed = (
        P((DP, GROUP), None),
        P((DP, GROUP)),
        P((DP, GROUP)),
        P((DP, GROUP), None),
        P(GROUP, None),
        P(GROUP, None),
        P(GROUP, None),
        P(GROUP, None),
        P(None, GROUP),
        P(None, GROUP),
        P(None, GROUP, None),
        P(None, GROUP, None),
        P(None, GROUP, None),
        P(None, GROUP, None),
        P(None, None, GROUP),
        P(None, None, GROUP),
    )
    return jax.shard_map(
        on_device,
        mesh=mesh,
        in_specs=placed,
        out_specs=(
            P((DP, GROUP), None),
            P((DP, GROUP), None),
            P(GROUP, DP),
            P(GROUP, DP),
            P(GROUP, DP),
            P(GROUP, DP),
            P(None, GROUP),
            P(None, GROUP),
            P(GROUP, None),
            P(GROUP, None),
            P(GROUP, None),
            P(GROUP, None),
            P(None, GROUP),
            P(None, GROUP),
            P(None, GROUP, None),
            P(None, GROUP, None),
            P(None, GROUP, None),
            P(None, GROUP, None),
            P(None, None, GROUP),
            P(None, None, GROUP),
        ),
        check_vma=False,
    )
```
